32 devices in a mesh: dp: 2 (over x), y: 4 (over z), x: 4 (over y, core).
Axes of the slice: x: 2, y: 2, z: 4, core: 2. Of those that a mesh axis runs over, the one named last changes fastest.
Arguments:
- hidden: bfloat16 [128, 5120], P('dp', 'x'), parts along dimension 0
- positions: int32 [128], P('dp'), parts along dimension 0
- k_cache: bfloat16 [2, 128, 128, 8, 128], P(None, ('dp', 'x'), None, 'y'), parts along dimension 1
- v_cache: bfloat16 [2, 128, 128, 8, 128], P(None, ('dp', 'x'), None, 'y'), parts along dimension 1
- g_attn: bfloat16 [2, 5120], P(None, 'x')
- g_mlp: bfloat16 [2, 5120], P(None, 'x')
- q_gain: bfloat16 [2, 128], replicated
- k_gain: bfloat16 [2, 128], replicated
- w_q: bfloat16 [2, 5120, 5120], P(None, 'x', 'y')
- w_k: bfloat16 [2, 5120, 1024], P(None, 'x', 'y')
- w_v: bfloat16 [2, 5120, 1024], P(None, 'x', 'y')
- w_o: bfloat16 [2, 5120, 5120], P(None, 'y', 'x')
- w_gate: bfloat16 [2, 5120, 17408], P(None, 'x', 'y')
- w_up: bfloat16 [2, 5120, 17408], P(None, 'x', 'y')
- w_down: bfloat16 [2, 17408, 5120], P(None, 'y', 'x')
Outputs:
- output 1: bfloat16 [128, 5120], P('dp', 'x'), parts along dimension 0
- output 2: bfloat16 [2, 128, 128, 8, 128], P(None, ('dp', 'x'), None, 'y'), parts along dimension 1
- output 3: bfloat16 [2, 128, 128, 8, 128], P(None, ('dp', 'x'), None, 'y'), parts along dimension 1
There are 2 independent parts. The reference program is written for one: setup_inputs(seed, part) draws one part's arguments, and reference() takes and returns one part's arrays. A program takes and returns all parts, laid end to end along the dimension named above; an argument that names none is the same for every part.
All inputs are finite; a program needn't handle non-finite values.
Results may differ from the reference program's by a relative error of at most 0.02.
Values are sent between devices in bfloat16 or wider.
A program may use at most 1 GiB of HBM per device.

```python
import jax
import jax.numpy as jnp
from jax import lax

LAYERS = 2
BATCH = 64
CACHE_LEN = 128
MODEL_DIM = 5120
Q_HEADS = 40
KV_HEADS = 8
FFN_DIM = 17408
HEAD_DIM = 128
NORM_EPS = 1e-6
ROPE_BASE = 1000000.0


def rms_scale(hidden, norm_gain):
    hidden_f32 = hidden.astype(jnp.float32)
    mean_sq = jnp.mean(hidden_f32 * hidden_f32, axis=-1, keepdims=True)
    return hidden_f32 * lax.rsqrt(mean_sq + NORM_EPS) * norm_gain.astype(jnp.float32)


def rope_tables(positions):
    half_dim = HEAD_DIM // 2
    inv_freq = jnp.power(ROPE_BASE, -2.0 * jnp.arange(half_dim, dtype=jnp.float32) / HEAD_DIM)
    angles = positions.astype(jnp.float32)[:, None] * inv_freq[None, :]
    return jnp.cos(angles), jnp.sin(angles)


def apply_rope(heads_f32, cos_tab, sin_tab):
    half_dim = HEAD_DIM // 2
    first_half = heads_f32[..., :half_dim]
    second_half = heads_f32[..., half_dim:]
    cos_b = cos_tab[:, None, :]
    sin_b = sin_tab[:, None, :]
    return jnp.concatenate([first_half * cos_b - second_half * sin_b, second_half * cos_b + first_half * sin_b], axis=-1)


def decoder_layer(hidden, positions, layer_params):
    k_cache, v_cache, g_attn, g_mlp, q_gain, k_gain, w_q, w_k, w_v, w_o, w_gate, w_up, w_down = layer_params
    batch_rows = hidden.shape[0]
    group_size = Q_HEADS // KV_HEADS
    normed = rms_scale(hidden, g_attn).astype(jnp.bfloat16)
    q_proj = jnp.dot(normed, w_q, preferred_element_type=jnp.float32).astype(jnp.bfloat16).reshape(batch_rows, Q_HEADS, HEAD_DIM)
    k_proj = jnp.dot(normed, w_k, preferred_element_type=jnp.float32).astype(jnp.bfloat16).reshape(batch_rows, KV_HEADS, HEAD_DIM)
    v_proj = jnp.dot(normed, w_v, preferred_element_type=jnp.float32).astype(jnp.bfloat16).reshape(batch_rows, KV_HEADS, HEAD_DIM)
    cos_tab, sin_tab = rope_tables(positions)
    q_rot = apply_rope(rms_scale(q_proj, q_gain), cos_tab, sin_tab).astype(jnp.bfloat16)
    k_rot = apply_rope(rms_scale(k_proj, k_gain), cos_tab, sin_tab).astype(jnp.bfloat16)
    slot_ids = jnp.arange(CACHE_LEN, dtype=jnp.int32)[None, :]
    slot_hit = (slot_ids == positions[:, None])[:, :, None, None]
    k_new = jnp.where(slot_hit, k_rot[:, None], k_cache)
    v_new = jnp.where(slot_hit, v_proj[:, None], v_cache)
    q_grouped = q_rot.reshape(batch_rows, KV_HEADS, group_size, HEAD_DIM)
    scores = jnp.einsum('bkge,blke->bkgl', q_grouped.astype(jnp.float32), k_new.astype(jnp.float32)) * (HEAD_DIM ** -0.5)
    valid_slot = (slot_ids <= positions[:, None])[:, None, None, :]
    scores = jnp.where(valid_slot, scores, -1e30)
    att_probs = jax.nn.softmax(scores, axis=-1).astype(jnp.bfloat16)
    attn_heads = jnp.einsum('bkgl,blke->bkge', att_probs.astype(jnp.float32), v_new.astype(jnp.float32)).astype(jnp.bfloat16)
    attn_out = jnp.dot(attn_heads.reshape(batch_rows, Q_HEADS * HEAD_DIM), w_o, preferred_element_type=jnp.float32).astype(jnp.bfloat16)
    mid_hidden = (hidden.astype(jnp.float32) + attn_out.astype(jnp.float32)).astype(jnp.bfloat16)
    normed_mlp = rms_scale(mid_hidden, g_mlp).astype(jnp.bfloat16)
    gate_val = jnp.dot(normed_mlp, w_gate, preferred_element_type=jnp.float32).astype(jnp.bfloat16)
    up_val = jnp.dot(normed_mlp, w_up, preferred_element_type=jnp.float32).astype(jnp.bfloat16)
    act_val = (jax.nn.silu(gate_val.astype(jnp.float32)) * up_val.astype(jnp.float32)).astype(jnp.bfloat16)
    mlp_out = jnp.dot(act_val, w_down, preferred_element_type=jnp.float32).astype(jnp.bfloat16)
    new_hidden = (mid_hidden.astype(jnp.float32) + mlp_out.astype(jnp.float32)).astype(jnp.bfloat16)
    return new_hidden, k_new, v_new


def setup_inputs(seed: int = 0, part: int = 0) -> dict:
    part_keys = jax.random.split(jax.random.fold_in(jax.random.key(seed), part), 5)
    weight_keys = jax.random.split(jax.random.key(seed + 7919), 11)
    q_width = Q_HEADS * HEAD_DIM
    kv_width = KV_HEADS * HEAD_DIM
    cache_shape = (LAYERS, BATCH, CACHE_LEN, KV_HEADS, HEAD_DIM)
    row_scale = jnp.exp(0.4 * jax.random.normal(part_keys[0], (BATCH, 1), jnp.float32))
    hidden = (jax.random.normal(part_keys[1], (BATCH, MODEL_DIM), jnp.float32) * row_scale).astype(jnp.bfloat16)
    raw_pos = jax.random.randint(part_keys[2], (BATCH,), 0, CACHE_LEN, jnp.int32)
    row_ids = jnp.arange(BATCH, dtype=jnp.int32)
    positions = jnp.where(row_ids == 0, CACHE_LEN - 1, jnp.where(row_ids == 1, 0, raw_pos)).astype(jnp.int32)
    k_cache = jax.random.normal(part_keys[3], cache_shape, jnp.float32).astype(jnp.bfloat16)
    v_cache = jax.random.normal(part_keys[4], cache_shape, jnp.float32).astype(jnp.bfloat16)
    g_attn = (1.0 + 0.25 * jax.random.normal(weight_keys[0], (LAYERS, MODEL_DIM), jnp.float32)).astype(jnp.bfloat16)
    g_mlp = (1.0 + 0.25 * jax.random.normal(weight_keys[1], (LAYERS, MODEL_DIM), jnp.float32)).astype(jnp.bfloat16)
    q_gain = (1.6 + 0.3 * jax.random.normal(weight_keys[2], (LAYERS, HEAD_DIM), jnp.float32)).astype(jnp.bfloat16)
    k_gain = (4.0 * jax.random.normal(weight_keys[3], (LAYERS, HEAD_DIM), jnp.float32)).astype(jnp.bfloat16)
    w_q = (jax.random.normal(weight_keys[4], (LAYERS, MODEL_DIM, q_width), jnp.float32) * MODEL_DIM ** -0.5).astype(jnp.bfloat16)
    w_k = (jax.random.normal(weight_keys[5], (LAYERS, MODEL_DIM, kv_width), jnp.float32) * MODEL_DIM ** -0.5).astype(jnp.bfloat16)
    w_v = (jax.random.normal(weight_keys[6], (LAYERS, MODEL_DIM, kv_width), jnp.float32) * MODEL_DIM ** -0.5).astype(jnp.bfloat16)
    w_o = (jax.random.normal(weight_keys[7], (LAYERS, q_width, MODEL_DIM), jnp.float32) * q_width ** -0.5).astype(jnp.bfloat16)
    w_gate = (jax.random.normal(weight_keys[8], (LAYERS, MODEL_DIM, FFN_DIM), jnp.float32) * MODEL_DIM ** -0.5).astype(jnp.bfloat16)
    w_up = (jax.random.normal(weight_keys[9], (LAYERS, MODEL_DIM, FFN_DIM), jnp.float32) * MODEL_DIM ** -0.5).astype(jnp.bfloat16)
    w_down = (jax.random.normal(weight_keys[10], (LAYERS, FFN_DIM, MODEL_DIM), jnp.float32) * FFN_DIM ** -0.5).astype(jnp.bfloat16)
    return {'hidden': hidden, 'positions': positions, 'k_cache': k_cache, 'v_cache': v_cache, 'g_attn': g_attn, 'g_mlp': g_mlp, 'q_gain': q_gain, 'k_gain': k_gain, 'w_q': w_q, 'w_k': w_k, 'w_v': w_v, 'w_o': w_o, 'w_gate': w_gate, 'w_up': w_up, 'w_down': w_down}


def reference(hidden, positions, k_cache, v_cache, g_attn, g_mlp, q_gain, k_gain, w_q, w_k, w_v, w_o, w_gate, w_up, w_down):
    def layer_step(carry_hidden, layer_params):
        new_hidden, k_new, v_new = decoder_layer(carry_hidden, positions, layer_params)
        return new_hidden, (k_new, v_new)
    out_hidden, cache_pair = lax.scan(layer_step, hidden, (k_cache, v_cache, g_attn, g_mlp, q_gain, k_gain, w_q, w_k, w_v, w_o, w_gate, w_up, w_down))
    return out_hidden, cache_pair[0], cache_pair[1]
```

```python
import functools

import jax
import jax.numpy as jnp
from jax import lax
from jax.experimental import pallas as pl
from jax.experimental.pallas import tpu as pltpu
from jax.sharding import PartitionSpec as P

HEAD_DIM = 128
NORM_EPS = 1e-6
ROPE_BASE = 1000000.0
TILE = 256
CHUNKS = 4
MESH = pl.DeviceIdType.MESH
F32 = jnp.float32
BF16 = jnp.bfloat16
N_REMOTE = 160
N_LOCAL = 48


def rope_tables(positions):
    half_dim = HEAD_DIM // 2
    inv_freq = jnp.power(ROPE_BASE, -2.0 * jnp.arange(half_dim, dtype=F32) / HEAD_DIM)
    angles = positions.astype(F32)[:, None] * inv_freq[None, :]
    return jnp.cos(angles), jnp.sin(angles)


def split_tiles(n_tiles, n_chunks):
    sizes = [n_tiles // n_chunks + (1 if i < n_tiles % n_chunks else 0) for i in range(n_chunks)]
    starts = [sum(sizes[:i]) for i in range(n_chunks)]
    return [(s * TILE, z * TILE) for s, z in zip(starts, sizes) if z]


def step_kernel(dims, *refs):
    (layers, n_y, n_x, rows, depth, q_cols, kv_cols, ffn) = dims
    (hid_ref, pos_ref, cos_ref, sin_ref, ga_ref, gm_ref, qg_ref, kg_ref, kc_ref, vc_ref,
     wq_ref, wk_ref, wv_ref, wo_ref, wg_ref, wu_ref, wd_ref,
     hid_out, kc_out, vc_out,
     wqkv, wo, wg, wu, wd, kbuf, vbuf, n_buf, stat, qkv_part, qkv_recv, q_rows, o_rows, attn_all,
     ar_part, ar_recv, h_all, gu_part, gu_pair, gu_send, gu_recv, act_all, acc,
     send_sem, recv_sem, local_sem) = refs
    batch = n_y * rows
    cols_qkv = q_cols + 2 * kv_cols
    q_heads = q_cols // HEAD_DIM
    kv_heads = kv_cols // HEAD_DIM
    group = q_heads // kv_heads
    chunks = split_tiles(ffn // TILE, CHUNKS)
    model_dim = depth * n_x
    slots2 = kbuf.shape[2]

    y = lax.axis_index("y")
    x = lax.axis_index("x")
    chip = x // 2
    core = x % 2
    partner = 2 * chip + (1 - core)
    across = 2 * (1 - chip) + core

    counter = {"remote": 0, "local": 0}
    sent = []
    stored = []

    def remote(src, dst, to_y, to_x):
        i = counter["remote"]
        counter["remote"] += 1
        copy = pltpu.make_async_remote_copy(
            src_ref=src, dst_ref=dst, send_sem=send_sem.at[i], recv_sem=recv_sem.at[i],
            device_id={"y": to_y, "x": to_x}, device_id_type=MESH)
        copy.start()
        sent.append(copy)
        return copy

    def local(src, dst):
        i = counter["local"]
        counter["local"] += 1
        copy = pltpu.make_async_copy(src, dst, local_sem.at[i])
        copy.start()
        return copy

    def load_qkv(layer):
        return [local(wq_ref.at[layer], wqkv.at[:, 0:q_cols]),
                local(wk_ref.at[layer], wqkv.at[:, q_cols:q_cols + kv_cols]),
                local(wv_ref.at[layer], wqkv.at[:, q_cols + kv_cols:cols_qkv])]

    def load_o(layer):
        return [local(wo_ref.at[layer], wo)]

    def load_gate_up(layer, j):
        cols = pl.ds(chunks[j][0], chunks[j][1])
        return [local(wg_ref.at[layer, :, cols], wg.at[:, cols]),
                local(wu_ref.at[layer, :, cols], wu.at[:, cols])]

    def load_down(layer, j):
        cols = pl.ds(chunks[j][0], chunks[j][1])
        return [local(wd_ref.at[layer, cols, :], wd.at[cols, :])]

    def load_cache(layer):
        return [local(kc_ref.at[layer], kbuf.at[layer]), local(vc_ref.at[layer], vbuf.at[layer])]

    def wait_all(copies):
        for copy in copies:
            copy.wait()

    row_i = lax.broadcasted_iota(jnp.int32, (rows, HEAD_DIM), 0)
    lane_i = lax.broadcasted_iota(jnp.int32, (rows, HEAD_DIM), 1)

    def pack_rows(vals_f32, first_row):
        sums = jnp.sum(vals_f32 * vals_f32, axis=1, keepdims=True)
        return jnp.sum(jnp.where(lane_i == row_i + first_row, sums, 0.0), axis=0, keepdims=True)

    all_row = lax.broadcasted_iota(jnp.int32, (batch, HEAD_DIM), 0)
    all_lane = lax.broadcasted_iota(jnp.int32, (batch, HEAD_DIM), 1)

    def row_scales(i, count):
        total = stat[i, 0]
        for s in range(1, count):
            total = total + stat[i, s]
        scale = lax.rsqrt(total / model_dim + NORM_EPS)
        return jnp.sum(jnp.where(all_lane == all_row, scale, 0.0), axis=1, keepdims=True)

    def normalise(hidden_ref, i, count, gain_ref, layer):
        scales = row_scales(i, count)
        gain = gain_ref[...].astype(F32)[layer:layer + 1]
        vals = hidden_ref[...].reshape(batch, depth).astype(F32)
        n_buf[...] = (vals * scales * gain).astype(BF16)

    def all_reduce(i, residual_ref, with_stats):
        copies = [remote(ar_part.at[i, (y + d) % n_y], ar_recv.at[i, d], (y + d) % n_y, x) for d in (3, 2, 1)]
        total = ar_part[i, y].astype(F32)
        for copy in copies:
            copy.wait_recv()
        for d in range(1, n_y):
            total = total + ar_recv[i, d].astype(F32)
        new = (residual_ref[y].astype(F32) + total.astype(BF16).astype(F32)).astype(BF16)
        h_all[i, y] = new
        gathers = [remote(h_all.at[i, y], h_all.at[i, y], (y + d) % n_y, x) for d in (3, 2, 1)]
        stats = []
        if with_stats:
            stat[i + 1, 0] = pack_rows(new.astype(F32), y * rows)
            stats = [remote(stat.at[i + 1, 0], stat.at[i + 1, dy * n_x + dx], (y + dy) % n_y, (x + dx) % n_x)
                     for dy in (3, 2, 1, 0) for dx in range(n_x) if dy or dx]
        for copy in gathers + stats:
            copy.wait_recv()

    pending_qkv = load_qkv(0)
    barrier = pltpu.get_barrier_semaphore()
    for dy in range(n_y):
        for dx in range(n_x):
            if dy or dx:
                pl.semaphore_signal(barrier, inc=1, device_id={"y": (y + dy) % n_y, "x": (x + dx) % n_x}, device_id_type=MESH)
    own = jnp.zeros((1, HEAD_DIM), F32)
    for b in range(n_y):
        own = own + pack_rows(hid_ref[b].astype(F32), b * rows)
    stat[0, 0] = own
    pl.semaphore_wait(barrier, n_y * n_x - 1)
    first_stats = [remote(stat.at[0, 0], stat.at[0, d], y, (x + d) % n_x) for d in range(1, n_x)]
    pending_o = load_o(0)
    pending_cache = [load_cache(0)]
    pending_gu = [load_gate_up(0, j) for j in range(len(chunks))]
    pending_down = [load_down(0, j) for j in range(len(chunks))]
    pending_cache += [load_cache(layer) for layer in range(1, layers)]
    q_rows[...] = jnp.zeros_like(q_rows)
    for copy in first_stats:
        copy.wait_recv()

    cos_tab = cos_ref[...]
    sin_tab = sin_ref[...]
    slot_row = lax.broadcasted_iota(jnp.int32, (slots2, HEAD_DIM), 0)
    slot_id = slot_row // kv_heads
    head_id = slot_row % kv_heads
    score_col = lax.broadcasted_iota(jnp.int32, (16, slots2), 1)
    score_head = lax.broadcasted_iota(jnp.int32, (16, slots2), 0) // group

    residual = hid_ref
    for layer in range(layers):
        more = layer + 1 < layers
        a, m = 2 * layer, 2 * layer + 1
        normalise(residual, a, n_x if layer == 0 else n_y * n_x, ga_ref, layer)
        wait_all(pending_qkv)

        def qkv_tile(t, carry):
            cols = pl.ds(pl.multiple_of(t * TILE, TILE), TILE)
            part = jnp.dot(n_buf[...], wqkv[:, cols], preferred_element_type=F32).astype(BF16)
            qkv_part[layer, :, :, cols] = part.reshape(n_x, batch // n_x, TILE)
            return carry

        lax.fori_loop(0, cols_qkv // TILE, qkv_tile, 0)
        copies = [remote(qkv_part.at[layer, (x + d) % n_x], qkv_recv.at[layer, d], y, (x + d) % n_x) for d in (2, 3, 1)]
        if more:
            pending_qkv = load_qkv(layer + 1)
        total = qkv_part[layer, x].astype(F32)
        for copy in copies:
            copy.wait_recv()
        for d in range(1, n_x):
            total = total + qkv_recv[layer, d].astype(F32)
        proj = total.astype(BF16).astype(F32)

        def rotate(vals, gain):
            mean_sq = jnp.mean(vals * vals, axis=-1, keepdims=True)
            normed = vals * lax.rsqrt(mean_sq + NORM_EPS) * gain
            turned = normed * cos_tab + pltpu.roll(normed, HEAD_DIM // 2, 1) * sin_tab
            return turned.astype(BF16).astype(F32)

        q_gain = qg_ref[...].astype(F32)[layer:layer + 1]
        k_gain = kg_ref[...].astype(F32)[layer:layer + 1]
        n_seq = batch // n_x
        for h in range(q_heads):
            q_rows[h * n_seq:(h + 1) * n_seq, :] = rotate(proj[:, h * HEAD_DIM:(h + 1) * HEAD_DIM], q_gain)
        k_new = [rotate(proj[:, q_cols + h * HEAD_DIM:q_cols + (h + 1) * HEAD_DIM], k_gain) for h in range(kv_heads)]
        v_new = [proj[:, q_cols + kv_cols + h * HEAD_DIM:q_cols + kv_cols + (h + 1) * HEAD_DIM] for h in range(kv_heads)]

        wait_all(pending_cache[layer])
        for b in range(n_seq):
            pos = pos_ref[b]
            hit = slot_id == pos[:, :HEAD_DIM]
            for buf, new in ((kbuf, k_new), (vbuf, v_new)):
                fresh = new[0][b:b + 1]
                for h in range(1, kv_heads):
                    fresh = jnp.where(head_id == h, new[h][b:b + 1], fresh)
                buf[layer, b] = jnp.where(hit, fresh, buf[layer, b].astype(F32)).astype(BF16)
            q_b = q_rows[pl.ds(b, 16, stride=n_seq), :].astype(BF16)
            scores = lax.dot_general(q_b, kbuf[layer, b], (((1,), (1,)), ((), ())), preferred_element_type=F32) * (HEAD_DIM ** -0.5)
            valid = (score_col // kv_heads <= pos) & (score_col % kv_heads == score_head)
            valid = valid | (score_head >= kv_heads)
            scores = jnp.where(valid, scores, -1e30)
            top = jnp.max(scores, axis=1, keepdims=True)
            e = jnp.exp(scores - top)
            probs = (e / jnp.sum(e, axis=1, keepdims=True)).astype(BF16)
            o_rows[b * 16:(b + 1) * 16, :] = jnp.dot(probs, vbuf[layer, b], preferred_element_type=F32)
        stored += [local(kbuf.at[layer], kc_out.at[layer]), local(vbuf.at[layer], vc_out.at[layer])]
        for h in range(q_heads):
            attn_all[layer, x, :, h * HEAD_DIM:(h + 1) * HEAD_DIM] = o_rows[pl.ds(h, n_seq, stride=16), :].astype(BF16)
        copies = [remote(attn_all.at[layer, x], attn_all.at[layer, x], y, (x + d) % n_x) for d in (2, 3, 1)]
        wait_all(pending_o)
        for copy in copies:
            copy.wait_recv()

        def o_tile(t, carry):
            cols = pl.ds(pl.multiple_of(t * TILE, TILE), TILE)
            part = jnp.dot(attn_all[layer].reshape(batch, q_cols), wo[:, cols], preferred_element_type=F32).astype(BF16)
            ar_part[a, :, :, cols] = part.reshape(n_y, rows, TILE)
            return carry

        lax.fori_loop(0, depth // TILE, o_tile, 0)
        if more:
            pending_o = load_o(layer + 1)
        all_reduce(a, residual, True)

        normalise(h_all.at[a], a + 1, n_y * n_x, gm_ref, layer)
        to_pair, to_across, own_gather, across_gather, forward = {}, {}, {}, {}, {}

        def project(j):
            wait_all(pending_gu[j])
            start, width = chunks[j]

            def tile(t, carry):
                cols = pl.ds(pl.multiple_of(start + t * TILE, TILE), TILE)
                gate = jnp.dot(n_buf[...], wg[:, cols], preferred_element_type=F32).astype(BF16)
                up = jnp.dot(n_buf[...], wu[:, cols], preferred_element_type=F32).astype(BF16)
                gu_part[layer, 0, :, :, :, cols] = gate.reshape(2, 2, rows, TILE)
                gu_part[layer, 1, :, :, :, cols] = up.reshape(2, 2, rows, TILE)
                return carry

            lax.fori_loop(0, width // TILE, tile, 0)
            cols = pl.ds(start, width)
            to_pair[j] = remote(gu_part.at[layer, :, :, 1 - core, :, cols], gu_pair.at[layer, :, :, :, cols], y, partner)
            if more:
                pending_gu[j] = load_gate_up(layer + 1, j)

        def cross(j):
            cols = pl.ds(*chunks[j])
            to_pair[j].wait_recv()
            pair = gu_part[layer, :, 1 - chip, core, :, cols].astype(F32) + gu_pair[layer, :, 1 - chip, :, cols].astype(F32)
            gu_send[layer, :, :, cols] = pair.astype(BF16)
            to_across[j] = remote(gu_send.at[layer, :, :, cols], gu_recv.at[layer, :, :, cols], y, across)

        def activate(j):
            cols = pl.ds(*chunks[j])
            to_across[j].wait_recv()
            gate_up = (gu_part[layer, :, chip, core, :, cols].astype(F32) + gu_pair[layer, :, chip, :, cols].astype(F32)
                       + gu_recv[layer, :, :, cols].astype(F32)).astype(BF16).astype(F32)
            act_all[layer, x, :, cols] = (jax.nn.silu(gate_up[0]) * gate_up[1]).astype(BF16)
            mine = act_all.at[layer, x, :, cols]
            across_gather[j] = remote(mine, mine, y, across)
            own_gather[j] = remote(mine, mine, y, partner)

        def pass_on(j):
            cols = pl.ds(*chunks[j])
            across_gather[j].wait_recv()
            theirs = act_all.at[layer, across, :, cols]
            forward[j] = remote(theirs, theirs, y, partner)

        def down(j):
            own_gather[j].wait_recv()
            forward[j].wait_recv()
            wait_all(pending_down[j])
            start, width = chunks[j]

            def tile(t, carry):
                cols = pl.ds(pl.multiple_of(t * TILE, TILE), TILE)
                vals = act_all[layer, :, :, pl.ds(start, width)].reshape(batch, width)
                part = jnp.dot(vals, wd[pl.ds(start, width), cols], preferred_element_type=F32)
                if j:
                    part = part + acc[:, cols]
                if j < len(chunks) - 1:
                    acc[:, cols] = part
                else:
                    ar_part[m, :, :, cols] = part.astype(BF16).reshape(n_y, rows, TILE)
                return carry

            lax.fori_loop(0, depth // TILE, tile, 0)
            if more:
                pending_down[j] = load_down(layer + 1, j)

        phases = (project, cross, activate, pass_on, down)
        for stage in range(len(chunks) + len(phases) - 1):
            for lag, phase in enumerate(phases):
                if 0 <= stage - lag < len(chunks):
                    phase(stage - lag)
        all_reduce(m, h_all.at[a], more)
        residual = h_all.at[m]

    hid_out[...] = residual[...]
    for copy in sent:
        copy.wait_send()
    wait_all(stored)


def solution(mesh):
    n_x, n_y = mesh.shape['x'], mesh.shape['y']
    cache_spec = P(None, ('dp', 'x'), None, 'y', None)
    col_spec = P(None, 'x', 'y')
    row_spec = P(None, 'y', 'x')
    in_specs = (P('dp', 'x'), P('dp'), cache_spec, cache_spec, P(None, 'x'), P(None, 'x'), P(), P(), col_spec, col_spec, col_spec, row_spec, col_spec, col_spec, row_spec)
    out_specs = (P('dp', 'x'), cache_spec, cache_spec)

    def device_step(hidden, positions, k_cache, v_cache, g_attn, g_mlp, q_gain, k_gain, w_q, w_k, w_v, w_o, w_gate, w_up, w_down):
        batch, depth = hidden.shape
        layers, n_seq, slots, kv_heads, _ = k_cache.shape
        q_cols, kv_cols, ffn = w_q.shape[2], w_k.shape[2], w_gate.shape[2]
        rows = batch // n_y
        slots2 = slots * kv_heads
        my_pos = lax.dynamic_slice_in_dim(positions, lax.axis_index('x') * n_seq, n_seq)
        cos_half, sin_half = rope_tables(my_pos)
        cos_tab = jnp.concatenate([cos_half, cos_half], axis=1)
        sin_tab = jnp.concatenate([-sin_half, sin_half], axis=1)
        pos_rows = jnp.broadcast_to(my_pos[:, None, None], (n_seq, 1, slots2))
        dims = (layers, n_y, n_x, rows, depth, q_cols, kv_cols, ffn)
        cols_qkv = q_cols + 2 * kv_cols
        vmem = pl.BlockSpec(memory_space=pltpu.VMEM)
        hbm = pl.BlockSpec(memory_space=pl.ANY)
        cache_shape = (layers, n_seq, slots2, HEAD_DIM)
        norms = 2 * layers
        new_hidden, k_new, v_new = pl.pallas_call(
            functools.partial(step_kernel, dims),
            out_shape=(jax.ShapeDtypeStruct((n_y, rows, depth), BF16), jax.ShapeDtypeStruct(cache_shape, BF16), jax.ShapeDtypeStruct(cache_shape, BF16)),
            in_specs=[vmem] * 8 + [hbm] * 9,
            out_specs=(vmem, hbm, hbm),
            scratch_shapes=[
                pltpu.VMEM((depth, cols_qkv), BF16),
                pltpu.VMEM((q_cols, depth), BF16),
                pltpu.VMEM((depth, ffn), BF16),
                pltpu.VMEM((depth, ffn), BF16),
                pltpu.VMEM((ffn, depth), BF16),
                pltpu.VMEM(cache_shape, BF16),
                pltpu.VMEM(cache_shape, BF16),
                pltpu.VMEM((batch, depth), BF16),
                pltpu.VMEM((norms, n_y * n_x, 1, HEAD_DIM), F32),
                pltpu.VMEM((layers, n_x, n_seq, cols_qkv), BF16),
                pltpu.VMEM((layers, n_x, n_seq, cols_qkv), BF16),
                pltpu.VMEM((16 * n_seq, HEAD_DIM), F32),
                pltpu.VMEM((16 * n_seq, HEAD_DIM), F32),
                pltpu.VMEM((layers, n_x, n_seq, q_cols), BF16),
                pltpu.VMEM((norms, n_y, rows, depth), BF16),
                pltpu.VMEM((norms, n_y, rows, depth), BF16),
                pltpu.VMEM((norms, n_y, rows, depth), BF16),
                pltpu.VMEM((layers, 2, 2, 2, rows, ffn), BF16),
                pltpu.VMEM((layers, 2, 2, rows, ffn), BF16),
                pltpu.VMEM((layers, 2, rows, ffn), BF16),
                pltpu.VMEM((layers, 2, rows, ffn), BF16),
                pltpu.VMEM((layers, n_x, rows, ffn), BF16),
                pltpu.VMEM((batch, depth), F32),
                pltpu.SemaphoreType.DMA((N_REMOTE,)),
                pltpu.SemaphoreType.DMA((N_REMOTE,)),
                pltpu.SemaphoreType.DMA((N_LOCAL,)),
            ],
            compiler_params=pltpu.CompilerParams(collective_id=0, has_side_effects=True, vmem_limit_bytes=64 * 1024 * 1024 - 65536),
        )(hidden.reshape(n_y, rows, depth), pos_rows, cos_tab, sin_tab, g_attn, g_mlp, q_gain, k_gain,
          k_cache.reshape(cache_shape), v_cache.reshape(cache_shape), w_q, w_k, w_v, w_o, w_gate, w_up, w_down)
        return new_hidden.reshape(batch, depth), k_new.reshape(k_cache.shape), v_new.reshape(v_cache.shape)

    return jax.shard_map(device_step, mesh=mesh, in_specs=in_specs, out_specs=out_specs, check_vma=False)
```

```python
import functools

import jax
import jax.numpy as jnp
import numpy as np
from jax import lax
from jax.experimental import pallas as pl
from jax.experimental.pallas import tpu as pltpu
from jax.sharding import PartitionSpec as P

HEAD_DIM = 128
NORM_EPS = 1e-6
ROPE_BASE = 1000000.0
TILE = 256
CHUNKS = 4
MESH = pl.DeviceIdType.MESH
F32 = jnp.float32
BF16 = jnp.bfloat16
N_REMOTE = 160
N_LOCAL = 48


def inverse_frequencies():
    half_dim = HEAD_DIM // 2
    freqs = np.power(np.float32(ROPE_BASE), (-2.0 * np.arange(half_dim) / HEAD_DIM).astype(np.float32))
    return np.concatenate([freqs, freqs])[None].astype(np.float32)


def split_tiles(n_tiles, n_chunks):
    sizes = [n_tiles // n_chunks + (1 if i < n_tiles % n_chunks else 0) for i in range(n_chunks)]
    starts = [sum(sizes[:i]) for i in range(n_chunks)]
    return [(s * TILE, z * TILE) for s, z in zip(starts, sizes) if z]


def step_kernel(dims, *refs):
    (layers, n_y, n_x, rows, depth, q_cols, kv_cols, ffn) = dims
    (hid_ref, pos_ref, freq_ref, ga_ref, gm_ref, qg_ref, kg_ref, kc_ref, vc_ref,
     wq_ref, wk_ref, wv_ref, wo_ref, wg_ref, wu_ref, wd_ref,
     hid_out, new_out,
     wqkv, wo, wg, wu, wd, kbuf, vbuf, n_buf, stat, qkv_part, qkv_recv, q_rows, o_rows, attn_all,
     ar_part, ar_recv, h_all, gu_part, gu_pair, gu_send, gu_recv, act_all, acc,
     send_sem, recv_sem, local_sem) = refs
    batch = n_y * rows
    cols_qkv = q_cols + 2 * kv_cols
    q_heads = q_cols // HEAD_DIM
    kv_heads = kv_cols // HEAD_DIM
    group = q_heads // kv_heads
    chunks = split_tiles(ffn // TILE, CHUNKS)
    model_dim = depth * n_x
    slots2 = kbuf.shape[2]

    y = lax.axis_index("y")
    x = lax.axis_index("x")
    chip = x // 2
    core = x % 2
    partner = 2 * chip + (1 - core)
    across = 2 * (1 - chip) + core

    counter = {"remote": 0, "local": 0}
    sent = []

    def remote(src, dst, to_y, to_x):
        i = counter["remote"]
        counter["remote"] += 1
        copy = pltpu.make_async_remote_copy(
            src_ref=src, dst_ref=dst, send_sem=send_sem.at[i], recv_sem=recv_sem.at[i],
            device_id={"y": to_y, "x": to_x}, device_id_type=MESH)
        copy.start()
        sent.append(copy)
        return copy

    def local(src, dst):
        i = counter["local"]
        counter["local"] += 1
        copy = pltpu.make_async_copy(src, dst, local_sem.at[i])
        copy.start()
        return copy

    def load_qkv(layer):
        return [local(wq_ref.at[layer], wqkv.at[:, 0:q_cols]),
                local(wk_ref.at[layer], wqkv.at[:, q_cols:q_cols + kv_cols]),
                local(wv_ref.at[layer], wqkv.at[:, q_cols + kv_cols:cols_qkv])]

    def load_o(layer):
        return [local(wo_ref.at[layer], wo)]

    def load_gate_up(layer, j):
        cols = pl.ds(chunks[j][0], chunks[j][1])
        return [local(wg_ref.at[layer, :, cols], wg.at[:, cols]),
                local(wu_ref.at[layer, :, cols], wu.at[:, cols])]

    def load_down(layer, j):
        cols = pl.ds(chunks[j][0], chunks[j][1])
        return [local(wd_ref.at[layer, cols, :], wd.at[cols, :])]

    def load_cache(layer):
        return [local(kc_ref.at[layer], kbuf.at[layer]), local(vc_ref.at[layer], vbuf.at[layer])]

    def wait_all(copies):
        for copy in copies:
            copy.wait()

    row_i = lax.broadcasted_iota(jnp.int32, (rows, HEAD_DIM), 0)
    lane_i = lax.broadcasted_iota(jnp.int32, (rows, HEAD_DIM), 1)

    def pack_rows(vals_f32, first_row):
        sums = jnp.sum(vals_f32 * vals_f32, axis=1, keepdims=True)
        return jnp.sum(jnp.where(lane_i == row_i + first_row, sums, 0.0), axis=0, keepdims=True)

    all_row = lax.broadcasted_iota(jnp.int32, (batch, HEAD_DIM), 0)
    all_lane = lax.broadcasted_iota(jnp.int32, (batch, HEAD_DIM), 1)

    def row_scales(i, count):
        total = stat[i, 0]
        for s in range(1, count):
            total = total + stat[i, s]
        scale = lax.rsqrt(total / model_dim + NORM_EPS)
        return jnp.sum(jnp.where(all_lane == all_row, scale, 0.0), axis=1, keepdims=True)

    def normalise(hidden_ref, i, count, gain_ref, layer):
        scales = row_scales(i, count)
        gain = gain_ref[...].astype(F32)[layer:layer + 1]
        vals = hidden_ref[...].reshape(batch, depth).astype(F32)
        n_buf[...] = (vals * scales * gain).astype(BF16)

    def all_reduce(i, residual_ref, with_stats):
        copies = [remote(ar_part.at[i, (y + d) % n_y], ar_recv.at[i, d], (y + d) % n_y, x) for d in (3, 2, 1)]
        total = ar_part[i, y].astype(F32)
        for copy in copies:
            copy.wait_recv()
        for d in range(1, n_y):
            total = total + ar_recv[i, d].astype(F32)
        new = (residual_ref[y].astype(F32) + total.astype(BF16).astype(F32)).astype(BF16)
        h_all[i, y] = new
        gathers = [remote(h_all.at[i, y], h_all.at[i, y], (y + d) % n_y, x) for d in (3, 2, 1)]
        stats = []
        if with_stats:
            stat[i + 1, 0] = pack_rows(new.astype(F32), y * rows)
            stats = [remote(stat.at[i + 1, 0], stat.at[i + 1, dy * n_x + dx], (y + dy) % n_y, (x + dx) % n_x)
                     for dy in (3, 2, 1, 0) for dx in range(n_x) if dy or dx]
        for copy in gathers + stats:
            copy.wait_recv()

    pending_qkv = load_qkv(0)
    barrier = pltpu.get_barrier_semaphore()
    for dy in range(n_y):
        for dx in range(n_x):
            if dy or dx:
                pl.semaphore_signal(barrier, inc=1, device_id={"y": (y + dy) % n_y, "x": (x + dx) % n_x}, device_id_type=MESH)
    own = jnp.zeros((1, HEAD_DIM), F32)
    for b in range(n_y):
        own = own + pack_rows(hid_ref[b].astype(F32), b * rows)
    stat[0, 0] = own
    pl.semaphore_wait(barrier, n_y * n_x - 1)
    first_stats = [remote(stat.at[0, 0], stat.at[0, d], y, (x + d) % n_x) for d in range(1, n_x)]
    pending_o = load_o(0)
    pending_cache = [load_cache(0)]
    pending_gu = [load_gate_up(0, j) for j in range(len(chunks))]
    pending_down = [load_down(0, j) for j in range(len(chunks))]
    pending_cache += [load_cache(layer) for layer in range(1, layers)]
    q_rows[...] = jnp.zeros_like(q_rows)
    for copy in first_stats:
        copy.wait_recv()

    n_seq = batch // n_x
    seq_i = lax.broadcasted_iota(jnp.int32, (n_seq, batch), 0)
    at_lane = lax.broadcasted_iota(jnp.int32, (n_seq, batch), 1)
    my_pos = jnp.sum(jnp.where(at_lane == seq_i + x * n_seq, pos_ref[...].astype(F32), 0.0), axis=1, keepdims=True)
    angles = my_pos * freq_ref[...]
    cos_tab = jnp.cos(angles)
    sin_tab = jnp.where(lax.broadcasted_iota(jnp.int32, (n_seq, HEAD_DIM), 1) < HEAD_DIM // 2, -1.0, 1.0) * jnp.sin(angles)
    my_slot = my_pos.astype(jnp.int32)
    slot_row = lax.broadcasted_iota(jnp.int32, (slots2, HEAD_DIM), 0)
    slot_id = slot_row // kv_heads
    head_id = slot_row % kv_heads
    score_col = lax.broadcasted_iota(jnp.int32, (16, slots2), 1)
    score_head = lax.broadcasted_iota(jnp.int32, (16, slots2), 0) // group

    residual = hid_ref
    for layer in range(layers):
        more = layer + 1 < layers
        a, m = 2 * layer, 2 * layer + 1
        normalise(residual, a, n_x if layer == 0 else n_y * n_x, ga_ref, layer)
        wait_all(pending_qkv)

        def qkv_tile(t, carry):
            cols = pl.ds(pl.multiple_of(t * TILE, TILE), TILE)
            part = jnp.dot(n_buf[...], wqkv[:, cols], preferred_element_type=F32).astype(BF16)
            qkv_part[layer, :, :, cols] = part.reshape(n_x, batch // n_x, TILE)
            return carry

        lax.fori_loop(0, cols_qkv // TILE, qkv_tile, 0)
        copies = [remote(qkv_part.at[layer, (x + d) % n_x], qkv_recv.at[layer, d], y, (x + d) % n_x) for d in (2, 3, 1)]
        if more:
            pending_qkv = load_qkv(layer + 1)
        total = qkv_part[layer, x].astype(F32)
        for copy in copies:
            copy.wait_recv()
        for d in range(1, n_x):
            total = total + qkv_recv[layer, d].astype(F32)
        proj = total.astype(BF16).astype(F32)

        def rotate(vals, gain):
            mean_sq = jnp.mean(vals * vals, axis=-1, keepdims=True)
            normed = vals * lax.rsqrt(mean_sq + NORM_EPS) * gain
            turned = normed * cos_tab + pltpu.roll(normed, HEAD_DIM // 2, 1) * sin_tab
            return turned.astype(BF16).astype(F32)

        q_gain = qg_ref[...].astype(F32)[layer:layer + 1]
        k_gain = kg_ref[...].astype(F32)[layer:layer + 1]
        for h in range(q_heads):
            q_rows[h * n_seq:(h + 1) * n_seq, :] = rotate(proj[:, h * HEAD_DIM:(h + 1) * HEAD_DIM], q_gain)
        k_new = [rotate(proj[:, q_cols + h * HEAD_DIM:q_cols + (h + 1) * HEAD_DIM], k_gain) for h in range(kv_heads)]
        v_new = [proj[:, q_cols + kv_cols + h * HEAD_DIM:q_cols + kv_cols + (h + 1) * HEAD_DIM] for h in range(kv_heads)]

        for h in range(kv_heads):
            new_out[layer, 0, h] = k_new[h]
            new_out[layer, 1, h] = v_new[h]

        wait_all(pending_cache[layer])
        for b in range(n_seq):
            pos = my_slot[b:b + 1]
            hit = slot_id == pos
            for buf, new in ((kbuf, k_new), (vbuf, v_new)):
                fresh = new[0][b:b + 1]
                for h in range(1, kv_heads):
                    fresh = jnp.where(head_id == h, new[h][b:b + 1], fresh)
                buf[layer, b] = jnp.where(hit, fresh, buf[layer, b].astype(F32)).astype(BF16)
            q_b = q_rows[pl.ds(b, 16, stride=n_seq), :].astype(BF16)
            scores = lax.dot_general(q_b, kbuf[layer, b], (((1,), (1,)), ((), ())), preferred_element_type=F32) * (HEAD_DIM ** -0.5)
            valid = (score_col // kv_heads <= pos) & (score_col % kv_heads == score_head)
            valid = valid | (score_head >= kv_heads)
            scores = jnp.where(valid, scores, -1e30)
            top = jnp.max(scores, axis=1, keepdims=True)
            e = jnp.exp(scores - top)
            probs = (e / jnp.sum(e, axis=1, keepdims=True)).astype(BF16)
            o_rows[b * 16:(b + 1) * 16, :] = jnp.dot(probs, vbuf[layer, b], preferred_element_type=F32)
        for h in range(q_heads):
            attn_all[layer, x, :, h * HEAD_DIM:(h + 1) * HEAD_DIM] = o_rows[pl.ds(h, n_seq, stride=16), :].astype(BF16)
        copies = [remote(attn_all.at[layer, x], attn_all.at[layer, x], y, (x + d) % n_x) for d in (2, 3, 1)]
        wait_all(pending_o)
        for copy in copies:
            copy.wait_recv()

        def o_tile(t, carry):
            cols = pl.ds(pl.multiple_of(t * TILE, TILE), TILE)
            part = jnp.dot(attn_all[layer].reshape(batch, q_cols), wo[:, cols], preferred_element_type=F32).astype(BF16)
            ar_part[a, :, :, cols] = part.reshape(n_y, rows, TILE)
            return carry

        lax.fori_loop(0, depth // TILE, o_tile, 0)
        if more:
            pending_o = load_o(layer + 1)
        all_reduce(a, residual, True)

        normalise(h_all.at[a], a + 1, n_y * n_x, gm_ref, layer)
        to_pair, to_across, own_gather, across_gather, forward = {}, {}, {}, {}, {}

        def project(j):
            wait_all(pending_gu[j])
            start, width = chunks[j]

            def tile(t, carry):
                cols = pl.ds(pl.multiple_of(start + t * TILE, TILE), TILE)
                gate = jnp.dot(n_buf[...], wg[:, cols], preferred_element_type=F32).astype(BF16)
                up = jnp.dot(n_buf[...], wu[:, cols], preferred_element_type=F32).astype(BF16)
                gu_part[layer, 0, :, :, :, cols] = gate.reshape(2, 2, rows, TILE)
                gu_part[layer, 1, :, :, :, cols] = up.reshape(2, 2, rows, TILE)
                return carry

            lax.fori_loop(0, width // TILE, tile, 0)
            cols = pl.ds(start, width)
            to_pair[j] = remote(gu_part.at[layer, :, :, 1 - core, :, cols], gu_pair.at[layer, :, :, :, cols], y, partner)
            if more:
                pending_gu[j] = load_gate_up(layer + 1, j)

        def cross(j):
            cols = pl.ds(*chunks[j])
            to_pair[j].wait_recv()
            pair = gu_part[layer, :, 1 - chip, core, :, cols].astype(F32) + gu_pair[layer, :, 1 - chip, :, cols].astype(F32)
            gu_send[layer, :, :, cols] = pair.astype(BF16)
            to_across[j] = remote(gu_send.at[layer, :, :, cols], gu_recv.at[layer, :, :, cols], y, across)

        def activate(j):
            cols = pl.ds(*chunks[j])
            to_across[j].wait_recv()
            gate_up = (gu_part[layer, :, chip, core, :, cols].astype(F32) + gu_pair[layer, :, chip, :, cols].astype(F32)
                       + gu_recv[layer, :, :, cols].astype(F32)).astype(BF16).astype(F32)
            act_all[layer, x, :, cols] = (jax.nn.silu(gate_up[0]) * gate_up[1]).astype(BF16)
            mine = act_all.at[layer, x, :, cols]
            across_gather[j] = remote(mine, mine, y, across)
            own_gather[j] = remote(mine, mine, y, partner)

        def pass_on(j):
            cols = pl.ds(*chunks[j])
            across_gather[j].wait_recv()
            theirs = act_all.at[layer, across, :, cols]
            forward[j] = remote(theirs, theirs, y, partner)

        def down(j):
            own_gather[j].wait_recv()
            forward[j].wait_recv()
            wait_all(pending_down[j])
            start, width = chunks[j]

            def tile(t, carry):
                cols = pl.ds(pl.multiple_of(t * TILE, TILE), TILE)
                vals = act_all[layer, :, :, pl.ds(start, width)].reshape(batch, width)
                part = jnp.dot(vals, wd[pl.ds(start, width), cols], preferred_element_type=F32)
                if j:
                    part = part + acc[:, cols]
                if j < len(chunks) - 1:
                    acc[:, cols] = part
                else:
                    ar_part[m, :, :, cols] = part.astype(BF16).reshape(n_y, rows, TILE)
                return carry

            lax.fori_loop(0, depth // TILE, tile, 0)
            if more:
                pending_down[j] = load_down(layer + 1, j)

        phases = (project, cross, activate, pass_on, down)
        for stage in range(len(chunks) + len(phases) - 1):
            for lag, phase in enumerate(phases):
                if 0 <= stage - lag < len(chunks):
                    phase(stage - lag)
        all_reduce(m, h_all.at[a], more)
        residual = h_all.at[m]

    hid_out[...] = residual[...]
    for copy in sent:
        copy.wait_send()


def cache_kernel(dims, hid_ref, new_ref, pos_ref, kc_ref, vc_ref, hid_out, kc_out, vc_out, hid_buf, kbuf, vbuf, in_sem, out_sem):
    layers, n_seq, kv_heads = dims
    first = lax.axis_index("x") * n_seq
    arrive, leave = [], []
    for layer in range(layers):
        for src, dst in ((kc_ref, kbuf), (vc_ref, vbuf)):
            arrive.append(pltpu.make_async_copy(src.at[layer], dst.at[layer], in_sem.at[len(arrive)]))
            arrive[-1].start()
    hidden_in = pltpu.make_async_copy(hid_ref, hid_buf, in_sem.at[len(arrive)])
    hidden_in.start()
    for layer in range(layers):
        for i, (buf, dst) in enumerate(((kbuf, kc_out), (vbuf, vc_out))):
            arrive[2 * layer + i].wait()
            for b in range(n_seq):
                rows = jnp.concatenate([new_ref[layer, i, h, b:b + 1, :] for h in range(kv_heads)], axis=0)
                buf[layer, b, pos_ref[0, first + b]] = rows.astype(BF16)
            leave.append(pltpu.make_async_copy(buf.at[layer], dst.at[layer], out_sem.at[len(leave)]))
            leave[-1].start()
    hidden_in.wait()
    leave.append(pltpu.make_async_copy(hid_buf, hid_out, out_sem.at[len(leave)]))
    leave[-1].start()
    for copy in leave:
        copy.wait()


def solution(mesh):
    n_x, n_y = mesh.shape['x'], mesh.shape['y']
    cache_spec = P(None, ('dp', 'x'), None, 'y', None)
    col_spec = P(None, 'x', 'y')
    row_spec = P(None, 'y', 'x')
    in_specs = (P('dp', 'x'), P('dp'), cache_spec, cache_spec, P(None, 'x'), P(None, 'x'), P(), P(), col_spec, col_spec, col_spec, row_spec, col_spec, col_spec, row_spec)
    out_specs = (P('dp', 'x'), cache_spec, cache_spec)

    def device_step(hidden, positions, k_cache, v_cache, g_attn, g_mlp, q_gain, k_gain, w_q, w_k, w_v, w_o, w_gate, w_up, w_down):
        batch, depth = hidden.shape
        layers, n_seq, slots, kv_heads, _ = k_cache.shape
        q_cols, kv_cols, ffn = w_q.shape[2], w_k.shape[2], w_gate.shape[2]
        rows = batch // n_y
        slots2 = slots * kv_heads
        dims = (layers, n_y, n_x, rows, depth, q_cols, kv_cols, ffn)
        cols_qkv = q_cols + 2 * kv_cols
        vmem = pl.BlockSpec(memory_space=pltpu.VMEM)
        hbm = pl.BlockSpec(memory_space=pl.ANY)
        cache_shape = (layers, n_seq, slots2, HEAD_DIM)
        norms = 2 * layers
        positions = positions.reshape(1, batch)
        new_hidden, new_rows = pl.pallas_call(
            functools.partial(step_kernel, dims),
            out_shape=(jax.ShapeDtypeStruct((n_y, rows, depth), BF16), jax.ShapeDtypeStruct((layers, 2, kv_heads, n_seq, HEAD_DIM), F32)),
            in_specs=[vmem] * 7 + [hbm] * 9,
            out_specs=(vmem, vmem),
            scratch_shapes=[
                pltpu.VMEM((depth, cols_qkv), BF16),
                pltpu.VMEM((q_cols, depth), BF16),
                pltpu.VMEM((depth, ffn), BF16),
                pltpu.VMEM((depth, ffn), BF16),
                pltpu.VMEM((ffn, depth), BF16),
                pltpu.VMEM(cache_shape, BF16),
                pltpu.VMEM(cache_shape, BF16),
                pltpu.VMEM((batch, depth), BF16),
                pltpu.VMEM((norms, n_y * n_x, 1, HEAD_DIM), F32),
                pltpu.VMEM((layers, n_x, n_seq, cols_qkv), BF16),
                pltpu.VMEM((layers, n_x, n_seq, cols_qkv), BF16),
                pltpu.VMEM((16 * n_seq, HEAD_DIM), F32),
                pltpu.VMEM((16 * n_seq, HEAD_DIM), F32),
                pltpu.VMEM((layers, n_x, n_seq, q_cols), BF16),
                pltpu.VMEM((norms, n_y, rows, depth), BF16),
                pltpu.VMEM((norms, n_y, rows, depth), BF16),
                pltpu.VMEM((norms, n_y, rows, depth), BF16),
                pltpu.VMEM((layers, 2, 2, 2, rows, ffn), BF16),
                pltpu.VMEM((layers, 2, 2, rows, ffn), BF16),
                pltpu.VMEM((layers, 2, rows, ffn), BF16),
                pltpu.VMEM((layers, 2, rows, ffn), BF16),
                pltpu.VMEM((layers, n_x, rows, ffn), BF16),
                pltpu.VMEM((batch, depth), F32),
                pltpu.SemaphoreType.DMA((N_REMOTE,)),
                pltpu.SemaphoreType.DMA((N_REMOTE,)),
                pltpu.SemaphoreType.DMA((N_LOCAL,)),
            ],
            compiler_params=pltpu.CompilerParams(collective_id=0, has_side_effects=True, vmem_limit_bytes=64 * 1024 * 1024 - 65536),
        )(hidden.reshape(n_y, rows, depth), positions, inverse_frequencies(), g_attn, g_mlp, q_gain, k_gain,
          k_cache.reshape(cache_shape), v_cache.reshape(cache_shape), w_q, w_k, w_v, w_o, w_gate, w_up, w_down)
        return pl.pallas_call(
            functools.partial(cache_kernel, (layers, n_seq, kv_heads)),
            out_shape=tuple(jax.ShapeDtypeStruct(a.shape, a.dtype) for a in (hidden, k_cache, v_cache)),
            in_specs=[hbm, vmem, pl.BlockSpec(memory_space=pltpu.SMEM), hbm, hbm],
            out_specs=(hbm, hbm, hbm),
            scratch_shapes=[
                pltpu.VMEM(hidden.shape, BF16),
                pltpu.VMEM(k_cache.shape, BF16),
                pltpu.VMEM(k_cache.shape, BF16),
                pltpu.SemaphoreType.DMA((2 * layers + 1,)),
                pltpu.SemaphoreType.DMA((2 * layers + 1,)),
            ],
            compiler_params=pltpu.CompilerParams(vmem_limit_bytes=64 * 1024 * 1024 - 65536),
        )(new_hidden.reshape(batch, depth), new_rows, positions, k_cache, v_cache)

    return jax.shard_map(device_step, mesh=mesh, in_specs=in_specs, out_specs=out_specs, check_vma=False)
```

```python
import functools

import jax
import jax.numpy as jnp
import numpy as np
from jax import lax
from jax.experimental import pallas as pl
from jax.experimental.pallas import tpu as pltpu
from jax.sharding import PartitionSpec as P

HEAD_DIM = 128
NORM_EPS = 1e-6
ROPE_BASE = 1000000.0
TILE = 256
CHUNK_TILES = (2, 3, 4, 4, 2, 2)
DIRECT = 2
MESH = pl.DeviceIdType.MESH
F32 = jnp.float32
BF16 = jnp.bfloat16
N_REMOTE = 280
N_LOCAL = 72


def inverse_frequencies():
    half_dim = HEAD_DIM // 2
    freqs = np.power(np.float32(ROPE_BASE), (-2.0 * np.arange(half_dim) / HEAD_DIM).astype(np.float32))
    return np.concatenate([freqs, freqs])[None].astype(np.float32)


def split_tiles(n_tiles):
    share = n_tiles / sum(CHUNK_TILES)
    edges = [round(share * sum(CHUNK_TILES[:i])) for i in range(len(CHUNK_TILES) + 1)]
    return [(a * TILE, (b - a) * TILE) for a, b in zip(edges, edges[1:]) if b > a]


def step_kernel(dims, *refs):
    (layers, n_y, n_x, rows, depth, q_cols, kv_cols, ffn) = dims
    (hid_any, pos_any, freq_any, ga_any, gm_any, qg_any, kg_any, kc_ref, vc_ref,
     wq_ref, wk_ref, wv_ref, wo_ref, wg_ref, wu_ref, wd_ref,
     hid_out, new_out,
     wqkv, wo, wg, wu, wd, kbuf, vbuf, n_buf, stat, qkv_part, qkv_recv, q_rows, o_rows, attn_all,
     ar_part, ar_recv, h_all, gu_part, gu_pair, gu_send, gu_recv, act_all, acc,
     hid_ref, pos_ref, freq_ref, ga_ref, gm_ref, qg_ref, kg_ref,
     send_sem, recv_sem, local_sem) = refs
    batch = n_y * rows
    cols_qkv = q_cols + 2 * kv_cols
    q_heads = q_cols // HEAD_DIM
    kv_heads = kv_cols // HEAD_DIM
    group = q_heads // kv_heads
    chunks = split_tiles(ffn // TILE)
    model_dim = depth * n_x
    slots2 = kbuf.shape[2]

    y = lax.axis_index("y")
    x = lax.axis_index("x")
    chip = x // 2
    core = x % 2
    partner = 2 * chip + (1 - core)
    across = 2 * (1 - chip) + core
    diagonal = 2 * (1 - chip) + (1 - core)

    counter = {"remote": 0, "local": 0}
    sent = []

    def remote(src, dst, to_y, to_x):
        i = counter["remote"]
        counter["remote"] += 1
        copy = pltpu.make_async_remote_copy(
            src_ref=src, dst_ref=dst, send_sem=send_sem.at[i], recv_sem=recv_sem.at[i],
            device_id={"y": to_y, "x": to_x}, device_id_type=MESH)
        copy.start()
        sent.append(copy)
        return copy

    def local(src, dst):
        i = counter["local"]
        counter["local"] += 1
        copy = pltpu.make_async_copy(src, dst, local_sem.at[i])
        copy.start()
        return copy

    def load_qkv(layer):
        return [local(wq_ref.at[layer], wqkv.at[:, 0:q_cols]),
                local(wk_ref.at[layer], wqkv.at[:, q_cols:q_cols + kv_cols]),
                local(wv_ref.at[layer], wqkv.at[:, q_cols + kv_cols:cols_qkv])]

    def load_o(layer):
        return [local(wo_ref.at[layer], wo)]

    def load_gate_up(layer, j):
        cols = pl.ds(chunks[j][0], chunks[j][1])
        return [local(wg_ref.at[layer, :, cols], wg.at[:, cols]),
                local(wu_ref.at[layer, :, cols], wu.at[:, cols])]

    def load_down(layer, j):
        cols = pl.ds(chunks[j][0], chunks[j][1])
        return [local(wd_ref.at[layer, cols, :], wd.at[cols, :])]

    def load_cache(layer):
        return [local(kc_ref.at[layer], kbuf.at[layer]), local(vc_ref.at[layer], vbuf.at[layer])]

    def wait_all(copies):
        for copy in copies:
            copy.wait()

    row_i = lax.broadcasted_iota(jnp.int32, (rows, HEAD_DIM), 0)
    lane_i = lax.broadcasted_iota(jnp.int32, (rows, HEAD_DIM), 1)

    def pack_rows(squares, first_row):
        sums = jnp.sum(squares, axis=1, keepdims=True)
        return jnp.sum(jnp.where(lane_i == row_i + first_row, sums, 0.0), axis=0, keepdims=True)

    all_row = lax.broadcasted_iota(jnp.int32, (batch, HEAD_DIM), 0)
    all_lane = lax.broadcasted_iota(jnp.int32, (batch, HEAD_DIM), 1)

    def row_scales(i, count):
        total = stat[i, 0]
        for s in range(1, count):
            total = total + stat[i, s]
        scale = lax.rsqrt(total / model_dim + NORM_EPS)
        return jnp.sum(jnp.where(all_lane == all_row, scale, 0.0), axis=1, keepdims=True)

    def normalise(hidden_ref, i, count, gain_ref, layer):
        scales = row_scales(i, count)
        gain = gain_ref[...].astype(F32)[layer:layer + 1]
        vals = hidden_ref[...].reshape(batch, depth).astype(F32)
        n_buf[...] = (vals * scales * gain).astype(BF16)

    def all_reduce(i, tile_product, residual_ref, with_stats):
        n_tiles = depth // TILE
        scatters, gathers, stats = [], [], []
        for t in range(n_tiles):
            cols = pl.ds(t * TILE, TILE)
            ar_part[i, :, :, cols] = tile_product(cols).astype(BF16).reshape(n_y, rows, TILE)
            scatters.append([remote(ar_part.at[i, (y + d) % n_y, :, cols], ar_recv.at[i, d, :, cols], (y + d) % n_y, x) for d in (2, 3, 1)])
        squares = jnp.zeros((rows, TILE), F32)
        for t in range(n_tiles):
            cols = pl.ds(t * TILE, TILE)
            for copy in scatters[t]:
                copy.wait_recv()
            total = ar_part[i, y, :, cols].astype(F32)
            for d in range(1, n_y):
                total = total + ar_recv[i, d, :, cols].astype(F32)
            new = (residual_ref[y, :, cols].astype(F32) + total.astype(BF16).astype(F32)).astype(BF16)
            h_all[i, y, :, cols] = new
            gathers += [remote(h_all.at[i, y, :, cols], h_all.at[i, y, :, cols], (y + d) % n_y, x) for d in (2, 3, 1)]
            squares = squares + new.astype(F32) * new.astype(F32)
        if with_stats:
            stat[i + 1, 0] = pack_rows(squares, y * rows)
            stats = [remote(stat.at[i + 1, 0], stat.at[i + 1, dy * n_x + dx], (y + dy) % n_y, (x + dx) % n_x)
                     for dy in (2, 3, 1, 0) for dx in range(n_x) if dy or dx]
        for copy in gathers + stats:
            copy.wait_recv()

    barrier = pltpu.get_barrier_semaphore()
    for dy in range(n_y):
        for dx in range(n_x):
            if dy or dx:
                pl.semaphore_signal(barrier, inc=1, device_id={"y": (y + dy) % n_y, "x": (x + dx) % n_x}, device_id_type=MESH)
    small = [local(src, dst) for src, dst in ((hid_any, hid_ref), (ga_any, ga_ref), (gm_any, gm_ref), (qg_any, qg_ref), (kg_any, kg_ref),
                                              (pos_any, pos_ref), (freq_any, freq_ref))]
    pending_qkv = load_qkv(0)
    wait_all(small)
    pending_o = load_o(0)
    pending_cache = [load_cache(0)]
    pending_gu = [load_gate_up(0, j) for j in range(len(chunks))]
    pending_down = [load_down(0, j) for j in range(len(chunks))]
    pending_cache += [load_cache(layer) for layer in range(1, layers)]
    gain = ga_ref[...].astype(F32)[0:1]
    own = jnp.zeros((1, HEAD_DIM), F32)
    for b in range(n_y):
        vals = hid_ref[b].astype(F32)
        own = own + pack_rows(vals * vals, b * rows)
        sums = jnp.sum(vals * vals, axis=1, keepdims=True)
        n_buf[b * rows:(b + 1) * rows, :] = (vals * lax.rsqrt(sums / depth + NORM_EPS) * gain).astype(BF16)
    stat[0, 0] = own
    q_rows[...] = jnp.zeros_like(q_rows)
    n_seq = batch // n_x
    seq_i = lax.broadcasted_iota(jnp.int32, (n_seq, batch), 0)
    at_lane = lax.broadcasted_iota(jnp.int32, (n_seq, batch), 1)
    my_pos = jnp.sum(jnp.where(at_lane == seq_i + x * n_seq, pos_ref[...].astype(F32), 0.0), axis=1, keepdims=True)
    angles = my_pos * freq_ref[...]
    cos_tab = jnp.cos(angles)
    sin_tab = jnp.where(lax.broadcasted_iota(jnp.int32, (n_seq, HEAD_DIM), 1) < HEAD_DIM // 2, -1.0, 1.0) * jnp.sin(angles)
    my_slot = my_pos.astype(jnp.int32)
    slot_row = lax.broadcasted_iota(jnp.int32, (slots2, HEAD_DIM), 0)
    slot_id = slot_row // kv_heads
    head_id = slot_row % kv_heads
    score_col = lax.broadcasted_iota(jnp.int32, (16, slots2), 1)
    score_head = lax.broadcasted_iota(jnp.int32, (16, slots2), 0) // group

    residual = hid_ref
    for layer in range(layers):
        more = layer + 1 < layers
        a, m = 2 * layer, 2 * layer + 1
        if layer:
            normalise(residual, a, n_y * n_x, ga_ref, layer)
        wait_all(pending_qkv)

        def qkv_tiles(first, last):
            def tile(t, carry):
                cols = pl.ds(pl.multiple_of(t * TILE, TILE), TILE)
                part = jnp.dot(n_buf[...], wqkv[:, cols], preferred_element_type=F32).astype(BF16)
                qkv_part[layer, :, :, cols] = part.reshape(n_x, batch // n_x, TILE)
                return carry

            lax.fori_loop(first, last, tile, 0)

        def qkv_send(first, last):
            cols = pl.ds(first * TILE, (last - first) * TILE)
            return [remote(qkv_part.at[layer, (x + d) % n_x, :, cols], qkv_recv.at[layer, d, :, cols], y, (x + d) % n_x) for d in (2, 3, 1)]

        n_tiles = cols_qkv // TILE
        copies = []
        if layer:
            for first, last in ((0, n_tiles // 2), (n_tiles // 2, n_tiles)):
                qkv_tiles(first, last)
                copies += qkv_send(first, last)
        else:
            qkv_tiles(0, n_tiles)
            pl.semaphore_wait(barrier, n_y * n_x - 1)
            copies += [remote(stat.at[0, 0], stat.at[0, d], y, (x + d) % n_x) for d in (2, 3, 1)]
            copies += qkv_send(0, n_tiles)
        if more:
            pending_qkv = load_qkv(layer + 1)
        for copy in copies:
            copy.wait_recv()
        parts = [qkv_part[layer, x].astype(F32)] + [qkv_recv[layer, d].astype(F32) for d in range(1, n_x)]
        if not layer:
            seq_lane = lax.broadcasted_iota(jnp.int32, (n_seq, HEAD_DIM), 1)
            seq_row = lax.broadcasted_iota(jnp.int32, (n_seq, HEAD_DIM), 0) + x * n_seq
            sums = [jnp.sum(jnp.where(seq_lane == seq_row, stat[0, d], 0.0), axis=1, keepdims=True) for d in range(n_x)]
            scale = lax.rsqrt(sum(sums) / model_dim + NORM_EPS)
            parts = [part * jnp.where(scale > 0.0, scale / lax.rsqrt(own_sum / depth + NORM_EPS), 0.0) for part, own_sum in zip(parts, sums)]
        total = parts[0]
        for part in parts[1:]:
            total = total + part
        proj = total.astype(BF16).astype(F32)

        def rotate(vals, gain):
            mean_sq = jnp.mean(vals * vals, axis=-1, keepdims=True)
            normed = vals * lax.rsqrt(mean_sq + NORM_EPS) * gain
            turned = normed * cos_tab + pltpu.roll(normed, HEAD_DIM // 2, 1) * sin_tab
            return turned.astype(BF16).astype(F32)

        q_gain = qg_ref[...].astype(F32)[layer:layer + 1]
        k_gain = kg_ref[...].astype(F32)[layer:layer + 1]
        for h in range(q_heads):
            q_rows[h * n_seq:(h + 1) * n_seq, :] = rotate(proj[:, h * HEAD_DIM:(h + 1) * HEAD_DIM], q_gain)
        k_new = [rotate(proj[:, q_cols + h * HEAD_DIM:q_cols + (h + 1) * HEAD_DIM], k_gain) for h in range(kv_heads)]
        v_new = [proj[:, q_cols + kv_cols + h * HEAD_DIM:q_cols + kv_cols + (h + 1) * HEAD_DIM] for h in range(kv_heads)]

        for h in range(kv_heads):
            new_out[layer, 0, h] = k_new[h]
            new_out[layer, 1, h] = v_new[h]

        wait_all(pending_cache[layer])
        for b in range(n_seq):
            pos = my_slot[b:b + 1]
            hit = slot_id == pos
            for buf, new in ((kbuf, k_new), (vbuf, v_new)):
                fresh = new[0][b:b + 1]
                for h in range(1, kv_heads):
                    fresh = jnp.where(head_id == h, new[h][b:b + 1], fresh)
                buf[layer, b] = jnp.where(hit, fresh, buf[layer, b].astype(F32)).astype(BF16)
            q_b = q_rows[pl.ds(b, 16, stride=n_seq), :].astype(BF16)
            scores = lax.dot_general(q_b, kbuf[layer, b], (((1,), (1,)), ((), ())), preferred_element_type=F32) * (HEAD_DIM ** -0.5)
            valid = (score_col // kv_heads <= pos) & (score_col % kv_heads == score_head)
            valid = valid | (score_head >= kv_heads)
            scores = jnp.where(valid, scores, -1e30)
            top = jnp.max(scores, axis=1, keepdims=True)
            e = jnp.exp(scores - top)
            probs = (e / jnp.sum(e, axis=1, keepdims=True)).astype(BF16)
            o_rows[b * 16:(b + 1) * 16, :] = jnp.dot(probs, vbuf[layer, b], preferred_element_type=F32)
        for h in range(q_heads):
            attn_all[layer, x, :, h * HEAD_DIM:(h + 1) * HEAD_DIM] = o_rows[pl.ds(h, n_seq, stride=16), :].astype(BF16)
        copies = [remote(attn_all.at[layer, x], attn_all.at[layer, x], y, (x + d) % n_x) for d in (2, 3, 1)]
        wait_all(pending_o)
        for copy in copies:
            copy.wait_recv()

        def o_product(cols):
            return jnp.dot(attn_all[layer].reshape(batch, q_cols), wo[:, cols], preferred_element_type=F32)

        all_reduce(a, o_product, residual, True)
        if more:
            pending_o = load_o(layer + 1)

        normalise(h_all.at[a], a + 1, n_y * n_x, gm_ref, layer)
        to_pair, to_across, own_gather, across_gather, last_gather = {}, {}, {}, {}, {}

        def project(j):
            wait_all(pending_gu[j])
            start, width = chunks[j]

            def tile(t, carry):
                cols = pl.ds(pl.multiple_of(start + t * TILE, TILE), TILE)
                gate = jnp.dot(n_buf[...], wg[:, cols], preferred_element_type=F32).astype(BF16)
                up = jnp.dot(n_buf[...], wu[:, cols], preferred_element_type=F32).astype(BF16)
                gu_part[layer, 0, :, :, :, cols] = gate.reshape(2, 2, rows, TILE)
                gu_part[layer, 1, :, :, :, cols] = up.reshape(2, 2, rows, TILE)
                return carry

            lax.fori_loop(0, width // TILE, tile, 0)
            cols = pl.ds(start, width)
            to_pair[j] = remote(gu_part.at[layer, :, :, 1 - core, :, cols], gu_pair.at[layer, :, :, :, cols], y, partner)
            if more:
                pending_gu[j] = load_gate_up(layer + 1, j)

        def cross(j):
            cols = pl.ds(*chunks[j])
            to_pair[j].wait_recv()
            pair = gu_part[layer, :, 1 - chip, core, :, cols].astype(F32) + gu_pair[layer, :, 1 - chip, :, cols].astype(F32)
            gu_send[layer, :, :, cols] = pair.astype(BF16)
            to_across[j] = remote(gu_send.at[layer, :, :, cols], gu_recv.at[layer, :, :, cols], y, across)

        def activate(j):
            cols = pl.ds(*chunks[j])
            to_across[j].wait_recv()
            gate_up = (gu_part[layer, :, chip, core, :, cols].astype(F32) + gu_pair[layer, :, chip, :, cols].astype(F32)
                       + gu_recv[layer, :, :, cols].astype(F32)).astype(BF16).astype(F32)
            act_all[layer, x, :, cols] = (jax.nn.silu(gate_up[0]) * gate_up[1]).astype(BF16)
            mine = act_all.at[layer, x, :, cols]
            across_gather[j] = remote(mine, mine, y, across)
            if j >= len(chunks) - DIRECT:
                last_gather[j] = remote(mine, mine, y, diagonal)
            own_gather[j] = remote(mine, mine, y, partner)

        def pass_on(j):
            cols = pl.ds(*chunks[j])
            across_gather[j].wait_recv()
            if j < len(chunks) - DIRECT:
                theirs = act_all.at[layer, across, :, cols]
                last_gather[j] = remote(theirs, theirs, y, partner)

        def down_product(j, cols):
            start, width = chunks[j]
            vals = act_all[layer, :, :, pl.ds(start, width)].reshape(batch, width)
            part = jnp.dot(vals, wd[pl.ds(start, width), cols], preferred_element_type=F32)
            return part + acc[:, cols] if j else part

        def arrived(j):
            own_gather[j].wait_recv()
            last_gather[j].wait_recv()
            wait_all(pending_down[j])

        def down(j):
            arrived(j)

            def tile(t, carry):
                cols = pl.ds(pl.multiple_of(t * TILE, TILE), TILE)
                acc[:, cols] = down_product(j, cols)
                return carry

            lax.fori_loop(0, depth // TILE, tile, 0)
            if more:
                pending_down[j] = load_down(layer + 1, j)

        last = len(chunks) - 1
        for j in range(last + 1):
            project(j)
            if j >= 2:
                cross(j - 2)
        for j in range(max(last - 1, 0), last + 1):
            cross(j)
        for j in range(last + 4):
            if j <= last:
                activate(j)
            if 0 <= j - 2 <= last:
                pass_on(j - 2)
            if 0 <= j - 3 < last:
                down(j - 3)
        arrived(last)
        all_reduce(m, functools.partial(down_product, last), h_all.at[a], more)
        if more:
            pending_down[last] = load_down(layer + 1, last)
        residual = h_all.at[m]

    hid_out[...] = residual[...]
    for copy in sent:
        copy.wait_send()


def cache_kernel(dims, hid_ref, new_ref, pos_ref, kc_ref, vc_ref, hid_out, kc_out, vc_out, hid_buf, kbuf, vbuf, in_sem, out_sem):
    layers, n_seq, kv_heads = dims
    first = lax.axis_index("x") * n_seq
    arrive, leave = [], []
    for layer in range(layers):
        for src, dst in ((kc_ref, kbuf), (vc_ref, vbuf)):
            arrive.append(pltpu.make_async_copy(src.at[layer], dst.at[layer], in_sem.at[len(arrive)]))
            arrive[-1].start()
    hidden_in = pltpu.make_async_copy(hid_ref, hid_buf, in_sem.at[len(arrive)])
    hidden_in.start()
    for layer in range(layers):
        for i, (buf, dst) in enumerate(((kbuf, kc_out), (vbuf, vc_out))):
            arrive[2 * layer + i].wait()
            for b in range(n_seq):
                rows = jnp.concatenate([new_ref[layer, i, h, b:b + 1, :] for h in range(kv_heads)], axis=0)
                buf[layer, b, pos_ref[0, first + b]] = rows.astype(BF16)
            leave.append(pltpu.make_async_copy(buf.at[layer], dst.at[layer], out_sem.at[len(leave)]))
            leave[-1].start()
    hidden_in.wait()
    leave.append(pltpu.make_async_copy(hid_buf, hid_out, out_sem.at[len(leave)]))
    leave[-1].start()
    for copy in leave:
        copy.wait()


def solution(mesh):
    n_x, n_y = mesh.shape['x'], mesh.shape['y']
    cache_spec = P(None, ('dp', 'x'), None, 'y', None)
    col_spec = P(None, 'x', 'y')
    row_spec = P(None, 'y', 'x')
    in_specs = (P('dp', 'x'), P('dp'), cache_spec, cache_spec, P(None, 'x'), P(None, 'x'), P(), P(), col_spec, col_spec, col_spec, row_spec, col_spec, col_spec, row_spec)
    out_specs = (P('dp', 'x'), cache_spec, cache_spec)

    def device_step(hidden, positions, k_cache, v_cache, g_attn, g_mlp, q_gain, k_gain, w_q, w_k, w_v, w_o, w_gate, w_up, w_down):
        batch, depth = hidden.shape
        layers, n_seq, slots, kv_heads, _ = k_cache.shape
        q_cols, kv_cols, ffn = w_q.shape[2], w_k.shape[2], w_gate.shape[2]
        rows = batch // n_y
        slots2 = slots * kv_heads
        dims = (layers, n_y, n_x, rows, depth, q_cols, kv_cols, ffn)
        cols_qkv = q_cols + 2 * kv_cols
        vmem = pl.BlockSpec(memory_space=pltpu.VMEM)
        hbm = pl.BlockSpec(memory_space=pl.ANY)
        cache_shape = (layers, n_seq, slots2, HEAD_DIM)
        norms = 2 * layers
        positions = positions.reshape(1, batch)
        new_hidden, new_rows = pl.pallas_call(
            functools.partial(step_kernel, dims),
            out_shape=(jax.ShapeDtypeStruct((n_y, rows, depth), BF16), jax.ShapeDtypeStruct((layers, 2, kv_heads, n_seq, HEAD_DIM), F32)),
            in_specs=[hbm] * 16,
            out_specs=(vmem, vmem),
            scratch_shapes=[
                pltpu.VMEM((depth, cols_qkv), BF16),
                pltpu.VMEM((q_cols, depth), BF16),
                pltpu.VMEM((depth, ffn), BF16),
                pltpu.VMEM((depth, ffn), BF16),
                pltpu.VMEM((ffn, depth), BF16),
                pltpu.VMEM(cache_shape, BF16),
                pltpu.VMEM(cache_shape, BF16),
                pltpu.VMEM((batch, depth), BF16),
                pltpu.VMEM((norms, n_y * n_x, 1, HEAD_DIM), F32),
                pltpu.VMEM((layers, n_x, n_seq, cols_qkv), BF16),
                pltpu.VMEM((layers, n_x, n_seq, cols_qkv), BF16),
                pltpu.VMEM((16 * n_seq, HEAD_DIM), F32),
                pltpu.VMEM((16 * n_seq, HEAD_DIM), F32),
                pltpu.VMEM((layers, n_x, n_seq, q_cols), BF16),
                pltpu.VMEM((norms, n_y, rows, depth), BF16),
                pltpu.VMEM((norms, n_y, rows, depth), BF16),
                pltpu.VMEM((norms, n_y, rows, depth), BF16),
                pltpu.VMEM((layers, 2, 2, 2, rows, ffn), BF16),
                pltpu.VMEM((layers, 2, 2, rows, ffn), BF16),
                pltpu.VMEM((layers, 2, rows, ffn), BF16),
                pltpu.VMEM((layers, 2, rows, ffn), BF16),
                pltpu.VMEM((layers, n_x, rows, ffn), BF16),
                pltpu.VMEM((batch, depth), F32),
                pltpu.VMEM((n_y, rows, depth), BF16),
                pltpu.VMEM((1, batch), jnp.int32),
                pltpu.VMEM((1, HEAD_DIM), F32),
                pltpu.VMEM(g_attn.shape, BF16),
                pltpu.VMEM(g_mlp.shape, BF16),
                pltpu.VMEM(q_gain.shape, BF16),
                pltpu.VMEM(k_gain.shape, BF16),
                pltpu.SemaphoreType.DMA((N_REMOTE,)),
                pltpu.SemaphoreType.DMA((N_REMOTE,)),
                pltpu.SemaphoreType.DMA((N_LOCAL,)),
            ],
            compiler_params=pltpu.CompilerParams(collective_id=0, has_side_effects=True, vmem_limit_bytes=64 * 1024 * 1024 - 65536),
        )(hidden.reshape(n_y, rows, depth), positions, inverse_frequencies(), g_attn, g_mlp, q_gain, k_gain,
          k_cache.reshape(cache_shape), v_cache.reshape(cache_shape), w_q, w_k, w_v, w_o, w_gate, w_up, w_down)
        return pl.pallas_call(
            functools.partial(cache_kernel, (layers, n_seq, kv_heads)),
            out_shape=tuple(jax.ShapeDtypeStruct(a.shape, a.dtype) for a in (hidden, k_cache, v_cache)),
            in_specs=[hbm, vmem, pl.BlockSpec(memory_space=pltpu.SMEM), hbm, hbm],
            out_specs=(hbm, hbm, hbm),
            scratch_shapes=[
                pltpu.VMEM(hidden.shape, BF16),
                pltpu.VMEM(k_cache.shape, BF16),
                pltpu.VMEM(k_cache.shape, BF16),
                pltpu.SemaphoreType.DMA((2 * layers + 1,)),
                pltpu.SemaphoreType.DMA((2 * layers + 1,)),
            ],
            compiler_params=pltpu.CompilerParams(vmem_limit_bytes=64 * 1024 * 1024 - 65536),
        )(new_hidden.reshape(batch, depth), new_rows, positions, k_cache, v_cache)

    return jax.shard_map(device_step, mesh=mesh, in_specs=in_specs, out_specs=out_specs, check_vma=False)
```

```python
import functools

import jax
import jax.numpy as jnp
import numpy as np
from jax import lax
from jax.experimental import pallas as pl
from jax.experimental.pallas import tpu as pltpu
from jax.sharding import PartitionSpec as P

HEAD_DIM = 128
NORM_EPS = 1e-6
ROPE_BASE = 1000000.0
TILE = 256
PAIR_LAG = 5
SEQS = 4
MESH = pl.DeviceIdType.MESH
F32 = jnp.float32
BF16 = jnp.bfloat16


def inverse_frequencies():
    half_dim = HEAD_DIM // 2
    freqs = np.power(np.float32(ROPE_BASE), (-2.0 * np.arange(half_dim) / HEAD_DIM).astype(np.float32))
    return np.concatenate([freqs, freqs])[None].astype(np.float32)


def step_kernel(dims, *refs):
    (layers, n_y, n_x, rows, depth, q_cols, kv_cols, ffn) = dims
    (hid_any, pos_any, freq_any, ga_any, gm_any, qg_any, kg_any, kc_ref, vc_ref,
     wq_ref, wk_ref, wv_ref, wo_ref, wg_ref, wu_ref, wd_ref,
     hid_out, new_out,
     wqkv, wo, wg, wu, wd, kbuf, vbuf, n_buf, stat, qkv_part, qkv_recv, q_rows, o_rows, attn_all,
     ar_part, ar_recv, h_mid, h_end, gu_part, gu_pair, gu_send, gu_recv, act_all, acc,
     pos_ref, freq_ref, ga_raw, gm_raw, qg_raw, kg_raw, ga_ref, gm_ref, qg_ref, kg_ref, slot_ref, part_scale, kv_rows,
     send_sem, recv_sem, local_sem) = refs
    batch = n_y * rows
    cols_qkv = q_cols + 2 * kv_cols
    q_heads = q_cols // HEAD_DIM
    kv_heads = kv_cols // HEAD_DIM
    group = q_heads // kv_heads
    model_dim = depth * n_x
    slots2 = kbuf.shape[2]
    n_seq = batch // n_x
    peers = n_y * n_x
    d_tiles, f_tiles, qkv_tiles = depth // TILE, ffn // TILE, cols_qkv // TILE

    y = lax.axis_index("y")
    x = lax.axis_index("x")
    chip = x // 2
    core = x % 2
    partner = 2 * chip + (1 - core)
    across = 2 * (1 - chip) + core
    diagonal = 2 * (1 - chip) + (1 - core)

    at_qkv, at_first, at_attn, at_mid = 0, n_x - 1, 2 * (n_x - 1), 3 * (n_x - 1)
    per_reduce = 2 * (n_y - 1) * d_tiles + peers - 1
    at_end = at_mid + per_reduce
    at_mlp = at_end + per_reduce

    def remote(src, dst, i, to_y, to_x):
        return pltpu.make_async_remote_copy(
            src_ref=src, dst_ref=dst, send_sem=send_sem.at[i], recv_sem=recv_sem.at[i],
            device_id={"y": to_y, "x": to_x}, device_id_type=MESH)

    def each(first, last, body):
        def step(i, carry):
            body(i)
            return carry

        lax.fori_loop(first, last, step, 0)

    def tile_cols(t):
        return pl.ds(pl.multiple_of(t * TILE, TILE), TILE)

    def qkv_loads(layer):
        return [pltpu.make_async_copy(wq_ref.at[layer], wqkv.at[:, 0:q_cols], local_sem.at[0]),
                pltpu.make_async_copy(wk_ref.at[layer], wqkv.at[:, q_cols:q_cols + kv_cols], local_sem.at[1]),
                pltpu.make_async_copy(wv_ref.at[layer], wqkv.at[:, q_cols + kv_cols:cols_qkv], local_sem.at[2])]

    def o_loads(layer):
        return [pltpu.make_async_copy(wo_ref.at[layer], wo, local_sem.at[3])]

    def gate_up_loads(layer):
        half = depth // 2
        return [pltpu.make_async_copy(src.at[layer, r * half:(r + 1) * half, :], dst.at[r * half:(r + 1) * half, :], local_sem.at[4 + 2 * i + r])
                for r in range(2) for i, (src, dst) in enumerate(((wg_ref, wg), (wu_ref, wu)))]

    def down_loads(layer):
        half = ffn // 2
        return [pltpu.make_async_copy(wd_ref.at[layer, r * half:(r + 1) * half, :], wd.at[r * half:(r + 1) * half, :], local_sem.at[8 + r]) for r in range(2)]

    def cache_loads(layer):
        return [pltpu.make_async_copy(src.at[layer], dst.at[layer], local_sem.at[10 + i * layers + layer])
                for i, (src, dst) in enumerate(((kc_ref, kbuf), (vc_ref, vbuf)))]

    def start(copies):
        for copy in copies:
            copy.start()

    def finish(copies):
        for copy in copies:
            copy.wait()

    row_i = lax.broadcasted_iota(jnp.int32, (rows, HEAD_DIM), 0)
    lane_i = lax.broadcasted_iota(jnp.int32, (rows, HEAD_DIM), 1)

    def along_lanes(column, first_row):
        return jnp.sum(jnp.where(lane_i == row_i + first_row, column, 0.0), axis=0, keepdims=True)

    def along_rows(lanes, first_row):
        return jnp.sum(jnp.where(lane_i == row_i + first_row, lanes, 0.0), axis=1, keepdims=True)

    def normalise(hidden_ref, i, gain_ref, layer):
        total = jnp.sum(stat[i], axis=0)
        scales = lax.rsqrt(total / model_dim + NORM_EPS)
        gain = gain_ref[layer]

        def block(b):
            n_buf[pl.ds(pl.multiple_of(b * rows, rows), rows), :] = (hidden_ref[b].astype(F32) * along_rows(scales, b * rows) * gain).astype(BF16)

        each(0, n_y, block)

    def all_reduce(i, base, tile_product, residual_ref, result_ref, with_stats):
        def scatter(t, d):
            cols = tile_cols(t)
            return remote(ar_part.at[i, (y + d) % n_y, :, cols], ar_recv.at[i, d, :, cols], base + t * (n_y - 1) + d - 1, (y + d) % n_y, x)

        def gather(t, d):
            mine = result_ref.at[y, :, tile_cols(t)]
            return remote(mine, mine, base + (d_tiles + t) * (n_y - 1) + d - 1, (y + d) % n_y, x)

        def share(e):
            return remote(stat.at[i + 1, 0], stat.at[i + 1, e], base + 2 * d_tiles * (n_y - 1) + e - 1, (y + e // n_x) % n_y, (x + e % n_x) % n_x)

        def send_tile(t):
            ar_part[i, :, :, tile_cols(t)] = tile_product(tile_cols(t)).astype(BF16).reshape(n_y, rows, TILE)
            for d in (2, 3, 1):
                scatter(t, d).start()

        each(0, d_tiles, send_tile)

        def sum_tile(t, squares):
            cols = tile_cols(t)
            for d in range(1, n_y):
                scatter(t, d).wait_recv()
            total = ar_part[i, y, :, cols].astype(F32)
            for d in range(1, n_y):
                total = total + ar_recv[i, d, :, cols].astype(F32)
            new = (residual_ref[y, :, cols].astype(F32) + total.astype(BF16).astype(F32)).astype(BF16)
            result_ref[y, :, cols] = new
            for d in (2, 3, 1):
                gather(t, d).start()
            return squares + new.astype(F32) * new.astype(F32)

        squares = lax.fori_loop(0, d_tiles, sum_tile, jnp.zeros((rows, TILE), F32))

        def statistics(act):
            @pl.when(with_stats)
            def _():
                each(1, peers, act)

        stat[i + 1, 0] = along_lanes(jnp.sum(squares, axis=1, keepdims=True), y * rows)
        statistics(lambda e: share(e).start())

        def settle(t):
            for d in range(1, n_y):
                gather(t, d).wait_recv()
                scatter(t, d).wait_send()

        each(0, d_tiles, settle)
        statistics(lambda e: share(e).wait_recv())

        def drain():
            def tile(t):
                for d in range(1, n_y):
                    gather(t, d).wait_send()

            each(0, d_tiles, tile)
            statistics(lambda e: share(e).wait_send())

        return drain

    def qkv_copy(d):
        return remote(qkv_part.at[(x + d) % n_x], qkv_recv.at[d], at_qkv + d - 1, y, (x + d) % n_x)

    def first_copy(d):
        return remote(stat.at[0, 0], stat.at[0, d], at_first + d - 1, y, (x + d) % n_x)

    def attn_copy(d):
        return remote(attn_all.at[x], attn_all.at[x], at_attn + d - 1, y, (x + d) % n_x)

    def pair_copy(t):
        cols = tile_cols(t)
        return remote(gu_part.at[:, :, 1 - core, :, cols], gu_pair.at[:, :, :, cols], at_mlp + t, y, partner)

    def across_copy(t):
        cols = tile_cols(t)
        return remote(gu_send.at[:, :, cols], gu_recv.at[:, :, cols], at_mlp + f_tiles + t, y, across)

    def act_copies(t):
        mine = act_all.at[x, :, tile_cols(t)]
        return [remote(mine, mine, at_mlp + (2 + i) * f_tiles + t, y, to_x) for i, to_x in enumerate((diagonal, across, partner))]

    def project_qkv():
        def tile(t):
            cols = tile_cols(t)
            part = jnp.dot(n_buf[...], wqkv[:, cols], preferred_element_type=F32).astype(BF16)
            qkv_part[:, :, cols] = part.reshape(n_x, n_seq, TILE)

        each(0, qkv_tiles, tile)

    barrier = pltpu.get_barrier_semaphore()
    each(1, peers, lambda e: pl.semaphore_signal(
        barrier, inc=1, device_id={"y": (y + e // n_x) % n_y, "x": (x + e % n_x) % n_x}, device_id_type=MESH))
    small = [pltpu.make_async_copy(src, dst, local_sem.at[10 + 2 * layers + i]) for i, (src, dst) in enumerate((
        (hid_any, h_end), (ga_any, ga_raw), (gm_any, gm_raw), (qg_any, qg_raw), (kg_any, kg_raw), (pos_any, pos_ref), (freq_any, freq_ref)))]
    start(small)
    start(qkv_loads(0))
    finish(small)
    start(o_loads(0) + cache_loads(0) + gate_up_loads(0) + down_loads(0))
    for layer in range(1, layers):
        start(cache_loads(layer))
    for raw, wide in ((ga_raw, ga_ref), (gm_raw, gm_ref), (qg_raw, qg_ref), (kg_raw, kg_ref)):
        for layer in range(layers):
            wide[layer] = raw[...].astype(F32)[layer:layer + 1]

    def first_norm(b, lanes):
        vals = h_end[b].astype(F32)
        sums = jnp.sum(vals * vals, axis=1, keepdims=True)
        n_buf[pl.ds(pl.multiple_of(b * rows, rows), rows), :] = (vals * lax.rsqrt(sums / depth + NORM_EPS) * ga_ref[0]).astype(BF16)
        return lanes + along_lanes(sums, b * rows)

    stat[0, 0] = lax.fori_loop(0, n_y, first_norm, jnp.zeros((1, HEAD_DIM), F32))
    q_rows[...] = jnp.zeros_like(q_rows)
    finish(qkv_loads(0))
    project_qkv()
    pl.semaphore_wait(barrier, peers - 1)
    for d in (2, 3, 1):
        first_copy(d).start()
        qkv_copy(d).start()

    my_pos = jnp.sum(
        jnp.where(lax.broadcasted_iota(jnp.int32, (n_seq, batch), 1) == lax.broadcasted_iota(jnp.int32, (n_seq, batch), 0) + x * n_seq,
                  pos_ref[...].astype(F32), 0.0), axis=1, keepdims=True)
    angles = my_pos * freq_ref[...]
    cos_tab = jnp.cos(angles)
    sin_tab = jnp.where(lax.broadcasted_iota(jnp.int32, (n_seq, HEAD_DIM), 1) < HEAD_DIM // 2, -1.0, 1.0) * jnp.sin(angles)
    slot_ref[...] = jnp.broadcast_to(my_pos.astype(jnp.int32), (n_seq, slots2)).reshape(slot_ref.shape)

    slot_row = lax.broadcasted_iota(jnp.int32, (slots2, HEAD_DIM), 0)
    slot_id = slot_row // kv_heads
    head_id = slot_row % kv_heads
    score_col = lax.broadcasted_iota(jnp.int32, (16, slots2), 1)
    score_head = lax.broadcasted_iota(jnp.int32, (16, slots2), 0) // group
    score_slot = score_col // kv_heads
    score_own = (score_col % kv_heads == score_head) | (score_head >= kv_heads)

    for d in range(1, n_x):
        first_copy(d).wait_recv()
        first_copy(d).wait_send()
    sums = [along_rows(stat[0, d], x * n_seq) for d in range(n_x)]
    scale = lax.rsqrt(sum(sums) / model_dim + NORM_EPS)
    for d in range(n_x):
        part_scale[d] = jnp.broadcast_to(jnp.where(scale > 0.0, scale / lax.rsqrt(sums[d] / depth + NORM_EPS), 0.0), (n_seq, TILE))

    def run_layer(layer):
        more = layer + 1 < layers

        def reload(loads):
            @pl.when(more)
            def _():
                start(loads(layer + 1))

        reload(qkv_loads)
        for d in range(1, n_x):
            qkv_copy(d).wait_recv()

        def projected(cols, scale_cols):
            total = qkv_part[x, :, cols].astype(F32) * part_scale[0, :, scale_cols]
            for d in range(1, n_x):
                total = total + qkv_recv[d, :, cols].astype(F32) * part_scale[d, :, scale_cols]
            return total.astype(BF16).astype(F32)

        for h in range(q_heads + kv_heads):
            vals = projected(pl.ds(h * HEAD_DIM, HEAD_DIM), pl.ds(0, HEAD_DIM))
            mean_sq = jnp.mean(vals * vals, axis=-1, keepdims=True)
            normed = vals * lax.rsqrt(mean_sq + NORM_EPS) * (qg_ref if h < q_heads else kg_ref)[layer]
            turned = (normed * cos_tab + pltpu.roll(normed, HEAD_DIM // 2, 1) * sin_tab).astype(BF16).astype(F32)
            if h < q_heads:
                q_rows[pl.ds(h, n_seq, stride=16), :] = turned
            else:
                new_out[layer, 0, h - q_heads] = turned
                kv_rows[0, h - q_heads] = turned.reshape(n_seq, 1, HEAD_DIM)
        for h in range(kv_heads):
            vals = projected(pl.ds(q_cols + kv_cols + h * HEAD_DIM, HEAD_DIM), pl.ds(0, HEAD_DIM))
            new_out[layer, 1, h] = vals
            kv_rows[1, h] = vals.reshape(n_seq, 1, HEAD_DIM)

        finish(cache_loads(layer))

        def sequences(i):
            for u in range(SEQS):
                b = i * SEQS + u
                slots = slot_ref[b]
                hit = slot_id == slots[:, :HEAD_DIM]
                for j, buf in enumerate((kbuf, vbuf)):
                    fresh = kv_rows[j, 0, b]
                    for h in range(1, kv_heads):
                        fresh = jnp.where(head_id == h, kv_rows[j, h, b], fresh)
                    buf[layer, b] = jnp.where(hit, fresh, buf[layer, b].astype(F32)).astype(BF16)
                q_b = q_rows[pl.ds(pl.multiple_of(b * 16, 16), 16), :].astype(BF16)
                scores = lax.dot_general(q_b, kbuf[layer, b], (((1,), (1,)), ((), ())), preferred_element_type=F32) * (HEAD_DIM ** -0.5)
                scores = jnp.where(score_own & (score_slot <= slots), scores, -1e30)
                top = jnp.max(scores, axis=1, keepdims=True)
                e = jnp.exp(scores - top)
                probs = (e / jnp.sum(e, axis=1, keepdims=True)).astype(BF16)
                o_rows[pl.ds(pl.multiple_of(b * 16, 16), 16), :] = jnp.dot(probs, vbuf[layer, b], preferred_element_type=F32)

        each(0, n_seq // SEQS, sequences)
        for h in range(q_heads):
            attn_all[x, :, h * HEAD_DIM:(h + 1) * HEAD_DIM] = o_rows[pl.ds(h, n_seq, stride=16), :].astype(BF16)
        for d in (2, 3, 1):
            attn_copy(d).start()
        finish(o_loads(layer))
        for d in range(1, n_x):
            qkv_copy(d).wait_send()
            attn_copy(d).wait_recv()

        drain_mid = all_reduce(
            0, at_mid, lambda cols: jnp.dot(attn_all[...].reshape(batch, q_cols), wo[:, cols], preferred_element_type=F32), h_end, h_mid, True)
        reload(o_loads)

        normalise(h_mid, 1, gm_ref, layer)
        finish(gate_up_loads(layer))

        def project(s):
            @pl.when(s < f_tiles)
            def _():
                cols = tile_cols(s)
                gate = jnp.dot(n_buf[...], wg[:, cols], preferred_element_type=F32).astype(BF16)
                up = jnp.dot(n_buf[...], wu[:, cols], preferred_element_type=F32).astype(BF16)
                gu_part[0, :, :, :, cols] = gate.reshape(2, 2, rows, TILE)
                gu_part[1, :, :, :, cols] = up.reshape(2, 2, rows, TILE)
                pair_copy(s).start()

            @pl.when(s >= PAIR_LAG)
            def _():
                t = s - PAIR_LAG
                cols = tile_cols(t)
                pair_copy(t).wait_recv()
                pair = gu_part[:, 1 - chip, core, :, cols].astype(F32) + gu_pair[:, 1 - chip, :, cols].astype(F32)
                gu_send[:, :, cols] = pair.astype(BF16)
                across_copy(t).start()

        each(0, f_tiles + PAIR_LAG, project)
        reload(gate_up_loads)

        def activate(t):
            cols = tile_cols(t)
            across_copy(t).wait_recv()
            gate_up = (gu_part[:, chip, core, :, cols].astype(F32) + gu_pair[:, chip, :, cols].astype(F32)
                       + gu_recv[:, :, cols].astype(F32)).astype(BF16).astype(F32)
            act_all[x, :, cols] = (jax.nn.silu(gate_up[0]) * gate_up[1]).astype(BF16)
            start(act_copies(t))

        each(0, f_tiles, activate)
        drain_mid()
        for d in range(1, n_x):
            attn_copy(d).wait_send()
        acc[...] = jnp.zeros_like(acc)
        finish(down_loads(layer))

        def down(t):
            for copy in act_copies(t):
                copy.wait_recv()
            vals = act_all[:, :, tile_cols(t)].reshape(batch, TILE)
            acc[...] += jnp.dot(vals, wd[tile_cols(t), :], preferred_element_type=F32)

        each(0, f_tiles, down)
        reload(down_loads)
        drain_end = all_reduce(1, at_end, lambda cols: acc[:, cols], h_mid, h_end, more)

        @pl.when(more)
        def _():
            normalise(h_end, 2, ga_ref, layer + 1)
            part_scale[...] = jnp.ones_like(part_scale)
            finish(qkv_loads(layer + 1))
            project_qkv()
            for d in (2, 3, 1):
                qkv_copy(d).start()

        drain_end()

        def drain_mlp(t):
            pair_copy(t).wait_send()
            across_copy(t).wait_send()
            for copy in act_copies(t):
                copy.wait_send()

        each(0, f_tiles, drain_mlp)

    each(0, layers, run_layer)
    hid_out[...] = h_end[...]


def cache_kernel(dims, hid_ref, new_ref, pos_ref, kc_ref, vc_ref, hid_out, kc_out, vc_out, hid_buf, kbuf, vbuf, in_sem, out_sem):
    layers, n_seq, kv_heads = dims
    first = lax.axis_index("x") * n_seq
    arrive, leave = [], []
    for layer in range(layers):
        for src, dst in ((kc_ref, kbuf), (vc_ref, vbuf)):
            arrive.append(pltpu.make_async_copy(src.at[layer], dst.at[layer], in_sem.at[len(arrive)]))
            arrive[-1].start()
    hidden_in = pltpu.make_async_copy(hid_ref, hid_buf, in_sem.at[len(arrive)])
    hidden_in.start()
    for layer in range(layers):
        for i, (buf, dst) in enumerate(((kbuf, kc_out), (vbuf, vc_out))):
            arrive[2 * layer + i].wait()
            for b in range(n_seq):
                rows = jnp.concatenate([new_ref[layer, i, h, b:b + 1, :] for h in range(kv_heads)], axis=0)
                buf[layer, b, pos_ref[0, first + b]] = rows.astype(BF16)
            leave.append(pltpu.make_async_copy(buf.at[layer], dst.at[layer], out_sem.at[len(leave)]))
            leave[-1].start()
    hidden_in.wait()
    leave.append(pltpu.make_async_copy(hid_buf, hid_out, out_sem.at[len(leave)]))
    leave[-1].start()
    for copy in leave:
        copy.wait()


def solution(mesh):
    n_x, n_y = mesh.shape['x'], mesh.shape['y']
    cache_spec = P(None, ('dp', 'x'), None, 'y', None)
    col_spec = P(None, 'x', 'y')
    row_spec = P(None, 'y', 'x')
    in_specs = (P('dp', 'x'), P('dp'), cache_spec, cache_spec, P(None, 'x'), P(None, 'x'), P(), P(), col_spec, col_spec, col_spec, row_spec, col_spec, col_spec, row_spec)
    out_specs = (P('dp', 'x'), cache_spec, cache_spec)

    def device_step(hidden, positions, k_cache, v_cache, g_attn, g_mlp, q_gain, k_gain, w_q, w_k, w_v, w_o, w_gate, w_up, w_down):
        batch, depth = hidden.shape
        layers, n_seq, slots, kv_heads, _ = k_cache.shape
        q_cols, kv_cols, ffn = w_q.shape[2], w_k.shape[2], w_gate.shape[2]
        rows = batch // n_y
        slots2 = slots * kv_heads
        dims = (layers, n_y, n_x, rows, depth, q_cols, kv_cols, ffn)
        cols_qkv = q_cols + 2 * kv_cols
        vmem = pl.BlockSpec(memory_space=pltpu.VMEM)
        hbm = pl.BlockSpec(memory_space=pl.ANY)
        cache_shape = (layers, n_seq, slots2, HEAD_DIM)
        peers = n_y * n_x
        d_tiles, f_tiles = depth // TILE, ffn // TILE
        copies = 3 * (n_x - 1) + 2 * (2 * (n_y - 1) * d_tiles + peers - 1) + 5 * f_tiles
        positions = positions.reshape(1, batch)
        new_hidden, new_rows = pl.pallas_call(
            functools.partial(step_kernel, dims),
            out_shape=(jax.ShapeDtypeStruct((n_y, rows, depth), BF16), jax.ShapeDtypeStruct((layers, 2, kv_heads, n_seq, HEAD_DIM), F32)),
            in_specs=[hbm] * 16,
            out_specs=(vmem, vmem),
            scratch_shapes=[
                pltpu.VMEM((depth, cols_qkv), BF16),
                pltpu.VMEM((q_cols, depth), BF16),
                pltpu.VMEM((depth, ffn), BF16),
                pltpu.VMEM((depth, ffn), BF16),
                pltpu.VMEM((ffn, depth), BF16),
                pltpu.VMEM(cache_shape, BF16),
                pltpu.VMEM(cache_shape, BF16),
                pltpu.VMEM((batch, depth), BF16),
                pltpu.VMEM((3, peers, 1, HEAD_DIM), F32),
                pltpu.VMEM((n_x, n_seq, cols_qkv), BF16),
                pltpu.VMEM((n_x, n_seq, cols_qkv), BF16),
                pltpu.VMEM((16 * n_seq, HEAD_DIM), F32),
                pltpu.VMEM((16 * n_seq, HEAD_DIM), F32),
                pltpu.VMEM((n_x, n_seq, q_cols), BF16),
                pltpu.VMEM((2, n_y, rows, depth), BF16),
                pltpu.VMEM((2, n_y, rows, depth), BF16),
                pltpu.VMEM((n_y, rows, depth), BF16),
                pltpu.VMEM((n_y, rows, depth), BF16),
                pltpu.VMEM((2, 2, 2, rows, ffn), BF16),
                pltpu.VMEM((2, 2, rows, ffn), BF16),
                pltpu.VMEM((2, rows, ffn), BF16),
                pltpu.VMEM((2, rows, ffn), BF16),
                pltpu.VMEM((n_x, rows, ffn), BF16),
                pltpu.VMEM((batch, depth), F32),
                pltpu.VMEM((1, batch), jnp.int32),
                pltpu.VMEM((1, HEAD_DIM), F32),
                pltpu.VMEM(g_attn.shape, BF16),
                pltpu.VMEM(g_mlp.shape, BF16),
                pltpu.VMEM(q_gain.shape, BF16),
                pltpu.VMEM(k_gain.shape, BF16),
                pltpu.VMEM((layers, 1, depth), F32),
                pltpu.VMEM((layers, 1, depth), F32),
                pltpu.VMEM((layers, 1, HEAD_DIM), F32),
                pltpu.VMEM((layers, 1, HEAD_DIM), F32),
                pltpu.VMEM((n_seq, 1, slots2), jnp.int32),
                pltpu.VMEM((n_x, n_seq, TILE), F32),
                pltpu.VMEM((2, kv_heads, n_seq, 1, HEAD_DIM), F32),
                pltpu.SemaphoreType.DMA((copies,)),
                pltpu.SemaphoreType.DMA((copies,)),
                pltpu.SemaphoreType.DMA((17 + 2 * layers,)),
            ],
            compiler_params=pltpu.CompilerParams(collective_id=0, has_side_effects=True, vmem_limit_bytes=64 * 1024 * 1024 - 65536),
        )(hidden.reshape(n_y, rows, depth), positions, inverse_frequencies(), g_attn, g_mlp, q_gain, k_gain,
          k_cache.reshape(cache_shape), v_cache.reshape(cache_shape), w_q, w_k, w_v, w_o, w_gate, w_up, w_down)
        return pl.pallas_call(
            functools.partial(cache_kernel, (layers, n_seq, kv_heads)),
            out_shape=tuple(jax.ShapeDtypeStruct(a.shape, a.dtype) for a in (hidden, k_cache, v_cache)),
            in_specs=[hbm, vmem, pl.BlockSpec(memory_space=pltpu.SMEM), hbm, hbm],
            out_specs=(hbm, hbm, hbm),
            scratch_shapes=[
                pltpu.VMEM(hidden.shape, BF16),
                pltpu.VMEM(k_cache.shape, BF16),
                pltpu.VMEM(k_cache.shape, BF16),
                pltpu.SemaphoreType.DMA((2 * layers + 1,)),
                pltpu.SemaphoreType.DMA((2 * layers + 1,)),
            ],
            compiler_params=pltpu.CompilerParams(vmem_limit_bytes=64 * 1024 * 1024 - 65536),
        )(new_hidden.reshape(batch, depth), new_rows, positions, k_cache, v_cache)

    return jax.shard_map(device_step, mesh=mesh, in_specs=in_specs, out_specs=out_specs, check_vma=False)
```

```python
import functools

import jax
import jax.numpy as jnp
import numpy as np
from jax import lax
from jax.experimental import pallas as pl
from jax.experimental.pallas import tpu as pltpu
from jax.sharding import PartitionSpec as P

HEAD_DIM = 128
NORM_EPS = 1e-6
ROPE_BASE = 1000000.0
TILE = 256
GROUP_TILES = (3, 3, 3, 3, 3, 2)
SEQS = 4
MESH = pl.DeviceIdType.MESH
F32 = jnp.float32
BF16 = jnp.bfloat16


def inverse_frequencies():
    half_dim = HEAD_DIM // 2
    freqs = np.power(np.float32(ROPE_BASE), (-2.0 * np.arange(half_dim) / HEAD_DIM).astype(np.float32))
    return np.concatenate([freqs, freqs])[None].astype(np.float32)


def split_tiles(n_tiles):
    share = n_tiles / sum(GROUP_TILES)
    edges = [round(share * sum(GROUP_TILES[:i])) for i in range(len(GROUP_TILES) + 1)]
    return [(a, b) for a, b in zip(edges, edges[1:]) if b > a]


def step_kernel(dims, *refs):
    (layers, n_y, n_x, rows, depth, q_cols, kv_cols, ffn) = dims
    (hid_any, pos_any, freq_any, ga_any, gm_any, qg_any, kg_any, kc_ref, vc_ref,
     wq_ref, wk_ref, wv_ref, wo_ref, wg_ref, wu_ref, wd_ref,
     hid_out, new_out,
     wqkv, wo, wg, wu, wd, kbuf, vbuf, n_buf, stat, qkv_part, qkv_recv, q_rows, o_rows, attn_all,
     ar_part, ar_recv, h_mid, h_end, gu_part, gu_pair, gu_send, gu_recv, act_all, acc,
     pos_ref, freq_ref, ga_raw, gm_raw, qg_raw, kg_raw, ga_ref, gm_ref, qg_ref, kg_ref, slot_ref, part_scale, kv_rows, s_rows, p_rows,
     send_sem, recv_sem, local_sem) = refs
    batch = n_y * rows
    cols_qkv = q_cols + 2 * kv_cols
    q_heads = q_cols // HEAD_DIM
    kv_heads = kv_cols // HEAD_DIM
    group = q_heads // kv_heads
    model_dim = depth * n_x
    slots2 = kbuf.shape[2]
    n_seq = batch // n_x
    peers = n_y * n_x
    d_tiles, f_tiles, qkv_tiles = depth // TILE, ffn // TILE, cols_qkv // TILE

    y = lax.axis_index("y")
    x = lax.axis_index("x")
    chip = x // 2
    core = x % 2
    partner = 2 * chip + (1 - core)
    across = 2 * (1 - chip) + core
    diagonal = 2 * (1 - chip) + (1 - core)

    groups = split_tiles(f_tiles)
    at_qkv, at_first, at_attn, at_mid = 0, 1, 2, 3
    at_end = at_mid + d_tiles + 2
    at_mlp = at_end + d_tiles + 2

    def remote(src, dst, to_send, to_recv, to_y, to_x):
        return pltpu.make_async_remote_copy(
            src_ref=src, dst_ref=dst, send_sem=send_sem.at[to_send], recv_sem=recv_sem.at[to_recv],
            device_id={"y": to_y, "x": to_x}, device_id_type=MESH)

    def received(i, like):
        pltpu.make_async_copy(like, like, recv_sem.at[i]).wait()

    def delivered(i, like):
        pltpu.make_async_copy(like, like, send_sem.at[i]).wait()

    def each(first, last, body):
        def step(i, carry):
            body(i)
            return carry

        lax.fori_loop(first, last, step, 0)

    def tile_cols(t):
        return pl.ds(pl.multiple_of(t * TILE, TILE), TILE)

    def qkv_loads(layer):
        return [pltpu.make_async_copy(wq_ref.at[layer], wqkv.at[:, 0:q_cols], local_sem.at[0]),
                pltpu.make_async_copy(wk_ref.at[layer], wqkv.at[:, q_cols:q_cols + kv_cols], local_sem.at[1]),
                pltpu.make_async_copy(wv_ref.at[layer], wqkv.at[:, q_cols + kv_cols:cols_qkv], local_sem.at[2])]

    def o_loads(layer):
        return [pltpu.make_async_copy(wo_ref.at[layer], wo, local_sem.at[3])]

    def gate_up_loads(layer):
        return [pltpu.make_async_copy(src.at[layer], dst, local_sem.at[4 + i]) for i, (src, dst) in enumerate(((wg_ref, wg), (wu_ref, wu)))]

    def down_loads(layer):
        return [pltpu.make_async_copy(wd_ref.at[layer], wd, local_sem.at[6])]

    def cache_loads(layer):
        return [pltpu.make_async_copy(src.at[layer], dst.at[layer], local_sem.at[7 + i * layers + layer])
                for i, (src, dst) in enumerate(((kc_ref, kbuf), (vc_ref, vbuf)))]

    def start(copies):
        for copy in copies:
            copy.start()

    def finish(copies):
        for copy in copies:
            copy.wait()

    row_i = lax.broadcasted_iota(jnp.int32, (rows, HEAD_DIM), 0)
    lane_i = lax.broadcasted_iota(jnp.int32, (rows, HEAD_DIM), 1)

    def along_lanes(column, first_row):
        return jnp.sum(jnp.where(lane_i == row_i + first_row, column, 0.0), axis=0, keepdims=True)

    def along_rows(lanes, first_row):
        return jnp.sum(jnp.where(lane_i == row_i + first_row, lanes, 0.0), axis=1, keepdims=True)

    def normalise(hidden_ref, i, gain_ref, layer):
        total = jnp.sum(stat[i], axis=0)
        scales = lax.rsqrt(total / model_dim + NORM_EPS)
        gain = gain_ref[layer]

        def block(b):
            n_buf[pl.ds(pl.multiple_of(b * rows, rows), rows), :] = (hidden_ref[b].astype(F32) * along_rows(scales, b * rows) * gain).astype(BF16)

        each(0, n_y, block)

    def all_reduce(i, base, tile_product, residual_ref, result_ref, with_stats):
        others = n_y - 1
        send = 3 + 3 * i

        def scatter(t, d):
            cols = tile_cols(t)
            return remote(ar_part.at[i, (y + d) % n_y, :, cols], ar_recv.at[i, d, :, cols], send, base + t, (y + d) % n_y, x)

        def gather(t, d):
            mine = result_ref.at[y, :, tile_cols(t)]
            return remote(mine, mine, send + 1, base + d_tiles, (y + d) % n_y, x)

        def share(e):
            return remote(stat.at[i + 1, 0], stat.at[i + 1, e], send + 2, base + d_tiles + 1, (y + e // n_x) % n_y, (x + e % n_x) % n_x)

        def send_tile(t):
            ar_part[i, :, :, tile_cols(t)] = tile_product(tile_cols(t)).astype(BF16).reshape(n_y, rows, TILE)
            for d in (2, 3, 1):
                scatter(t, d).start()

        each(0, d_tiles, send_tile)

        def sum_tile(t, squares):
            cols = tile_cols(t)
            received(base + t, ar_recv.at[i, 1:n_y, :, cols])
            total = ar_part[i, y, :, cols].astype(F32)
            for d in range(1, n_y):
                total = total + ar_recv[i, d, :, cols].astype(F32)
            new = (residual_ref[y, :, cols].astype(F32) + total.astype(BF16).astype(F32)).astype(BF16)
            result_ref[y, :, cols] = new
            for d in (2, 3, 1):
                gather(t, d).start()
            return squares + new.astype(F32) * new.astype(F32)

        squares = lax.fori_loop(0, d_tiles, sum_tile, jnp.zeros((rows, TILE), F32))
        stat[i + 1, 0] = along_lanes(jnp.sum(squares, axis=1, keepdims=True), y * rows)

        @pl.when(with_stats)
        def _():
            each(1, peers, lambda e: share(e).start())

        received(base + d_tiles, ar_recv.at[i, 1:n_y])

        @pl.when(with_stats)
        def _():
            received(base + d_tiles + 1, stat.at[i + 1, 1:peers])

        def drain():
            delivered(send, ar_recv.at[i, 1:n_y])
            delivered(send + 1, ar_recv.at[i, 1:n_y])

            @pl.when(with_stats)
            def _():
                delivered(send + 2, stat.at[i + 1, 1:peers])

        return drain

    def qkv_copy(d):
        return remote(qkv_part.at[(x + d) % n_x], qkv_recv.at[d], 0, at_qkv, y, (x + d) % n_x)

    def first_copy(d):
        return remote(stat.at[0, 0], stat.at[0, d], 1, at_first, y, (x + d) % n_x)

    def attn_copy(d):
        return remote(attn_all.at[x], attn_all.at[x], 2, at_attn, y, (x + d) % n_x)

    def group_cols(g):
        return pl.ds(groups[g][0] * TILE, (groups[g][1] - groups[g][0]) * TILE)

    def pair_copy(g):
        cols = group_cols(g)
        return remote(gu_part.at[:, :, 1 - core, :, cols], gu_pair.at[:, :, :, cols], 9, at_mlp + g, y, partner)

    def across_copy(g):
        cols = group_cols(g)
        return remote(gu_send.at[:, :, cols], gu_recv.at[:, :, cols], 10, at_mlp + len(groups) + g, y, across)

    def act_copies(g):
        mine = act_all.at[x, :, group_cols(g)]
        return [remote(mine, mine, 11, at_mlp + 2 * len(groups) + g, y, to_x) for to_x in (diagonal, across, partner)]

    def project_qkv():
        def tile(t):
            cols = tile_cols(t)
            part = jnp.dot(n_buf[...], wqkv[:, cols], preferred_element_type=F32).astype(BF16)
            qkv_part[:, :, cols] = part.reshape(n_x, n_seq, TILE)

        each(0, qkv_tiles, tile)

    barrier = pltpu.get_barrier_semaphore()
    each(1, peers, lambda e: pl.semaphore_signal(
        barrier, inc=1, device_id={"y": (y + e // n_x) % n_y, "x": (x + e % n_x) % n_x}, device_id_type=MESH))
    small = [pltpu.make_async_copy(src, dst, local_sem.at[7 + 2 * layers + i]) for i, (src, dst) in enumerate((
        (hid_any, h_end), (ga_any, ga_raw), (gm_any, gm_raw), (qg_any, qg_raw), (kg_any, kg_raw), (pos_any, pos_ref), (freq_any, freq_ref)))]
    start(small)
    start(qkv_loads(0))
    finish(small)
    start(o_loads(0) + cache_loads(0) + gate_up_loads(0) + down_loads(0))
    for layer in range(1, layers):
        start(cache_loads(layer))
    for raw, wide in ((ga_raw, ga_ref), (gm_raw, gm_ref), (qg_raw, qg_ref), (kg_raw, kg_ref)):
        for layer in range(layers):
            wide[layer] = raw[...].astype(F32)[layer:layer + 1]

    def first_norm(b, lanes):
        vals = h_end[b].astype(F32)
        sums = jnp.sum(vals * vals, axis=1, keepdims=True)
        n_buf[pl.ds(pl.multiple_of(b * rows, rows), rows), :] = (vals * lax.rsqrt(sums / depth + NORM_EPS) * ga_ref[0]).astype(BF16)
        return lanes + along_lanes(sums, b * rows)

    stat[0, 0] = lax.fori_loop(0, n_y, first_norm, jnp.zeros((1, HEAD_DIM), F32))
    q_rows[...] = jnp.zeros_like(q_rows)
    finish(qkv_loads(0))
    project_qkv()
    pl.semaphore_wait(barrier, peers - 1)
    for d in (2, 3, 1):
        first_copy(d).start()
        qkv_copy(d).start()

    my_pos = jnp.sum(
        jnp.where(lax.broadcasted_iota(jnp.int32, (n_seq, batch), 1) == lax.broadcasted_iota(jnp.int32, (n_seq, batch), 0) + x * n_seq,
                  pos_ref[...].astype(F32), 0.0), axis=1, keepdims=True)
    angles = my_pos * freq_ref[...]
    cos_tab = jnp.cos(angles)
    sin_tab = jnp.where(lax.broadcasted_iota(jnp.int32, (n_seq, HEAD_DIM), 1) < HEAD_DIM // 2, -1.0, 1.0) * jnp.sin(angles)
    slot_ref[...] = jnp.broadcast_to(my_pos.astype(jnp.int32), (n_seq, slots2)).reshape(slot_ref.shape)

    slot_row = lax.broadcasted_iota(jnp.int32, (slots2, HEAD_DIM), 0)
    slot_id = slot_row // kv_heads
    head_id = slot_row % kv_heads
    score_col = lax.broadcasted_iota(jnp.int32, (16, slots2), 1)
    score_head = lax.broadcasted_iota(jnp.int32, (16, slots2), 0) // group
    score_slot = score_col // kv_heads
    score_own = (score_col % kv_heads == score_head) | (score_head >= kv_heads)

    received(at_first, stat.at[0, 1:n_x])
    delivered(1, stat.at[0, 1:n_x])
    sums = [along_rows(stat[0, d], x * n_seq) for d in range(n_x)]
    scale = lax.rsqrt(sum(sums) / model_dim + NORM_EPS)
    for d in range(n_x):
        part_scale[d] = jnp.broadcast_to(jnp.where(scale > 0.0, scale / lax.rsqrt(sums[d] / depth + NORM_EPS), 0.0), (n_seq, TILE))

    def run_layer(layer):
        more = layer + 1 < layers

        def reload(loads):
            @pl.when(more)
            def _():
                start(loads(layer + 1))

        reload(qkv_loads)
        received(at_qkv, qkv_recv.at[1:n_x])

        def projected(cols, scale_cols):
            total = qkv_part[x, :, cols].astype(F32) * part_scale[0, :, scale_cols]
            for d in range(1, n_x):
                total = total + qkv_recv[d, :, cols].astype(F32) * part_scale[d, :, scale_cols]
            return total.astype(BF16).astype(F32)

        for h in range(q_heads + kv_heads):
            vals = projected(pl.ds(h * HEAD_DIM, HEAD_DIM), pl.ds(0, HEAD_DIM))
            mean_sq = jnp.mean(vals * vals, axis=-1, keepdims=True)
            normed = vals * lax.rsqrt(mean_sq + NORM_EPS) * (qg_ref if h < q_heads else kg_ref)[layer]
            turned = (normed * cos_tab + pltpu.roll(normed, HEAD_DIM // 2, 1) * sin_tab).astype(BF16).astype(F32)
            if h < q_heads:
                q_rows[pl.ds(h, n_seq, stride=16), :] = turned
            else:
                new_out[layer, 0, h - q_heads] = turned
                kv_rows[0, h - q_heads] = turned.reshape(n_seq, 1, HEAD_DIM)
        for h in range(kv_heads):
            vals = projected(pl.ds(q_cols + kv_cols + h * HEAD_DIM, HEAD_DIM), pl.ds(0, HEAD_DIM))
            new_out[layer, 1, h] = vals
            kv_rows[1, h] = vals.reshape(n_seq, 1, HEAD_DIM)

        finish(cache_loads(layer))

        def update(i):
            for u in range(SEQS):
                b = i * SEQS + u
                hit = slot_id == slot_ref[b][:, :HEAD_DIM]
                for j, buf in enumerate((kbuf, vbuf)):
                    fresh = kv_rows[j, 0, b]
                    for h in range(1, kv_heads):
                        fresh = jnp.where(head_id == h, kv_rows[j, h, b], fresh)
                    buf[layer, b] = jnp.where(hit, fresh, buf[layer, b].astype(F32)).astype(BF16)

        each(0, n_seq // SEQS, update)
        for b in range(n_seq):
            q_b = q_rows[b * 16:(b + 1) * 16, :].astype(BF16)
            scores = lax.dot_general(q_b, kbuf[layer, b], (((1,), (1,)), ((), ())), preferred_element_type=F32) * (HEAD_DIM ** -0.5)
            s_rows[b * 16:(b + 1) * 16, :] = jnp.where(score_own & (score_slot <= slot_ref[b]), scores, -1e30)

        def softmax(i):
            block = pl.ds(pl.multiple_of(i * 16 * SEQS, 16 * SEQS), 16 * SEQS)
            scores = s_rows[block, :]
            e = jnp.exp(scores - jnp.max(scores, axis=1, keepdims=True))
            p_rows[block, :] = (e / jnp.sum(e, axis=1, keepdims=True)).astype(BF16)

        each(0, n_seq // SEQS, softmax)
        for b in range(n_seq):
            o_rows[b * 16:(b + 1) * 16, :] = jnp.dot(p_rows[b * 16:(b + 1) * 16, :], vbuf[layer, b], preferred_element_type=F32)
        for h in range(q_heads):
            attn_all[x, :, h * HEAD_DIM:(h + 1) * HEAD_DIM] = o_rows[pl.ds(h, n_seq, stride=16), :].astype(BF16)
        for d in (2, 3, 1):
            attn_copy(d).start()
        finish(o_loads(layer))
        delivered(0, qkv_recv.at[1:n_x])
        received(at_attn, attn_all.at[1:n_x])

        drain_mid = all_reduce(
            0, at_mid, lambda cols: jnp.dot(attn_all[...].reshape(batch, q_cols), wo[:, cols], preferred_element_type=F32), h_end, h_mid, True)
        reload(o_loads)

        normalise(h_mid, 1, gm_ref, layer)
        finish(gate_up_loads(layer))

        def project(t):
            cols = tile_cols(t)
            gate = jnp.dot(n_buf[...], wg[:, cols], preferred_element_type=F32).astype(BF16)
            up = jnp.dot(n_buf[...], wu[:, cols], preferred_element_type=F32).astype(BF16)
            gu_part[0, :, :, :, cols] = gate.reshape(2, 2, rows, TILE)
            gu_part[1, :, :, :, cols] = up.reshape(2, 2, rows, TILE)

        def cross(g):
            cols = group_cols(g)
            received(at_mlp + g, gu_pair.at[:, :, :, cols])

            def tile(t):
                cols = tile_cols(t)
                pair = gu_part[:, 1 - chip, core, :, cols].astype(F32) + gu_pair[:, 1 - chip, :, cols].astype(F32)
                gu_send[:, :, cols] = pair.astype(BF16)

            each(*groups[g], tile)
            across_copy(g).start()

        def activate(g):
            received(at_mlp + len(groups) + g, gu_recv.at[:, :, group_cols(g)])

            def tile(t):
                cols = tile_cols(t)
                gate_up = (gu_part[:, chip, core, :, cols].astype(F32) + gu_pair[:, chip, :, cols].astype(F32)
                           + gu_recv[:, :, cols].astype(F32)).astype(BF16).astype(F32)
                act_all[x, :, cols] = (jax.nn.silu(gate_up[0]) * gate_up[1]).astype(BF16)

            each(*groups[g], tile)
            start(act_copies(g))

        for g in range(len(groups)):
            each(*groups[g], project)
            pair_copy(g).start()
            if g >= 2:
                cross(g - 2)
        reload(gate_up_loads)
        for g in range(max(len(groups) - 2, 0), len(groups)):
            cross(g)
        for g in range(len(groups)):
            activate(g)
        drain_mid()
        delivered(2, attn_all.at[1:n_x])
        finish(down_loads(layer))
        for g, (first, last) in enumerate(groups):
            cols = group_cols(g)
            received(at_mlp + 2 * len(groups) + g, act_all.at[1:n_x, :, cols])

            def down(t):
                part = jnp.dot(act_all[:, :, cols].reshape(batch, (last - first) * TILE), wd[cols, tile_cols(t)], preferred_element_type=F32)
                acc[:, tile_cols(t)] = acc[:, tile_cols(t)] + part if g else part

            each(0, d_tiles, down)
        reload(down_loads)
        drain_end = all_reduce(1, at_end, lambda cols: acc[:, cols], h_mid, h_end, more)

        @pl.when(more)
        def _():
            normalise(h_end, 2, ga_ref, layer + 1)
            part_scale[...] = jnp.ones_like(part_scale)
            finish(qkv_loads(layer + 1))
            project_qkv()
            for d in (2, 3, 1):
                qkv_copy(d).start()

        drain_end()

        delivered(9, gu_pair)
        delivered(10, gu_recv)
        delivered(11, act_all.at[1:n_x])

    each(0, layers, run_layer)
    hid_out[...] = h_end[...]


def cache_kernel(dims, hid_ref, new_ref, pos_ref, kc_ref, vc_ref, hid_out, kc_out, vc_out, hid_buf, kbuf, vbuf, in_sem, out_sem):
    layers, n_seq, kv_heads = dims
    first = lax.axis_index("x") * n_seq
    arrive, leave = [], []
    for layer in range(layers):
        for src, dst in ((kc_ref, kbuf), (vc_ref, vbuf)):
            arrive.append(pltpu.make_async_copy(src.at[layer], dst.at[layer], in_sem.at[len(arrive)]))
            arrive[-1].start()
    hidden_in = pltpu.make_async_copy(hid_ref, hid_buf, in_sem.at[len(arrive)])
    hidden_in.start()
    for layer in range(layers):
        for i, (buf, dst) in enumerate(((kbuf, kc_out), (vbuf, vc_out))):
            arrive[2 * layer + i].wait()
            for b in range(n_seq):
                rows = jnp.concatenate([new_ref[layer, i, h, b:b + 1, :] for h in range(kv_heads)], axis=0)
                buf[layer, b, pos_ref[0, first + b]] = rows.astype(BF16)
            leave.append(pltpu.make_async_copy(buf.at[layer], dst.at[layer], out_sem.at[len(leave)]))
            leave[-1].start()
    hidden_in.wait()
    leave.append(pltpu.make_async_copy(hid_buf, hid_out, out_sem.at[len(leave)]))
    leave[-1].start()
    for copy in leave:
        copy.wait()


def solution(mesh):
    n_x, n_y = mesh.shape['x'], mesh.shape['y']
    cache_spec = P(None, ('dp', 'x'), None, 'y', None)
    col_spec = P(None, 'x', 'y')
    row_spec = P(None, 'y', 'x')
    in_specs = (P('dp', 'x'), P('dp'), cache_spec, cache_spec, P(None, 'x'), P(None, 'x'), P(), P(), col_spec, col_spec, col_spec, row_spec, col_spec, col_spec, row_spec)
    out_specs = (P('dp', 'x'), cache_spec, cache_spec)

    def device_step(hidden, positions, k_cache, v_cache, g_attn, g_mlp, q_gain, k_gain, w_q, w_k, w_v, w_o, w_gate, w_up, w_down):
        batch, depth = hidden.shape
        layers, n_seq, slots, kv_heads, _ = k_cache.shape
        q_cols, kv_cols, ffn = w_q.shape[2], w_k.shape[2], w_gate.shape[2]
        rows = batch // n_y
        slots2 = slots * kv_heads
        dims = (layers, n_y, n_x, rows, depth, q_cols, kv_cols, ffn)
        cols_qkv = q_cols + 2 * kv_cols
        vmem = pl.BlockSpec(memory_space=pltpu.VMEM)
        hbm = pl.BlockSpec(memory_space=pl.ANY)
        cache_shape = (layers, n_seq, slots2, HEAD_DIM)
        peers = n_y * n_x
        d_tiles, f_tiles = depth // TILE, ffn // TILE
        receives = 3 + 2 * (d_tiles + 2) + 3 * len(split_tiles(f_tiles))
        positions = positions.reshape(1, batch)
        new_hidden, new_rows = pl.pallas_call(
            functools.partial(step_kernel, dims),
            out_shape=(jax.ShapeDtypeStruct((n_y, rows, depth), BF16), jax.ShapeDtypeStruct((layers, 2, kv_heads, n_seq, HEAD_DIM), F32)),
            in_specs=[hbm] * 16,
            out_specs=(vmem, vmem),
            scratch_shapes=[
                pltpu.VMEM((depth, cols_qkv), BF16),
                pltpu.VMEM((q_cols, depth), BF16),
                pltpu.VMEM((depth, ffn), BF16),
                pltpu.VMEM((depth, ffn), BF16),
                pltpu.VMEM((ffn, depth), BF16),
                pltpu.VMEM(cache_shape, BF16),
                pltpu.VMEM(cache_shape, BF16),
                pltpu.VMEM((batch, depth), BF16),
                pltpu.VMEM((3, peers, 1, HEAD_DIM), F32),
                pltpu.VMEM((n_x, n_seq, cols_qkv), BF16),
                pltpu.VMEM((n_x, n_seq, cols_qkv), BF16),
                pltpu.VMEM((16 * n_seq, HEAD_DIM), F32),
                pltpu.VMEM((16 * n_seq, HEAD_DIM), F32),
                pltpu.VMEM((n_x, n_seq, q_cols), BF16),
                pltpu.VMEM((2, n_y, rows, depth), BF16),
                pltpu.VMEM((2, n_y, rows, depth), BF16),
                pltpu.VMEM((n_y, rows, depth), BF16),
                pltpu.VMEM((n_y, rows, depth), BF16),
                pltpu.VMEM((2, 2, 2, rows, ffn), BF16),
                pltpu.VMEM((2, 2, rows, ffn), BF16),
                pltpu.VMEM((2, rows, ffn), BF16),
                pltpu.VMEM((2, rows, ffn), BF16),
                pltpu.VMEM((n_x, rows, ffn), BF16),
                pltpu.VMEM((batch, depth), F32),
                pltpu.VMEM((1, batch), jnp.int32),
                pltpu.VMEM((1, HEAD_DIM), F32),
                pltpu.VMEM(g_attn.shape, BF16),
                pltpu.VMEM(g_mlp.shape, BF16),
                pltpu.VMEM(q_gain.shape, BF16),
                pltpu.VMEM(k_gain.shape, BF16),
                pltpu.VMEM((layers, 1, depth), F32),
                pltpu.VMEM((layers, 1, depth), F32),
                pltpu.VMEM((layers, 1, HEAD_DIM), F32),
                pltpu.VMEM((layers, 1, HEAD_DIM), F32),
                pltpu.VMEM((n_seq, 1, slots2), jnp.int32),
                pltpu.VMEM((n_x, n_seq, TILE), F32),
                pltpu.VMEM((2, kv_heads, n_seq, 1, HEAD_DIM), F32),
                pltpu.VMEM((16 * n_seq, slots2), F32),
                pltpu.VMEM((16 * n_seq, slots2), BF16),
                pltpu.SemaphoreType.DMA((12,)),
                pltpu.SemaphoreType.DMA((receives,)),
                pltpu.SemaphoreType.DMA((14 + 2 * layers,)),
            ],
            compiler_params=pltpu.CompilerParams(collective_id=0, has_side_effects=True, vmem_limit_bytes=64 * 1024 * 1024 - 65536),
        )(hidden.reshape(n_y, rows, depth), positions, inverse_frequencies(), g_attn, g_mlp, q_gain, k_gain,
          k_cache.reshape(cache_shape), v_cache.reshape(cache_shape), w_q, w_k, w_v, w_o, w_gate, w_up, w_down)
        return pl.pallas_call(
            functools.partial(cache_kernel, (layers, n_seq, kv_heads)),
            out_shape=tuple(jax.ShapeDtypeStruct(a.shape, a.dtype) for a in (hidden, k_cache, v_cache)),
            in_specs=[hbm, vmem, pl.BlockSpec(memory_space=pltpu.SMEM), hbm, hbm],
            out_specs=(hbm, hbm, hbm),
            scratch_shapes=[
                pltpu.VMEM(hidden.shape, BF16),
                pltpu.VMEM(k_cache.shape, BF16),
                pltpu.VMEM(k_cache.shape, BF16),
                pltpu.SemaphoreType.DMA((2 * layers + 1,)),
                pltpu.SemaphoreType.DMA((2 * layers + 1,)),
            ],
            compiler_params=pltpu.CompilerParams(vmem_limit_bytes=64 * 1024 * 1024 - 65536),
        )(new_hidden.reshape(batch, depth), new_rows, positions, k_cache, v_cache)

    return jax.shard_map(device_step, mesh=mesh, in_specs=in_specs, out_specs=out_specs, check_vma=False)
```

```python
import functools

import jax
import jax.numpy as jnp
import numpy as np
from jax import lax
from jax.experimental import pallas as pl
from jax.experimental.pallas import tpu as pltpu
from jax.sharding import PartitionSpec as P

HEAD_DIM = 128
NORM_EPS = 1e-6
ROPE_BASE = 1000000.0
TILE = 256
GROUP_TILES = (3, 3, 3, 3, 3, 2)
SEQS = 4
MESH = pl.DeviceIdType.MESH
F32 = jnp.float32
BF16 = jnp.bfloat16


def inverse_frequencies():
    half_dim = HEAD_DIM // 2
    freqs = np.power(np.float32(ROPE_BASE), (-2.0 * np.arange(half_dim) / HEAD_DIM).astype(np.float32))
    return np.concatenate([freqs, freqs])[None].astype(np.float32)


def split_tiles(n_tiles):
    share = n_tiles / sum(GROUP_TILES)
    edges = [round(share * sum(GROUP_TILES[:i])) for i in range(len(GROUP_TILES) + 1)]
    return [(a, b) for a, b in zip(edges, edges[1:]) if b > a]


def step_kernel(dims, *refs):
    (layers, n_y, n_x, rows, depth, q_cols, kv_cols, ffn) = dims
    (hid_any, pos_any, freq_any, ga_any, gm_any, qg_any, kg_any, kc_ref, vc_ref,
     wq_ref, wk_ref, wv_ref, wo_ref, wg_ref, wu_ref, wd_ref,
     hid_out, new_out,
     wqkv, wo, wg, wu, wd, kbuf, vbuf, n_buf, stat, qkv_part, qkv_recv, q_rows, o_rows, attn_all,
     ar_part, ar_recv, h_mid, h_end, gu_part, gu_pair, gu_send, gu_recv, act_all, acc,
     pos_ref, freq_ref, ga_raw, gm_raw, qg_raw, kg_raw, ga_ref, gm_ref, qg_ref, kg_ref, slot_ref, part_scale, kv_rows, s_rows, p_rows,
     send_sem, recv_sem, local_sem) = refs
    batch = n_y * rows
    cols_qkv = q_cols + 2 * kv_cols
    q_heads = q_cols // HEAD_DIM
    kv_heads = kv_cols // HEAD_DIM
    group = q_heads // kv_heads
    model_dim = depth * n_x
    slots2 = kbuf.shape[2]
    n_seq = batch // n_x
    peers = n_y * n_x
    d_tiles, f_tiles, qkv_tiles = depth // TILE, ffn // TILE, cols_qkv // TILE

    y = lax.axis_index("y")
    x = lax.axis_index("x")
    chip = x // 2
    core = x % 2
    partner = 2 * chip + (1 - core)
    across = 2 * (1 - chip) + core
    diagonal = 2 * (1 - chip) + (1 - core)

    groups = split_tiles(f_tiles)
    at_qkv, at_first, at_attn, at_mid = 0, 1, 3, 4
    at_end = at_mid + d_tiles + 1
    at_mlp = at_end + d_tiles + 1

    def remote(src, dst, to_send, to_recv, to_y, to_x):
        return pltpu.make_async_remote_copy(
            src_ref=src, dst_ref=dst, send_sem=send_sem.at[to_send], recv_sem=recv_sem.at[to_recv],
            device_id={"y": to_y, "x": to_x}, device_id_type=MESH)

    def received(i, like):
        pltpu.make_async_copy(like, like, recv_sem.at[i]).wait()

    def delivered(i, like):
        pltpu.make_async_copy(like, like, send_sem.at[i]).wait()

    def each(first, last, body):
        def step(i, carry):
            body(i)
            return carry

        lax.fori_loop(first, last, step, 0)

    def tile_cols(t):
        return pl.ds(pl.multiple_of(t * TILE, TILE), TILE)

    def qkv_loads(layer):
        return [pltpu.make_async_copy(wq_ref.at[layer], wqkv.at[:, 0:q_cols], local_sem.at[0]),
                pltpu.make_async_copy(wk_ref.at[layer], wqkv.at[:, q_cols:q_cols + kv_cols], local_sem.at[1]),
                pltpu.make_async_copy(wv_ref.at[layer], wqkv.at[:, q_cols + kv_cols:cols_qkv], local_sem.at[2])]

    def o_loads(layer):
        return [pltpu.make_async_copy(wo_ref.at[layer], wo, local_sem.at[3])]

    def gate_up_loads(layer):
        return [pltpu.make_async_copy(src.at[layer], dst, local_sem.at[4 + i]) for i, (src, dst) in enumerate(((wg_ref, wg), (wu_ref, wu)))]

    def down_loads(layer):
        return [pltpu.make_async_copy(wd_ref.at[layer], wd, local_sem.at[6])]

    def cache_loads(layer):
        return [pltpu.make_async_copy(src.at[layer], dst.at[layer], local_sem.at[7 + i * layers + layer])
                for i, (src, dst) in enumerate(((kc_ref, kbuf), (vc_ref, vbuf)))]

    def start(copies):
        for copy in copies:
            copy.start()

    def finish(copies):
        for copy in copies:
            copy.wait()

    row_i = lax.broadcasted_iota(jnp.int32, (rows, HEAD_DIM), 0)
    lane_i = lax.broadcasted_iota(jnp.int32, (rows, HEAD_DIM), 1)

    def along_lanes(column, first_row):
        return jnp.sum(jnp.where(lane_i == row_i + first_row, column, 0.0), axis=0, keepdims=True)

    def along_rows(lanes, first_row):
        return jnp.sum(jnp.where(lane_i == row_i + first_row, lanes, 0.0), axis=1, keepdims=True)

    def local_norm(hidden_ref, gain, i):
        def block(b, lanes):
            vals = hidden_ref[b].astype(F32)
            sums = jnp.sum(vals * vals, axis=1, keepdims=True)
            n_buf[pl.ds(pl.multiple_of(b * rows, rows), rows), :] = (vals * lax.rsqrt(sums / depth + NORM_EPS) * gain).astype(BF16)
            return lanes + along_lanes(sums, b * rows)

        stat[i, 0] = lax.fori_loop(0, n_y, block, jnp.zeros((1, HEAD_DIM), F32))

    def corrections(i):
        total = stat[i, 0]
        for d in range(1, n_x):
            total = total + stat[i, d]
        scale = lax.rsqrt(total / model_dim + NORM_EPS)
        return lambda d: jnp.where(scale > 0.0, scale / lax.rsqrt(stat[i, d] / depth + NORM_EPS), 0.0)

    def all_reduce(i, base, tile_product, residual_ref, result_ref):
        send = 4 + 2 * i

        def scatter(t, d):
            cols = tile_cols(t)
            return remote(ar_part.at[i, (y + d) % n_y, :, cols], ar_recv.at[i, d, :, cols], send, base + t, (y + d) % n_y, x)

        def gather(t, d):
            mine = result_ref.at[y, :, tile_cols(t)]
            return remote(mine, mine, send + 1, base + d_tiles, (y + d) % n_y, x)

        def send_tile(t):
            ar_part[i, :, :, tile_cols(t)] = tile_product(tile_cols(t)).astype(BF16).reshape(n_y, rows, TILE)
            for d in (2, 3, 1):
                scatter(t, d).start()

        each(0, d_tiles, send_tile)

        def sum_tile(t):
            cols = tile_cols(t)
            received(base + t, ar_recv.at[i, 1:n_y, :, cols])
            total = ar_part[i, y, :, cols].astype(F32)
            for d in range(1, n_y):
                total = total + ar_recv[i, d, :, cols].astype(F32)
            new = (residual_ref[y, :, cols].astype(F32) + total.astype(BF16).astype(F32)).astype(BF16)
            result_ref[y, :, cols] = new
            for d in (2, 3, 1):
                gather(t, d).start()

        each(0, d_tiles, sum_tile)
        received(base + d_tiles, ar_recv.at[i, 1:n_y])

        def drain():
            delivered(send, ar_recv.at[i, 1:n_y])
            delivered(send + 1, ar_recv.at[i, 1:n_y])

        return drain

    def qkv_copies(first, last):
        cols = pl.ds(first * TILE, (last - first) * TILE)
        return [remote(qkv_part.at[(x + d) % n_x, :, cols], qkv_recv.at[d, :, cols], 0, at_qkv, y, (x + d) % n_x) for d in (2, 3, 1)]

    def sum_copies(i):
        return [remote(stat.at[i, 0], stat.at[i, d], 1 + 2 * i, at_first + i, y, (x + d) % n_x) for d in (2, 3, 1)]

    def attn_copy(d):
        return remote(attn_all.at[x], attn_all.at[x], 2, at_attn, y, (x + d) % n_x)

    def group_cols(g):
        return pl.ds(groups[g][0] * TILE, (groups[g][1] - groups[g][0]) * TILE)

    def pair_copy(g):
        cols = group_cols(g)
        return remote(gu_part.at[:, :, 1 - core, :, cols], gu_pair.at[:, :, :, cols], 9, at_mlp + g, y, partner)

    def across_copy(g):
        cols = group_cols(g)
        return remote(gu_send.at[:, :, cols], gu_recv.at[:, :, cols], 10, at_mlp + len(groups) + g, y, across)

    def act_copies(g):
        mine = act_all.at[x, :, group_cols(g)]
        return [remote(mine, mine, 11, at_mlp + 2 * len(groups) + g, y, to_x) for to_x in (diagonal, across, partner)]

    def project_qkv(first, last):
        def tile(t):
            cols = tile_cols(t)
            part = jnp.dot(n_buf[...], wqkv[:, cols], preferred_element_type=F32).astype(BF16)
            qkv_part[:, :, cols] = part.reshape(n_x, n_seq, TILE)

        each(first, last, tile)

    halves = ((0, (qkv_tiles + 1) // 2), ((qkv_tiles + 1) // 2, qkv_tiles))

    barrier = pltpu.get_barrier_semaphore()
    each(1, peers, lambda e: pl.semaphore_signal(
        barrier, inc=1, device_id={"y": (y + e // n_x) % n_y, "x": (x + e % n_x) % n_x}, device_id_type=MESH))
    small = [pltpu.make_async_copy(src, dst, local_sem.at[7 + 2 * layers + i]) for i, (src, dst) in enumerate((
        (hid_any, h_end), (ga_any, ga_raw), (gm_any, gm_raw), (qg_any, qg_raw), (kg_any, kg_raw), (pos_any, pos_ref), (freq_any, freq_ref)))]
    start(small)
    start(qkv_loads(0))
    finish(small)
    start(o_loads(0) + cache_loads(0) + gate_up_loads(0) + down_loads(0))
    for layer in range(1, layers):
        start(cache_loads(layer))
    for raw, wide in ((ga_raw, ga_ref), (gm_raw, gm_ref), (qg_raw, qg_ref), (kg_raw, kg_ref)):
        for layer in range(layers):
            wide[layer] = raw[...].astype(F32)[layer:layer + 1]
    local_norm(h_end, ga_ref[0], 0)
    q_rows[...] = jnp.zeros_like(q_rows)
    finish(qkv_loads(0))
    project_qkv(0, qkv_tiles)
    pl.semaphore_wait(barrier, peers - 1)
    start(sum_copies(0))
    for half in halves:
        start(qkv_copies(*half))

    my_pos = jnp.sum(
        jnp.where(lax.broadcasted_iota(jnp.int32, (n_seq, batch), 1) == lax.broadcasted_iota(jnp.int32, (n_seq, batch), 0) + x * n_seq,
                  pos_ref[...].astype(F32), 0.0), axis=1, keepdims=True)
    angles = my_pos * freq_ref[...]
    cos_tab = jnp.cos(angles)
    sin_tab = jnp.where(lax.broadcasted_iota(jnp.int32, (n_seq, HEAD_DIM), 1) < HEAD_DIM // 2, -1.0, 1.0) * jnp.sin(angles)
    slot_ref[...] = jnp.broadcast_to(my_pos.astype(jnp.int32), (n_seq, slots2)).reshape(slot_ref.shape)

    slot_row = lax.broadcasted_iota(jnp.int32, (slots2, HEAD_DIM), 0)
    slot_id = slot_row // kv_heads
    head_id = slot_row % kv_heads
    score_col = lax.broadcasted_iota(jnp.int32, (16, slots2), 1)
    score_head = lax.broadcasted_iota(jnp.int32, (16, slots2), 0) // group
    score_slot = score_col // kv_heads
    score_own = (score_col % kv_heads == score_head) | (score_head >= kv_heads)

    def run_layer(layer):
        more = layer + 1 < layers

        def reload(loads):
            @pl.when(more)
            def _():
                start(loads(layer + 1))

        reload(qkv_loads)
        received(at_first, stat.at[0, 1:n_x])
        correction = corrections(0)
        for d in range(n_x):
            part_scale[d] = jnp.broadcast_to(along_rows(correction(d), x * n_seq), (n_seq, TILE))
        received(at_qkv, qkv_recv.at[1:n_x])

        def projected(cols, scale_cols):
            total = qkv_part[x, :, cols].astype(F32) * part_scale[0, :, scale_cols]
            for d in range(1, n_x):
                total = total + qkv_recv[d, :, cols].astype(F32) * part_scale[d, :, scale_cols]
            return total.astype(BF16).astype(F32)

        for h in range(q_heads + kv_heads):
            vals = projected(pl.ds(h * HEAD_DIM, HEAD_DIM), pl.ds(0, HEAD_DIM))
            mean_sq = jnp.mean(vals * vals, axis=-1, keepdims=True)
            normed = vals * lax.rsqrt(mean_sq + NORM_EPS) * (qg_ref if h < q_heads else kg_ref)[layer]
            turned = (normed * cos_tab + pltpu.roll(normed, HEAD_DIM // 2, 1) * sin_tab).astype(BF16).astype(F32)
            if h < q_heads:
                q_rows[pl.ds(h, n_seq, stride=16), :] = turned
            else:
                new_out[layer, 0, h - q_heads] = turned
                kv_rows[0, h - q_heads] = turned.reshape(n_seq, 1, HEAD_DIM)
        for h in range(kv_heads):
            vals = projected(pl.ds(q_cols + kv_cols + h * HEAD_DIM, HEAD_DIM), pl.ds(0, HEAD_DIM))
            new_out[layer, 1, h] = vals
            kv_rows[1, h] = vals.reshape(n_seq, 1, HEAD_DIM)

        finish(cache_loads(layer))

        def update(i):
            for u in range(SEQS):
                b = i * SEQS + u
                hit = slot_id == slot_ref[b][:, :HEAD_DIM]
                for j, buf in enumerate((kbuf, vbuf)):
                    fresh = kv_rows[j, 0, b]
                    for h in range(1, kv_heads):
                        fresh = jnp.where(head_id == h, kv_rows[j, h, b], fresh)
                    buf[layer, b] = jnp.where(hit, fresh, buf[layer, b].astype(F32)).astype(BF16)

        each(0, n_seq // SEQS, update)
        for b in range(n_seq):
            q_b = q_rows[b * 16:(b + 1) * 16, :].astype(BF16)
            scores = lax.dot_general(q_b, kbuf[layer, b], (((1,), (1,)), ((), ())), preferred_element_type=F32) * (HEAD_DIM ** -0.5)
            s_rows[b * 16:(b + 1) * 16, :] = jnp.where(score_own & (score_slot <= slot_ref[b]), scores, -1e30)

        def softmax(i):
            block = pl.ds(pl.multiple_of(i * 16 * SEQS, 16 * SEQS), 16 * SEQS)
            scores = s_rows[block, :]
            e = jnp.exp(scores - jnp.max(scores, axis=1, keepdims=True))
            p_rows[block, :] = (e / jnp.sum(e, axis=1, keepdims=True)).astype(BF16)

        each(0, n_seq // SEQS, softmax)
        for b in range(n_seq):
            o_rows[b * 16:(b + 1) * 16, :] = jnp.dot(p_rows[b * 16:(b + 1) * 16, :], vbuf[layer, b], preferred_element_type=F32)
        for h in range(q_heads):
            attn_all[x, :, h * HEAD_DIM:(h + 1) * HEAD_DIM] = o_rows[pl.ds(h, n_seq, stride=16), :].astype(BF16)
        for d in (2, 3, 1):
            attn_copy(d).start()
        finish(o_loads(layer))
        delivered(0, qkv_recv.at[1:n_x])
        delivered(1, stat.at[0, 1:n_x])
        received(at_attn, attn_all.at[1:n_x])

        drain_mid = all_reduce(
            0, at_mid, lambda cols: jnp.dot(attn_all[...].reshape(batch, q_cols), wo[:, cols], preferred_element_type=F32), h_end, h_mid)
        reload(o_loads)

        local_norm(h_mid, gm_ref[layer], 1)
        start(sum_copies(1))
        finish(gate_up_loads(layer))

        def project(t):
            cols = tile_cols(t)
            gate = jnp.dot(n_buf[...], wg[:, cols], preferred_element_type=F32).astype(BF16)
            up = jnp.dot(n_buf[...], wu[:, cols], preferred_element_type=F32).astype(BF16)
            gu_part[0, :, :, :, cols] = gate.reshape(2, 2, rows, TILE)
            gu_part[1, :, :, :, cols] = up.reshape(2, 2, rows, TILE)

        def cross(g):
            cols = group_cols(g)
            received(at_mlp + g, gu_pair.at[:, :, :, cols])

            def tile(t):
                cols = tile_cols(t)
                pair = gu_part[:, 1 - chip, core, :, cols].astype(F32) * part_scale[0] + gu_pair[:, 1 - chip, :, cols].astype(F32) * part_scale[1]
                gu_send[:, :, cols] = pair.astype(BF16)

            each(*groups[g], tile)
            across_copy(g).start()

        def activate(g):
            received(at_mlp + len(groups) + g, gu_recv.at[:, :, group_cols(g)])

            def tile(t):
                cols = tile_cols(t)
                gate_up = (gu_part[:, chip, core, :, cols].astype(F32) * part_scale[2] + gu_pair[:, chip, :, cols].astype(F32) * part_scale[3]
                           + gu_recv[:, :, cols].astype(F32)).astype(BF16).astype(F32)
                act_all[x, :, cols] = (jax.nn.silu(gate_up[0]) * gate_up[1]).astype(BF16)

            each(*groups[g], tile)
            start(act_copies(g))

        for g in range(len(groups)):
            each(*groups[g], project)
            pair_copy(g).start()
            if g == 2:
                received(at_first + 1, stat.at[1, 1:n_x])
                correction = corrections(1)
                for i, (d, block) in enumerate(((0, across), (3 - 2 * core, across), (0, x), (3 - 2 * core, x))):
                    part_scale[i] = jnp.broadcast_to(along_rows(correction(d), block * rows), (rows, TILE))
            if g >= 2:
                cross(g - 2)
        reload(gate_up_loads)
        for g in range(max(len(groups) - 2, 0), len(groups)):
            cross(g)
        for g in range(len(groups)):
            activate(g)
        drain_mid()
        delivered(2, attn_all.at[1:n_x])
        finish(down_loads(layer))
        for g, (first, last) in enumerate(groups):
            cols = group_cols(g)
            received(at_mlp + 2 * len(groups) + g, act_all.at[1:n_x, :, cols])

            def down(t):
                part = jnp.dot(act_all[:, :, cols].reshape(batch, (last - first) * TILE), wd[cols, tile_cols(t)], preferred_element_type=F32)
                acc[:, tile_cols(t)] = acc[:, tile_cols(t)] + part if g else part

            each(0, d_tiles, down)
        reload(down_loads)
        drain_end = all_reduce(1, at_end, lambda cols: acc[:, cols], h_mid, h_end)

        @pl.when(more)
        def _():
            local_norm(h_end, ga_ref[layer + 1], 0)
            start(sum_copies(0))
            finish(qkv_loads(layer + 1))
            for half in halves:
                project_qkv(*half)
                start(qkv_copies(*half))

        drain_end()

        delivered(3, stat.at[1, 1:n_x])
        delivered(9, gu_pair)
        delivered(10, gu_recv)
        delivered(11, act_all.at[1:n_x])

    each(0, layers, run_layer)
    hid_out[...] = h_end[...]


def cache_kernel(dims, hid_ref, new_ref, pos_ref, kc_ref, vc_ref, hid_out, kc_out, vc_out, hid_buf, kbuf, vbuf, in_sem, out_sem):
    layers, n_seq, kv_heads = dims
    first = lax.axis_index("x") * n_seq
    arrive, leave = [], []
    for layer in range(layers):
        for src, dst in ((kc_ref, kbuf), (vc_ref, vbuf)):
            arrive.append(pltpu.make_async_copy(src.at[layer], dst.at[layer], in_sem.at[len(arrive)]))
            arrive[-1].start()
    hidden_in = pltpu.make_async_copy(hid_ref, hid_buf, in_sem.at[len(arrive)])
    hidden_in.start()
    for layer in range(layers):
        for i, (buf, dst) in enumerate(((kbuf, kc_out), (vbuf, vc_out))):
            arrive[2 * layer + i].wait()
            for b in range(n_seq):
                rows = jnp.concatenate([new_ref[layer, i, h, b:b + 1, :] for h in range(kv_heads)], axis=0)
                buf[layer, b, pos_ref[0, first + b]] = rows.astype(BF16)
            leave.append(pltpu.make_async_copy(buf.at[layer], dst.at[layer], out_sem.at[len(leave)]))
            leave[-1].start()
    hidden_in.wait()
    leave.append(pltpu.make_async_copy(hid_buf, hid_out, out_sem.at[len(leave)]))
    leave[-1].start()
    for copy in leave:
        copy.wait()


def solution(mesh):
    n_x, n_y = mesh.shape['x'], mesh.shape['y']
    cache_spec = P(None, ('dp', 'x'), None, 'y', None)
    col_spec = P(None, 'x', 'y')
    row_spec = P(None, 'y', 'x')
    in_specs = (P('dp', 'x'), P('dp'), cache_spec, cache_spec, P(None, 'x'), P(None, 'x'), P(), P(), col_spec, col_spec, col_spec, row_spec, col_spec, col_spec, row_spec)
    out_specs = (P('dp', 'x'), cache_spec, cache_spec)

    def device_step(hidden, positions, k_cache, v_cache, g_attn, g_mlp, q_gain, k_gain, w_q, w_k, w_v, w_o, w_gate, w_up, w_down):
        batch, depth = hidden.shape
        layers, n_seq, slots, kv_heads, _ = k_cache.shape
        q_cols, kv_cols, ffn = w_q.shape[2], w_k.shape[2], w_gate.shape[2]
        rows = batch // n_y
        slots2 = slots * kv_heads
        dims = (layers, n_y, n_x, rows, depth, q_cols, kv_cols, ffn)
        cols_qkv = q_cols + 2 * kv_cols
        vmem = pl.BlockSpec(memory_space=pltpu.VMEM)
        hbm = pl.BlockSpec(memory_space=pl.ANY)
        cache_shape = (layers, n_seq, slots2, HEAD_DIM)
        peers = n_y * n_x
        d_tiles, f_tiles = depth // TILE, ffn // TILE
        receives = 4 + 2 * (d_tiles + 1) + 3 * len(split_tiles(f_tiles))
        positions = positions.reshape(1, batch)
        new_hidden, new_rows = pl.pallas_call(
            functools.partial(step_kernel, dims),
            out_shape=(jax.ShapeDtypeStruct((n_y, rows, depth), BF16), jax.ShapeDtypeStruct((layers, 2, kv_heads, n_seq, HEAD_DIM), F32)),
            in_specs=[hbm] * 16,
            out_specs=(vmem, vmem),
            scratch_shapes=[
                pltpu.VMEM((depth, cols_qkv), BF16),
                pltpu.VMEM((q_cols, depth), BF16),
                pltpu.VMEM((depth, ffn), BF16),
                pltpu.VMEM((depth, ffn), BF16),
                pltpu.VMEM((ffn, depth), BF16),
                pltpu.VMEM(cache_shape, BF16),
                pltpu.VMEM(cache_shape, BF16),
                pltpu.VMEM((batch, depth), BF16),
                pltpu.VMEM((2, n_x, 1, HEAD_DIM), F32),
                pltpu.VMEM((n_x, n_seq, cols_qkv), BF16),
                pltpu.VMEM((n_x, n_seq, cols_qkv), BF16),
                pltpu.VMEM((16 * n_seq, HEAD_DIM), F32),
                pltpu.VMEM((16 * n_seq, HEAD_DIM), F32),
                pltpu.VMEM((n_x, n_seq, q_cols), BF16),
                pltpu.VMEM((2, n_y, rows, depth), BF16),
                pltpu.VMEM((2, n_y, rows, depth), BF16),
                pltpu.VMEM((n_y, rows, depth), BF16),
                pltpu.VMEM((n_y, rows, depth), BF16),
                pltpu.VMEM((2, 2, 2, rows, ffn), BF16),
                pltpu.VMEM((2, 2, rows, ffn), BF16),
                pltpu.VMEM((2, rows, ffn), BF16),
                pltpu.VMEM((2, rows, ffn), BF16),
                pltpu.VMEM((n_x, rows, ffn), BF16),
                pltpu.VMEM((batch, depth), F32),
                pltpu.VMEM((1, batch), jnp.int32),
                pltpu.VMEM((1, HEAD_DIM), F32),
                pltpu.VMEM(g_attn.shape, BF16),
                pltpu.VMEM(g_mlp.shape, BF16),
                pltpu.VMEM(q_gain.shape, BF16),
                pltpu.VMEM(k_gain.shape, BF16),
                pltpu.VMEM((layers, 1, depth), F32),
                pltpu.VMEM((layers, 1, depth), F32),
                pltpu.VMEM((layers, 1, HEAD_DIM), F32),
                pltpu.VMEM((layers, 1, HEAD_DIM), F32),
                pltpu.VMEM((n_seq, 1, slots2), jnp.int32),
                pltpu.VMEM((n_x, n_seq, TILE), F32),
                pltpu.VMEM((2, kv_heads, n_seq, 1, HEAD_DIM), F32),
                pltpu.VMEM((16 * n_seq, slots2), F32),
                pltpu.VMEM((16 * n_seq, slots2), BF16),
                pltpu.SemaphoreType.DMA((12,)),
                pltpu.SemaphoreType.DMA((receives,)),
                pltpu.SemaphoreType.DMA((14 + 2 * layers,)),
            ],
            compiler_params=pltpu.CompilerParams(collective_id=0, has_side_effects=True, vmem_limit_bytes=64 * 1024 * 1024 - 65536),
        )(hidden.reshape(n_y, rows, depth), positions, inverse_frequencies(), g_attn, g_mlp, q_gain, k_gain,
          k_cache.reshape(cache_shape), v_cache.reshape(cache_shape), w_q, w_k, w_v, w_o, w_gate, w_up, w_down)
        return pl.pallas_call(
            functools.partial(cache_kernel, (layers, n_seq, kv_heads)),
            out_shape=tuple(jax.ShapeDtypeStruct(a.shape, a.dtype) for a in (hidden, k_cache, v_cache)),
            in_specs=[hbm, vmem, pl.BlockSpec(memory_space=pltpu.SMEM), hbm, hbm],
            out_specs=(hbm, hbm, hbm),
            scratch_shapes=[
                pltpu.VMEM(hidden.shape, BF16),
                pltpu.VMEM(k_cache.shape, BF16),
                pltpu.VMEM(k_cache.shape, BF16),
                pltpu.SemaphoreType.DMA((2 * layers + 1,)),
                pltpu.SemaphoreType.DMA((2 * layers + 1,)),
            ],
            compiler_params=pltpu.CompilerParams(vmem_limit_bytes=64 * 1024 * 1024 - 65536),
        )(new_hidden.reshape(batch, depth), new_rows, positions, k_cache, v_cache)

    return jax.shard_map(device_step, mesh=mesh, in_specs=in_specs, out_specs=out_specs, check_vma=False)
```

```python
import functools

import jax
import jax.numpy as jnp
import numpy as np
from jax import lax
from jax.experimental import pallas as pl
from jax.experimental.pallas import tpu as pltpu
from jax.sharding import PartitionSpec as P

HEAD_DIM = 128
NORM_EPS = 1e-6
ROPE_BASE = 1000000.0
TILE = 256
GROUP_TILES = (3, 3, 3, 3, 3, 2)
SEQS = 4
MESH = pl.DeviceIdType.MESH
F32 = jnp.float32
BF16 = jnp.bfloat16


def inverse_frequencies():
    half_dim = HEAD_DIM // 2
    freqs = np.power(np.float32(ROPE_BASE), (-2.0 * np.arange(half_dim) / HEAD_DIM).astype(np.float32))
    return np.concatenate([freqs, freqs])[None].astype(np.float32)


def split_tiles(n_tiles):
    share = n_tiles / sum(GROUP_TILES)
    edges = [round(share * sum(GROUP_TILES[:i])) for i in range(len(GROUP_TILES) + 1)]
    return [(a, b) for a, b in zip(edges, edges[1:]) if b > a]


def step_kernel(dims, *refs):
    (layers, n_y, n_x, rows, depth, q_cols, kv_cols, ffn) = dims
    (hid_any, pos_any, freq_any, ga_any, gm_any, qg_any, kg_any, kc_ref, vc_ref,
     wq_ref, wk_ref, wv_ref, wo_ref, wg_ref, wu_ref, wd_ref,
     hid_out, new_out,
     wqkv, wo, wg, wu, wd, kbuf, vbuf, n_buf, stat, qkv_part, qkv_recv, q_rows, o_rows, attn_all,
     ar_part, ar_recv, h_mid, h_end, gu_part, gu_pair, gu_send, gu_recv, act_all, acc,
     pos_ref, freq_ref, ga_raw, gm_raw, qg_raw, kg_raw, ga_ref, gm_ref, qg_ref, kg_ref, slot_ref, part_scale, pair_scale, kv_rows, gu_direct, s_rows, p_rows,
     send_sem, recv_sem, local_sem) = refs
    batch = n_y * rows
    cols_qkv = q_cols + 2 * kv_cols
    q_heads = q_cols // HEAD_DIM
    kv_heads = kv_cols // HEAD_DIM
    group = q_heads // kv_heads
    model_dim = depth * n_x
    slots2 = kbuf.shape[2]
    n_seq = batch // n_x
    peers = n_y * n_x
    d_tiles, f_tiles, qkv_tiles = depth // TILE, ffn // TILE, cols_qkv // TILE

    y = lax.axis_index("y")
    x = lax.axis_index("x")
    chip = x // 2
    core = x % 2
    partner = 2 * chip + (1 - core)
    across = 2 * (1 - chip) + core
    diagonal = 2 * (1 - chip) + (1 - core)
    from_partner = 3 - 2 * core

    groups = split_tiles(f_tiles)
    at_qkv, at_first, at_attn, at_mid = 0, 1, 3, 4
    at_end = at_mid + d_tiles + 1
    at_mlp = at_end + d_tiles + 1

    def remote(src, dst, to_send, to_recv, to_y, to_x):
        return pltpu.make_async_remote_copy(
            src_ref=src, dst_ref=dst, send_sem=send_sem.at[to_send], recv_sem=recv_sem.at[to_recv],
            device_id={"y": to_y, "x": to_x}, device_id_type=MESH)

    def received(i, like):
        pltpu.make_async_copy(like, like, recv_sem.at[i]).wait()

    def delivered(i, like):
        pltpu.make_async_copy(like, like, send_sem.at[i]).wait()

    def each(first, last, body):
        def step(i, carry):
            body(i)
            return carry

        lax.fori_loop(first, last, step, 0)

    def tile_cols(t):
        return pl.ds(pl.multiple_of(t * TILE, TILE), TILE)

    def qkv_loads(layer):
        return [pltpu.make_async_copy(wq_ref.at[layer], wqkv.at[:, 0:q_cols], local_sem.at[0]),
                pltpu.make_async_copy(wk_ref.at[layer], wqkv.at[:, q_cols:q_cols + kv_cols], local_sem.at[1]),
                pltpu.make_async_copy(wv_ref.at[layer], wqkv.at[:, q_cols + kv_cols:cols_qkv], local_sem.at[2])]

    def o_loads(layer):
        return [pltpu.make_async_copy(wo_ref.at[layer], wo, local_sem.at[3])]

    def gate_up_loads(layer):
        return [pltpu.make_async_copy(src.at[layer], dst, local_sem.at[4 + i]) for i, (src, dst) in enumerate(((wg_ref, wg), (wu_ref, wu)))]

    def down_loads(layer):
        return [pltpu.make_async_copy(wd_ref.at[layer], wd, local_sem.at[6])]

    def cache_loads(layer):
        return [pltpu.make_async_copy(src.at[layer], dst.at[layer], local_sem.at[7 + i * layers + layer])
                for i, (src, dst) in enumerate(((kc_ref, kbuf), (vc_ref, vbuf)))]

    def start(copies):
        for copy in copies:
            copy.start()

    def finish(copies):
        for copy in copies:
            copy.wait()

    row_i = lax.broadcasted_iota(jnp.int32, (rows, HEAD_DIM), 0)
    lane_i = lax.broadcasted_iota(jnp.int32, (rows, HEAD_DIM), 1)

    def along_lanes(column, first_row):
        return jnp.sum(jnp.where(lane_i == row_i + first_row, column, 0.0), axis=0, keepdims=True)

    def along_rows(lanes, first_row):
        return jnp.sum(jnp.where(lane_i == row_i + first_row, lanes, 0.0), axis=1, keepdims=True)

    def local_norm(hidden_ref, gain, i):
        def block(b, lanes):
            vals = hidden_ref[b].astype(F32)
            sums = jnp.sum(vals * vals, axis=1, keepdims=True)
            n_buf[pl.ds(pl.multiple_of(b * rows, rows), rows), :] = (vals * lax.rsqrt(sums / depth + NORM_EPS) * gain).astype(BF16)
            return lanes + along_lanes(sums, b * rows)

        stat[i, 0] = lax.fori_loop(0, n_y, block, jnp.zeros((1, HEAD_DIM), F32))

    def corrections(i):
        total = stat[i, 0]
        for d in range(1, n_x):
            total = total + stat[i, d]
        scale = lax.rsqrt(total / model_dim + NORM_EPS)
        return lambda d: jnp.where(scale > 0.0, scale / lax.rsqrt(stat[i, d] / depth + NORM_EPS), 0.0)

    def all_reduce(i, base, tile_product, residual_ref, result_ref):
        send = 4 + 2 * i

        def scatter(t, d):
            cols = tile_cols(t)
            return remote(ar_part.at[i, (y + d) % n_y, :, cols], ar_recv.at[i, d, :, cols], send, base + t, (y + d) % n_y, x)

        def gather(t, d):
            mine = result_ref.at[y, :, tile_cols(t)]
            return remote(mine, mine, send + 1, base + d_tiles, (y + d) % n_y, x)

        def send_tile(t):
            ar_part[i, :, :, tile_cols(t)] = tile_product(tile_cols(t)).astype(BF16).reshape(n_y, rows, TILE)
            for d in (2, 3, 1):
                scatter(t, d).start()

        each(0, d_tiles, send_tile)

        def sum_tile(t):
            cols = tile_cols(t)
            received(base + t, ar_recv.at[i, 1:n_y, :, cols])
            total = ar_part[i, y, :, cols].astype(F32)
            for d in range(1, n_y):
                total = total + ar_recv[i, d, :, cols].astype(F32)
            new = (residual_ref[y, :, cols].astype(F32) + total.astype(BF16).astype(F32)).astype(BF16)
            result_ref[y, :, cols] = new
            for d in (2, 3, 1):
                gather(t, d).start()

        each(0, d_tiles, sum_tile)
        received(base + d_tiles, ar_recv.at[i, 1:n_y])

        def drain():
            delivered(send, ar_recv.at[i, 1:n_y])
            delivered(send + 1, ar_recv.at[i, 1:n_y])

        return drain

    def qkv_copies(first, last):
        cols = pl.ds(first * TILE, (last - first) * TILE)
        return [remote(qkv_part.at[(x + d) % n_x, :, cols], qkv_recv.at[d, :, cols], 0, at_qkv, y, (x + d) % n_x) for d in (2, 3, 1)]

    def sum_copies(i):
        return [remote(stat.at[i, 0], stat.at[i, d], 1 + 2 * i, at_first + i, y, (x + d) % n_x) for d in (2, 3, 1)]

    def attn_copy(d):
        return remote(attn_all.at[x], attn_all.at[x], 2, at_attn, y, (x + d) % n_x)

    def group_cols(g):
        return pl.ds(groups[g][0] * TILE, (groups[g][1] - groups[g][0]) * TILE)

    def pair_copy(g):
        cols = group_cols(g)
        return remote(gu_part.at[:, :, 1 - core, :, cols], gu_pair.at[:, :, :, cols], 9, at_mlp + g, y, partner)

    def across_copy(g):
        cols = group_cols(g)
        return remote(gu_send.at[:, :, cols], gu_recv.at[:, :, cols], 10, at_mlp + len(groups) + g, y, across)

    tail = len(groups) - 1
    before = groups[tail][0] * TILE

    def tail_copies():
        def copy(d):
            to_x = (x + d) % n_x
            return remote(gu_part.at[:, to_x // 2, to_x % 2, :, group_cols(tail)], gu_direct.at[d], 8, at_mlp + tail, y, to_x)

        return [copy(d) for d in (2, 3, 1)]

    def act_copies(g):
        mine = act_all.at[x, :, group_cols(g)]
        return [remote(mine, mine, 11, at_mlp + 2 * len(groups) + g, y, to_x) for to_x in (diagonal, across, partner)]

    def project_qkv(first, last):
        def tile(t):
            cols = tile_cols(t)
            part = jnp.dot(n_buf[...], wqkv[:, cols], preferred_element_type=F32).astype(BF16)
            qkv_part[:, :, cols] = part.reshape(n_x, n_seq, TILE)

        each(first, last, tile)

    halves = ((0, (qkv_tiles + 1) // 2), ((qkv_tiles + 1) // 2, qkv_tiles))

    small = [pltpu.make_async_copy(src, dst, local_sem.at[7 + 2 * layers + i]) for i, (src, dst) in enumerate((
        (hid_any, h_end), (ga_any, ga_raw), (gm_any, gm_raw), (qg_any, qg_raw), (kg_any, kg_raw), (pos_any, pos_ref), (freq_any, freq_ref)))]
    start(small)
    start(qkv_loads(0))
    barrier = pltpu.get_barrier_semaphore()
    each(1, peers, lambda e: pl.semaphore_signal(
        barrier, inc=1, device_id={"y": (y + e // n_x) % n_y, "x": (x + e % n_x) % n_x}, device_id_type=MESH))
    finish(small)
    for raw, wide in ((ga_raw, ga_ref), (gm_raw, gm_ref), (qg_raw, qg_ref), (kg_raw, kg_ref)):
        for layer in range(layers):
            wide[layer] = raw[...].astype(F32)[layer:layer + 1]
    local_norm(h_end, ga_ref[0], 0)
    q_rows[...] = jnp.zeros_like(q_rows)
    finish(qkv_loads(0))
    start(cache_loads(0) + o_loads(0) + gate_up_loads(0) + down_loads(0))
    for layer in range(1, layers):
        start(cache_loads(layer))
    project_qkv(0, qkv_tiles)
    pl.semaphore_wait(barrier, peers - 1)
    start(sum_copies(0))
    for half in halves:
        start(qkv_copies(*half))

    my_pos = jnp.sum(
        jnp.where(lax.broadcasted_iota(jnp.int32, (n_seq, batch), 1) == lax.broadcasted_iota(jnp.int32, (n_seq, batch), 0) + x * n_seq,
                  pos_ref[...].astype(F32), 0.0), axis=1, keepdims=True)
    angles = my_pos * freq_ref[...]
    cos_tab = jnp.cos(angles)
    sin_tab = jnp.where(lax.broadcasted_iota(jnp.int32, (n_seq, HEAD_DIM), 1) < HEAD_DIM // 2, -1.0, 1.0) * jnp.sin(angles)
    slot_ref[...] = jnp.broadcast_to(my_pos.astype(jnp.int32), (n_seq, slots2)).reshape(slot_ref.shape)

    slot_row = lax.broadcasted_iota(jnp.int32, (slots2, HEAD_DIM), 0)
    slot_id = slot_row // kv_heads
    head_id = slot_row % kv_heads
    score_col = lax.broadcasted_iota(jnp.int32, (16, slots2), 1)
    score_head = lax.broadcasted_iota(jnp.int32, (16, slots2), 0) // group
    score_slot = score_col // kv_heads
    score_own = (score_col % kv_heads == score_head) | (score_head >= kv_heads)

    def run_layer(layer):
        more = layer + 1 < layers

        def reload(loads):
            @pl.when(more)
            def _():
                start(loads(layer + 1))

        reload(qkv_loads)
        received(at_first, stat.at[0, 1:n_x])
        correction = corrections(0)
        for d in range(n_x):
            part_scale[d] = jnp.broadcast_to(along_rows(correction(d), x * n_seq), (n_seq, TILE))
        received(at_qkv, qkv_recv.at[1:n_x])

        def projected(cols, scale_cols):
            total = qkv_part[x, :, cols].astype(F32) * part_scale[0, :, scale_cols]
            for d in range(1, n_x):
                total = total + qkv_recv[d, :, cols].astype(F32) * part_scale[d, :, scale_cols]
            return total.astype(BF16).astype(F32)

        for h in range(q_heads + kv_heads):
            vals = projected(pl.ds(h * HEAD_DIM, HEAD_DIM), pl.ds(0, HEAD_DIM))
            mean_sq = jnp.mean(vals * vals, axis=-1, keepdims=True)
            normed = vals * lax.rsqrt(mean_sq + NORM_EPS) * (qg_ref if h < q_heads else kg_ref)[layer]
            turned = (normed * cos_tab + pltpu.roll(normed, HEAD_DIM // 2, 1) * sin_tab).astype(BF16).astype(F32)
            if h < q_heads:
                q_rows[pl.ds(h, n_seq, stride=16), :] = turned
            else:
                new_out[layer, 0, h - q_heads] = turned
                kv_rows[0, h - q_heads] = turned.reshape(n_seq, 1, HEAD_DIM)
        for h in range(kv_heads):
            vals = projected(pl.ds(q_cols + kv_cols + h * HEAD_DIM, HEAD_DIM), pl.ds(0, HEAD_DIM))
            new_out[layer, 1, h] = vals
            kv_rows[1, h] = vals.reshape(n_seq, 1, HEAD_DIM)

        finish(cache_loads(layer))

        def update(i):
            for u in range(SEQS):
                b = i * SEQS + u
                hit = slot_id == slot_ref[b][:, :HEAD_DIM]
                for j, buf in enumerate((kbuf, vbuf)):
                    fresh = kv_rows[j, 0, b]
                    for h in range(1, kv_heads):
                        fresh = jnp.where(head_id == h, kv_rows[j, h, b], fresh)
                    buf[layer, b] = jnp.where(hit, fresh, buf[layer, b].astype(F32)).astype(BF16)

        each(0, n_seq // SEQS, update)
        for b in range(n_seq):
            q_b = q_rows[b * 16:(b + 1) * 16, :].astype(BF16)
            scores = lax.dot_general(q_b, kbuf[layer, b], (((1,), (1,)), ((), ())), preferred_element_type=F32) * (HEAD_DIM ** -0.5)
            s_rows[b * 16:(b + 1) * 16, :] = jnp.where(score_own & (score_slot <= slot_ref[b]), scores, -1e30)

        def softmax(i):
            block = pl.ds(pl.multiple_of(i * 16 * SEQS, 16 * SEQS), 16 * SEQS)
            scores = s_rows[block, :]
            e = jnp.exp(scores - jnp.max(scores, axis=1, keepdims=True))
            p_rows[block, :] = (e / jnp.sum(e, axis=1, keepdims=True)).astype(BF16)

        each(0, n_seq // SEQS, softmax)
        for b in range(n_seq):
            o_rows[b * 16:(b + 1) * 16, :] = jnp.dot(p_rows[b * 16:(b + 1) * 16, :], vbuf[layer, b], preferred_element_type=F32)
        for h in range(q_heads):
            attn_all[x, :, h * HEAD_DIM:(h + 1) * HEAD_DIM] = o_rows[pl.ds(h, n_seq, stride=16), :].astype(BF16)
        for d in (2, 3, 1):
            attn_copy(d).start()
        finish(o_loads(layer))
        delivered(0, qkv_recv.at[1:n_x])
        delivered(1, stat.at[0, 1:n_x])
        received(at_attn, attn_all.at[1:n_x])

        drain_mid = all_reduce(
            0, at_mid, lambda cols: jnp.dot(attn_all[...].reshape(batch, q_cols), wo[:, cols], preferred_element_type=F32), h_end, h_mid)
        reload(o_loads)

        local_norm(h_mid, gm_ref[layer], 1)
        start(sum_copies(1))
        finish(gate_up_loads(layer))

        def project(t):
            cols = tile_cols(t)
            gate = jnp.dot(n_buf[...], wg[:, cols], preferred_element_type=F32).astype(BF16)
            up = jnp.dot(n_buf[...], wu[:, cols], preferred_element_type=F32).astype(BF16)
            gu_part[0, :, :, :, cols] = gate.reshape(2, 2, rows, TILE)
            gu_part[1, :, :, :, cols] = up.reshape(2, 2, rows, TILE)

        def cross(g):
            cols = group_cols(g)
            received(at_mlp + g, gu_pair.at[:, :, :, cols])

            def tile(t):
                cols = tile_cols(t)
                pair = gu_part[:, 1 - chip, core, :, cols].astype(F32) * pair_scale[0] + gu_pair[:, 1 - chip, :, cols].astype(F32) * pair_scale[1]
                gu_send[:, :, cols] = pair.astype(BF16)

            each(*groups[g], tile)
            across_copy(g).start()

        def activate(g):
            received(at_mlp + len(groups) + g, gu_recv.at[:, :, group_cols(g)])

            def tile(t):
                cols = tile_cols(t)
                gate_up = (gu_part[:, chip, core, :, cols].astype(F32) * part_scale[0] + gu_pair[:, chip, :, cols].astype(F32) * part_scale[from_partner]
                           + gu_recv[:, :, cols].astype(F32)).astype(BF16).astype(F32)
                act_all[x, :, cols] = (jax.nn.silu(gate_up[0]) * gate_up[1]).astype(BF16)

            each(*groups[g], tile)
            start(act_copies(g))

        def activate_tail():
            received(at_mlp + tail, gu_direct.at[1:n_x])

            def tile(t):
                cols = tile_cols(t)
                total = gu_part[:, chip, core, :, cols].astype(F32) * part_scale[0]
                for d in range(1, n_x):
                    total = total + gu_direct[d, :, :, tile_cols(t - groups[tail][0])].astype(F32) * part_scale[d]
                gate_up = total.astype(BF16).astype(F32)
                act_all[x, :, cols] = (jax.nn.silu(gate_up[0]) * gate_up[1]).astype(BF16)

            each(*groups[tail], tile)
            start(act_copies(tail))

        for g in range(len(groups)):
            each(*groups[g], project)
            if g < tail:
                pair_copy(g).start()
            else:
                start(tail_copies())
            if g == 2:
                received(at_first + 1, stat.at[1, 1:n_x])
                correction = corrections(1)
                for d in range(n_x):
                    part_scale[d] = jnp.broadcast_to(along_rows(correction(d), x * rows), (rows, TILE))
                for i, d in enumerate((0, from_partner)):
                    pair_scale[i] = jnp.broadcast_to(along_rows(correction(d), across * rows), (rows, TILE))
            if g >= 2:
                cross(g - 2)
        reload(gate_up_loads)
        cross(tail - 1)
        for g in range(tail):
            activate(g)
        activate_tail()
        drain_mid()
        delivered(2, attn_all.at[1:n_x])
        finish(down_loads(layer))
        for g, (first, last) in enumerate(groups):
            cols = group_cols(g)
            received(at_mlp + 2 * len(groups) + g, act_all.at[1:n_x, :, cols])

            def down(t):
                part = jnp.dot(act_all[:, :, cols].reshape(batch, (last - first) * TILE), wd[cols, tile_cols(t)], preferred_element_type=F32)
                acc[:, tile_cols(t)] = acc[:, tile_cols(t)] + part if g else part

            each(0, d_tiles, down)
        reload(down_loads)
        drain_end = all_reduce(1, at_end, lambda cols: acc[:, cols], h_mid, h_end)

        @pl.when(more)
        def _():
            local_norm(h_end, ga_ref[layer + 1], 0)
            start(sum_copies(0))
            finish(qkv_loads(layer + 1))
            for half in halves:
                project_qkv(*half)
                start(qkv_copies(*half))

        drain_end()

        delivered(3, stat.at[1, 1:n_x])
        delivered(8, gu_direct.at[1:n_x])
        delivered(9, gu_pair.at[:, :, :, 0:before])
        delivered(10, gu_recv.at[:, :, 0:before])
        delivered(11, act_all.at[1:n_x])

    each(0, layers, run_layer)
    hid_out[...] = h_end[...]


def cache_kernel(dims, hid_ref, new_ref, pos_ref, kc_ref, vc_ref, hid_out, kc_out, vc_out, hid_buf, kbuf, vbuf, in_sem, out_sem):
    layers, n_seq, kv_heads = dims
    first = lax.axis_index("x") * n_seq
    arrive, leave = [], []
    for layer in range(layers):
        for src, dst in ((kc_ref, kbuf), (vc_ref, vbuf)):
            arrive.append(pltpu.make_async_copy(src.at[layer], dst.at[layer], in_sem.at[len(arrive)]))
            arrive[-1].start()
    hidden_in = pltpu.make_async_copy(hid_ref, hid_buf, in_sem.at[len(arrive)])
    hidden_in.start()
    for layer in range(layers):
        for i, (buf, dst) in enumerate(((kbuf, kc_out), (vbuf, vc_out))):
            arrive[2 * layer + i].wait()
            for b in range(n_seq):
                rows = jnp.concatenate([new_ref[layer, i, h, b:b + 1, :] for h in range(kv_heads)], axis=0)
                buf[layer, b, pos_ref[0, first + b]] = rows.astype(BF16)
            leave.append(pltpu.make_async_copy(buf.at[layer], dst.at[layer], out_sem.at[len(leave)]))
            leave[-1].start()
    hidden_in.wait()
    leave.append(pltpu.make_async_copy(hid_buf, hid_out, out_sem.at[len(leave)]))
    leave[-1].start()
    for copy in leave:
        copy.wait()


def solution(mesh):
    n_x, n_y = mesh.shape['x'], mesh.shape['y']
    cache_spec = P(None, ('dp', 'x'), None, 'y', None)
    col_spec = P(None, 'x', 'y')
    row_spec = P(None, 'y', 'x')
    in_specs = (P('dp', 'x'), P('dp'), cache_spec, cache_spec, P(None, 'x'), P(None, 'x'), P(), P(), col_spec, col_spec, col_spec, row_spec, col_spec, col_spec, row_spec)
    out_specs = (P('dp', 'x'), cache_spec, cache_spec)

    def device_step(hidden, positions, k_cache, v_cache, g_attn, g_mlp, q_gain, k_gain, w_q, w_k, w_v, w_o, w_gate, w_up, w_down):
        batch, depth = hidden.shape
        layers, n_seq, slots, kv_heads, _ = k_cache.shape
        q_cols, kv_cols, ffn = w_q.shape[2], w_k.shape[2], w_gate.shape[2]
        rows = batch // n_y
        slots2 = slots * kv_heads
        dims = (layers, n_y, n_x, rows, depth, q_cols, kv_cols, ffn)
        cols_qkv = q_cols + 2 * kv_cols
        vmem = pl.BlockSpec(memory_space=pltpu.VMEM)
        hbm = pl.BlockSpec(memory_space=pl.ANY)
        cache_shape = (layers, n_seq, slots2, HEAD_DIM)
        peers = n_y * n_x
        d_tiles, f_tiles = depth // TILE, ffn // TILE
        receives = 4 + 2 * (d_tiles + 1) + 3 * len(split_tiles(f_tiles))
        positions = positions.reshape(1, batch)
        new_hidden, new_rows = pl.pallas_call(
            functools.partial(step_kernel, dims),
            out_shape=(jax.ShapeDtypeStruct((n_y, rows, depth), BF16), jax.ShapeDtypeStruct((layers, 2, kv_heads, n_seq, HEAD_DIM), F32)),
            in_specs=[hbm] * 16,
            out_specs=(vmem, vmem),
            scratch_shapes=[
                pltpu.VMEM((depth, cols_qkv), BF16),
                pltpu.VMEM((q_cols, depth), BF16),
                pltpu.VMEM((depth, ffn), BF16),
                pltpu.VMEM((depth, ffn), BF16),
                pltpu.VMEM((ffn, depth), BF16),
                pltpu.VMEM(cache_shape, BF16),
                pltpu.VMEM(cache_shape, BF16),
                pltpu.VMEM((batch, depth), BF16),
                pltpu.VMEM((2, n_x, 1, HEAD_DIM), F32),
                pltpu.VMEM((n_x, n_seq, cols_qkv), BF16),
                pltpu.VMEM((n_x, n_seq, cols_qkv), BF16),
                pltpu.VMEM((16 * n_seq, HEAD_DIM), F32),
                pltpu.VMEM((16 * n_seq, HEAD_DIM), F32),
                pltpu.VMEM((n_x, n_seq, q_cols), BF16),
                pltpu.VMEM((2, n_y, rows, depth), BF16),
                pltpu.VMEM((2, n_y, rows, depth), BF16),
                pltpu.VMEM((n_y, rows, depth), BF16),
                pltpu.VMEM((n_y, rows, depth), BF16),
                pltpu.VMEM((2, 2, 2, rows, ffn), BF16),
                pltpu.VMEM((2, 2, rows, ffn), BF16),
                pltpu.VMEM((2, rows, ffn), BF16),
                pltpu.VMEM((2, rows, ffn), BF16),
                pltpu.VMEM((n_x, rows, ffn), BF16),
                pltpu.VMEM((batch, depth), F32),
                pltpu.VMEM((1, batch), jnp.int32),
                pltpu.VMEM((1, HEAD_DIM), F32),
                pltpu.VMEM(g_attn.shape, BF16),
                pltpu.VMEM(g_mlp.shape, BF16),
                pltpu.VMEM(q_gain.shape, BF16),
                pltpu.VMEM(k_gain.shape, BF16),
                pltpu.VMEM((layers, 1, depth), F32),
                pltpu.VMEM((layers, 1, depth), F32),
                pltpu.VMEM((layers, 1, HEAD_DIM), F32),
                pltpu.VMEM((layers, 1, HEAD_DIM), F32),
                pltpu.VMEM((n_seq, 1, slots2), jnp.int32),
                pltpu.VMEM((n_x, n_seq, TILE), F32),
                pltpu.VMEM((2, rows, TILE), F32),
                pltpu.VMEM((2, kv_heads, n_seq, 1, HEAD_DIM), F32),
                pltpu.VMEM((n_x, 2, rows, (split_tiles(f_tiles)[-1][1] - split_tiles(f_tiles)[-1][0]) * TILE), BF16),
                pltpu.VMEM((16 * n_seq, slots2), F32),
                pltpu.VMEM((16 * n_seq, slots2), BF16),
                pltpu.SemaphoreType.DMA((12,)),
                pltpu.SemaphoreType.DMA((receives,)),
                pltpu.SemaphoreType.DMA((14 + 2 * layers,)),
            ],
            compiler_params=pltpu.CompilerParams(collective_id=0, has_side_effects=True, vmem_limit_bytes=64 * 1024 * 1024 - 65536),
        )(hidden.reshape(n_y, rows, depth), positions, inverse_frequencies(), g_attn, g_mlp, q_gain, k_gain,
          k_cache.reshape(cache_shape), v_cache.reshape(cache_shape), w_q, w_k, w_v, w_o, w_gate, w_up, w_down)
        return pl.pallas_call(
            functools.partial(cache_kernel, (layers, n_seq, kv_heads)),
            out_shape=tuple(jax.ShapeDtypeStruct(a.shape, a.dtype) for a in (hidden, k_cache, v_cache)),
            in_specs=[hbm, vmem, pl.BlockSpec(memory_space=pltpu.SMEM), hbm, hbm],
            out_specs=(hbm, hbm, hbm),
            scratch_shapes=[
                pltpu.VMEM(hidden.shape, BF16),
                pltpu.VMEM(k_cache.shape, BF16),
                pltpu.VMEM(k_cache.shape, BF16),
                pltpu.SemaphoreType.DMA((2 * layers + 1,)),
                pltpu.SemaphoreType.DMA((2 * layers + 1,)),
            ],
            compiler_params=pltpu.CompilerParams(vmem_limit_bytes=64 * 1024 * 1024 - 65536),
        )(new_hidden.reshape(batch, depth), new_rows, positions, k_cache, v_cache)

    return jax.shard_map(device_step, mesh=mesh, in_specs=in_specs, out_specs=out_specs, check_vma=False)
```

```python
import functools

import jax
import jax.numpy as jnp
import numpy as np
from jax import lax
from jax.experimental import pallas as pl
from jax.experimental.pallas import tpu as pltpu
from jax.sharding import PartitionSpec as P

HEAD_DIM = 128
NORM_EPS = 1e-6
ROPE_BASE = 1000000.0
TILE = 256
GROUP_TILES = (3, 3, 3, 3, 3, 2)
SEQS = 4
MESH = pl.DeviceIdType.MESH
F32 = jnp.float32
BF16 = jnp.bfloat16


def inverse_frequencies():
    half_dim = HEAD_DIM // 2
    freqs = np.power(np.float32(ROPE_BASE), (-2.0 * np.arange(half_dim) / HEAD_DIM).astype(np.float32))
    return np.concatenate([freqs, freqs])[None].astype(np.float32)


def split_tiles(n_tiles):
    share = n_tiles / sum(GROUP_TILES)
    edges = [round(share * sum(GROUP_TILES[:i])) for i in range(len(GROUP_TILES) + 1)]
    return [(a, b) for a, b in zip(edges, edges[1:]) if b > a]


def step_kernel(dims, *refs):
    (layers, n_y, n_x, rows, depth, q_cols, kv_cols, ffn) = dims
    (hid_any, pos_any, freq_any, ga_any, gm_any, qg_any, kg_any, kc_ref, vc_ref,
     wq_ref, wk_ref, wv_ref, wo_ref, wg_ref, wu_ref, wd_ref,
     hid_out, new_out,
     wqkv, wo, wg, wu, wd, kbuf, vbuf, n_buf, stat, qkv_part, qkv_recv, q_rows, o_rows, attn_all,
     ar_part, ar_recv, h_mid, h_end, gu_part, gu_pair, gu_send, gu_recv, act_all, acc,
     pos_ref, freq_ref, ga_raw, gm_raw, qg_raw, kg_raw, ga_ref, gm_ref, qg_ref, kg_ref, slot_ref, part_scale, kv_rows, s_rows, p_rows,
     send_sem, recv_sem, local_sem) = refs
    batch = n_y * rows
    cols_qkv = q_cols + 2 * kv_cols
    q_heads = q_cols // HEAD_DIM
    kv_heads = kv_cols // HEAD_DIM
    group = q_heads // kv_heads
    model_dim = depth * n_x
    slots2 = kbuf.shape[2]
    n_seq = batch // n_x
    peers = n_y * n_x
    d_tiles, f_tiles, qkv_tiles = depth // TILE, ffn // TILE, cols_qkv // TILE

    y = lax.axis_index("y")
    x = lax.axis_index("x")
    chip = x // 2
    core = x % 2
    partner = 2 * chip + (1 - core)
    across = 2 * (1 - chip) + core
    diagonal = 2 * (1 - chip) + (1 - core)

    groups = split_tiles(f_tiles)
    at_qkv, at_first, at_attn, at_mid = 0, 1, 3, 4
    at_end = at_mid + d_tiles + 1
    at_mlp = at_end + d_tiles + 1

    def remote(src, dst, to_send, to_recv, to_y, to_x):
        return pltpu.make_async_remote_copy(
            src_ref=src, dst_ref=dst, send_sem=send_sem.at[to_send], recv_sem=recv_sem.at[to_recv],
            device_id={"y": to_y, "x": to_x}, device_id_type=MESH)

    def received(i, like):
        pltpu.make_async_copy(like, like, recv_sem.at[i]).wait()

    def delivered(i, like):
        pltpu.make_async_copy(like, like, send_sem.at[i]).wait()

    def each(first, last, body):
        def step(i, carry):
            body(i)
            return carry

        lax.fori_loop(first, last, step, 0)

    def tile_cols(t):
        return pl.ds(pl.multiple_of(t * TILE, TILE), TILE)

    def qkv_loads(layer):
        return [pltpu.make_async_copy(wq_ref.at[layer], wqkv.at[:, 0:q_cols], local_sem.at[0]),
                pltpu.make_async_copy(wk_ref.at[layer], wqkv.at[:, q_cols:q_cols + kv_cols], local_sem.at[1]),
                pltpu.make_async_copy(wv_ref.at[layer], wqkv.at[:, q_cols + kv_cols:cols_qkv], local_sem.at[2])]

    def o_loads(layer):
        return [pltpu.make_async_copy(wo_ref.at[layer], wo, local_sem.at[3])]

    def gate_up_loads(layer):
        return [pltpu.make_async_copy(src.at[layer], dst, local_sem.at[4 + i]) for i, (src, dst) in enumerate(((wg_ref, wg), (wu_ref, wu)))]

    def down_loads(layer):
        return [pltpu.make_async_copy(wd_ref.at[layer], wd, local_sem.at[6])]

    def cache_loads(layer):
        return [pltpu.make_async_copy(src.at[layer], dst.at[layer], local_sem.at[7 + i * layers + layer])
                for i, (src, dst) in enumerate(((kc_ref, kbuf), (vc_ref, vbuf)))]

    def start(copies):
        for copy in copies:
            copy.start()

    def finish(copies):
        for copy in copies:
            copy.wait()

    row_i = lax.broadcasted_iota(jnp.int32, (rows, HEAD_DIM), 0)
    lane_i = lax.broadcasted_iota(jnp.int32, (rows, HEAD_DIM), 1)

    def along_lanes(column, first_row):
        return jnp.sum(jnp.where(lane_i == row_i + first_row, column, 0.0), axis=0, keepdims=True)

    def along_rows(lanes, first_row):
        return jnp.sum(jnp.where(lane_i == row_i + first_row, lanes, 0.0), axis=1, keepdims=True)

    def local_norm(hidden_ref, gain, i):
        def block(b, lanes):
            vals = hidden_ref[b].astype(F32)
            sums = jnp.sum(vals * vals, axis=1, keepdims=True)
            n_buf[pl.ds(pl.multiple_of(b * rows, rows), rows), :] = (vals * lax.rsqrt(sums / depth + NORM_EPS) * gain).astype(BF16)
            return lanes + along_lanes(sums, b * rows)

        stat[i, 0] = lax.fori_loop(0, n_y, block, jnp.zeros((1, HEAD_DIM), F32))

    def corrections(i):
        total = stat[i, 0]
        for d in range(1, n_x):
            total = total + stat[i, d]
        scale = lax.rsqrt(total / model_dim + NORM_EPS)
        return lambda d: jnp.where(scale > 0.0, scale / lax.rsqrt(stat[i, d] / depth + NORM_EPS), 0.0)

    def all_reduce(i, base, tile_product, residual_ref, result_ref):
        send = 4 + 2 * i

        def scatter(t, d):
            cols = tile_cols(t)
            return remote(ar_part.at[i, (y + d) % n_y, :, cols], ar_recv.at[i, d, :, cols], send, base + t, (y + d) % n_y, x)

        def gather(t, d):
            mine = result_ref.at[y, :, tile_cols(t)]
            return remote(mine, mine, send + 1, base + d_tiles, (y + d) % n_y, x)

        def send_tile(t):
            ar_part[i, :, :, tile_cols(t)] = tile_product(tile_cols(t)).astype(BF16).reshape(n_y, rows, TILE)
            for d in (2, 3, 1):
                scatter(t, d).start()

        each(0, d_tiles, send_tile)

        def sum_tile(t):
            cols = tile_cols(t)
            received(base + t, ar_recv.at[i, 1:n_y, :, cols])
            total = ar_part[i, y, :, cols].astype(F32)
            for d in range(1, n_y):
                total = total + ar_recv[i, d, :, cols].astype(F32)
            new = (residual_ref[y, :, cols].astype(F32) + total.astype(BF16).astype(F32)).astype(BF16)
            result_ref[y, :, cols] = new
            for d in (2, 3, 1):
                gather(t, d).start()

        each(0, d_tiles, sum_tile)
        received(base + d_tiles, ar_recv.at[i, 1:n_y])

        def drain():
            delivered(send, ar_recv.at[i, 1:n_y])
            delivered(send + 1, ar_recv.at[i, 1:n_y])

        return drain

    def qkv_copies(first, last):
        cols = pl.ds(first * TILE, (last - first) * TILE)
        return [remote(qkv_part.at[(x + d) % n_x, :, cols], qkv_recv.at[d, :, cols], 0, at_qkv, y, (x + d) % n_x) for d in (2, 3, 1)]

    def sum_copies(i):
        return [remote(stat.at[i, 0], stat.at[i, d], 1 + 2 * i, at_first + i, y, (x + d) % n_x) for d in (2, 3, 1)]

    def attn_copy(d):
        return remote(attn_all.at[x], attn_all.at[x], 2, at_attn, y, (x + d) % n_x)

    def group_cols(g):
        return pl.ds(groups[g][0] * TILE, (groups[g][1] - groups[g][0]) * TILE)

    def pair_copy(g):
        cols = group_cols(g)
        return remote(gu_part.at[:, :, 1 - core, :, cols], gu_pair.at[:, :, :, cols], 9, at_mlp + g, y, partner)

    def across_copy(g):
        cols = group_cols(g)
        return remote(gu_send.at[:, :, cols], gu_recv.at[:, :, cols], 10, at_mlp + len(groups) + g, y, across)

    tail = len(groups) - 1
    at_act = at_mlp + 2 * len(groups)
    at_crossed = at_act + len(groups)

    def act_copies(g):
        mine = act_all.at[x, :, group_cols(g)]
        crossing = remote(mine, mine, 11, at_crossed + g if g < tail else at_act + g, y, across)
        return [crossing] + [remote(mine, mine, 11, at_act + g, y, to_x) for to_x in ((partner,) if g < tail else (diagonal, partner))]

    def pass_on(g):
        theirs = act_all.at[across, :, group_cols(g)]
        received(at_crossed + g, theirs)
        remote(theirs, theirs, 11, at_act + g, y, partner).start()

    def project_qkv(first, last):
        def tile(t):
            cols = tile_cols(t)
            part = jnp.dot(n_buf[...], wqkv[:, cols], preferred_element_type=F32).astype(BF16)
            qkv_part[:, :, cols] = part.reshape(n_x, n_seq, TILE)

        each(first, last, tile)

    halves = ((0, (qkv_tiles + 1) // 2), ((qkv_tiles + 1) // 2, qkv_tiles))

    small = [pltpu.make_async_copy(src, dst, local_sem.at[7 + 2 * layers + i]) for i, (src, dst) in enumerate((
        (hid_any, h_end), (ga_any, ga_raw), (gm_any, gm_raw), (qg_any, qg_raw), (kg_any, kg_raw), (pos_any, pos_ref), (freq_any, freq_ref)))]
    start(small)
    start(qkv_loads(0))
    barrier = pltpu.get_barrier_semaphore()
    each(1, peers, lambda e: pl.semaphore_signal(
        barrier, inc=1, device_id={"y": (y + e // n_x) % n_y, "x": (x + e % n_x) % n_x}, device_id_type=MESH))
    finish(small)
    for raw, wide in ((ga_raw, ga_ref), (gm_raw, gm_ref), (qg_raw, qg_ref), (kg_raw, kg_ref)):
        for layer in range(layers):
            wide[layer] = raw[...].astype(F32)[layer:layer + 1]
    local_norm(h_end, ga_ref[0], 0)
    q_rows[...] = jnp.zeros_like(q_rows)
    finish(qkv_loads(0))
    start(cache_loads(0) + o_loads(0) + gate_up_loads(0) + down_loads(0))
    for layer in range(1, layers):
        start(cache_loads(layer))
    project_qkv(0, qkv_tiles)
    pl.semaphore_wait(barrier, peers - 1)
    start(sum_copies(0))
    for half in halves:
        start(qkv_copies(*half))

    my_pos = jnp.sum(
        jnp.where(lax.broadcasted_iota(jnp.int32, (n_seq, batch), 1) == lax.broadcasted_iota(jnp.int32, (n_seq, batch), 0) + x * n_seq,
                  pos_ref[...].astype(F32), 0.0), axis=1, keepdims=True)
    angles = my_pos * freq_ref[...]
    cos_tab = jnp.cos(angles)
    sin_tab = jnp.where(lax.broadcasted_iota(jnp.int32, (n_seq, HEAD_DIM), 1) < HEAD_DIM // 2, -1.0, 1.0) * jnp.sin(angles)
    slot_ref[...] = jnp.broadcast_to(my_pos.astype(jnp.int32), (n_seq, slots2)).reshape(slot_ref.shape)

    slot_row = lax.broadcasted_iota(jnp.int32, (slots2, HEAD_DIM), 0)
    slot_id = slot_row // kv_heads
    head_id = slot_row % kv_heads
    score_col = lax.broadcasted_iota(jnp.int32, (16, slots2), 1)
    score_head = lax.broadcasted_iota(jnp.int32, (16, slots2), 0) // group
    score_slot = score_col // kv_heads
    score_own = (score_col % kv_heads == score_head) | (score_head >= kv_heads)

    def run_layer(layer):
        more = layer + 1 < layers

        def reload(loads):
            @pl.when(more)
            def _():
                start(loads(layer + 1))

        reload(qkv_loads)
        received(at_first, stat.at[0, 1:n_x])
        correction = corrections(0)
        for d in range(n_x):
            part_scale[d] = jnp.broadcast_to(along_rows(correction(d), x * n_seq), (n_seq, TILE))
        received(at_qkv, qkv_recv.at[1:n_x])

        def projected(cols, scale_cols):
            total = qkv_part[x, :, cols].astype(F32) * part_scale[0, :, scale_cols]
            for d in range(1, n_x):
                total = total + qkv_recv[d, :, cols].astype(F32) * part_scale[d, :, scale_cols]
            return total.astype(BF16).astype(F32)

        for h in range(q_heads + kv_heads):
            vals = projected(pl.ds(h * HEAD_DIM, HEAD_DIM), pl.ds(0, HEAD_DIM))
            mean_sq = jnp.mean(vals * vals, axis=-1, keepdims=True)
            normed = vals * lax.rsqrt(mean_sq + NORM_EPS) * (qg_ref if h < q_heads else kg_ref)[layer]
            turned = (normed * cos_tab + pltpu.roll(normed, HEAD_DIM // 2, 1) * sin_tab).astype(BF16).astype(F32)
            if h < q_heads:
                q_rows[pl.ds(h, n_seq, stride=16), :] = turned
            else:
                new_out[layer, 0, h - q_heads] = turned
                kv_rows[0, h - q_heads] = turned.reshape(n_seq, 1, HEAD_DIM)
        for h in range(kv_heads):
            vals = projected(pl.ds(q_cols + kv_cols + h * HEAD_DIM, HEAD_DIM), pl.ds(0, HEAD_DIM))
            new_out[layer, 1, h] = vals
            kv_rows[1, h] = vals.reshape(n_seq, 1, HEAD_DIM)

        finish(cache_loads(layer))

        def update(i):
            for u in range(SEQS):
                b = i * SEQS + u
                hit = slot_id == slot_ref[b][:, :HEAD_DIM]
                for j, buf in enumerate((kbuf, vbuf)):
                    fresh = kv_rows[j, 0, b]
                    for h in range(1, kv_heads):
                        fresh = jnp.where(head_id == h, kv_rows[j, h, b], fresh)
                    buf[layer, b] = jnp.where(hit, fresh, buf[layer, b].astype(F32)).astype(BF16)

        each(0, n_seq // SEQS, update)
        for b in range(n_seq):
            q_b = q_rows[b * 16:(b + 1) * 16, :].astype(BF16)
            scores = lax.dot_general(q_b, kbuf[layer, b], (((1,), (1,)), ((), ())), preferred_element_type=F32) * (HEAD_DIM ** -0.5)
            s_rows[b * 16:(b + 1) * 16, :] = jnp.where(score_own & (score_slot <= slot_ref[b]), scores, -1e30)

        def softmax(i):
            block = pl.ds(pl.multiple_of(i * 16 * SEQS, 16 * SEQS), 16 * SEQS)
            scores = s_rows[block, :]
            e = jnp.exp(scores - jnp.max(scores, axis=1, keepdims=True))
            p_rows[block, :] = (e / jnp.sum(e, axis=1, keepdims=True)).astype(BF16)

        each(0, n_seq // SEQS, softmax)
        for b in range(n_seq):
            o_rows[b * 16:(b + 1) * 16, :] = jnp.dot(p_rows[b * 16:(b + 1) * 16, :], vbuf[layer, b], preferred_element_type=F32)
        for h in range(q_heads):
            attn_all[x, :, h * HEAD_DIM:(h + 1) * HEAD_DIM] = o_rows[pl.ds(h, n_seq, stride=16), :].astype(BF16)
        for d in (2, 3, 1):
            attn_copy(d).start()
        finish(o_loads(layer))
        delivered(0, qkv_recv.at[1:n_x])
        delivered(1, stat.at[0, 1:n_x])
        received(at_attn, attn_all.at[1:n_x])

        drain_mid = all_reduce(
            0, at_mid, lambda cols: jnp.dot(attn_all[...].reshape(batch, q_cols), wo[:, cols], preferred_element_type=F32), h_end, h_mid)
        reload(o_loads)

        local_norm(h_mid, gm_ref[layer], 1)
        start(sum_copies(1))
        finish(gate_up_loads(layer))

        def project(t):
            cols = tile_cols(t)
            gate = jnp.dot(n_buf[...], wg[:, cols], preferred_element_type=F32).astype(BF16)
            up = jnp.dot(n_buf[...], wu[:, cols], preferred_element_type=F32).astype(BF16)
            gu_part[0, :, :, :, cols] = gate.reshape(2, 2, rows, TILE)
            gu_part[1, :, :, :, cols] = up.reshape(2, 2, rows, TILE)

        def cross(g):
            cols = group_cols(g)
            received(at_mlp + g, gu_pair.at[:, :, :, cols])

            def tile(t):
                cols = tile_cols(t)
                pair = gu_part[:, 1 - chip, core, :, cols].astype(F32) * part_scale[0] + gu_pair[:, 1 - chip, :, cols].astype(F32) * part_scale[1]
                gu_send[:, :, cols] = pair.astype(BF16)

            each(*groups[g], tile)
            across_copy(g).start()

        def activate(g):
            received(at_mlp + len(groups) + g, gu_recv.at[:, :, group_cols(g)])

            def tile(t):
                cols = tile_cols(t)
                gate_up = (gu_part[:, chip, core, :, cols].astype(F32) * part_scale[2] + gu_pair[:, chip, :, cols].astype(F32) * part_scale[3]
                           + gu_recv[:, :, cols].astype(F32)).astype(BF16).astype(F32)
                act_all[x, :, cols] = (jax.nn.silu(gate_up[0]) * gate_up[1]).astype(BF16)

            each(*groups[g], tile)
            start(act_copies(g))

        for g in range(len(groups)):
            each(*groups[g], project)
            pair_copy(g).start()
            if g == 2:
                received(at_first + 1, stat.at[1, 1:n_x])
                correction = corrections(1)
                for i, (d, block) in enumerate(((0, across), (3 - 2 * core, across), (0, x), (3 - 2 * core, x))):
                    part_scale[i] = jnp.broadcast_to(along_rows(correction(d), block * rows), (rows, TILE))
            if g >= 2:
                cross(g - 2)
        reload(gate_up_loads)
        for g in range(max(len(groups) - 2, 0), len(groups)):
            cross(g)
        def down(g):
            cols = group_cols(g)
            first, last = groups[g]
            received(at_act + g, act_all.at[1:3 if g < tail else n_x, :, cols])

            def tile(t):
                part = jnp.dot(act_all[:, :, cols].reshape(batch, (last - first) * TILE), wd[cols, tile_cols(t)], preferred_element_type=F32)
                acc[:, tile_cols(t)] = acc[:, tile_cols(t)] + part if g else part

            each(0, d_tiles, tile)

        for g in range(len(groups)):
            activate(g)
            if g >= 3:
                pass_on(g - 3)
        drain_mid()
        delivered(2, attn_all.at[1:n_x])
        finish(down_loads(layer))
        waiting = list(range(max(len(groups) - 3, 0), tail))
        for g in range(len(groups)):
            if waiting:
                pass_on(waiting.pop(0))
            down(g)
        reload(down_loads)
        drain_end = all_reduce(1, at_end, lambda cols: acc[:, cols], h_mid, h_end)

        @pl.when(more)
        def _():
            local_norm(h_end, ga_ref[layer + 1], 0)
            start(sum_copies(0))
            finish(qkv_loads(layer + 1))
            for half in halves:
                project_qkv(*half)
                start(qkv_copies(*half))

        drain_end()

        delivered(3, stat.at[1, 1:n_x])
        delivered(9, gu_pair)
        delivered(10, gu_recv)
        delivered(11, act_all.at[1:n_x])

    each(0, layers, run_layer)
    hid_out[...] = h_end[...]


def cache_kernel(dims, hid_ref, new_ref, pos_ref, kc_ref, vc_ref, hid_out, kc_out, vc_out, hid_buf, kbuf, vbuf, in_sem, out_sem):
    layers, n_seq, kv_heads = dims
    first = lax.axis_index("x") * n_seq
    arrive, leave = [], []
    for layer in range(layers):
        for src, dst in ((kc_ref, kbuf), (vc_ref, vbuf)):
            arrive.append(pltpu.make_async_copy(src.at[layer], dst.at[layer], in_sem.at[len(arrive)]))
            arrive[-1].start()
    hidden_in = pltpu.make_async_copy(hid_ref, hid_buf, in_sem.at[len(arrive)])
    hidden_in.start()
    for layer in range(layers):
        for i, (buf, dst) in enumerate(((kbuf, kc_out), (vbuf, vc_out))):
            arrive[2 * layer + i].wait()
            for b in range(n_seq):
                rows = jnp.concatenate([new_ref[layer, i, h, b:b + 1, :] for h in range(kv_heads)], axis=0)
                buf[layer, b, pos_ref[0, first + b]] = rows.astype(BF16)
            leave.append(pltpu.make_async_copy(buf.at[layer], dst.at[layer], out_sem.at[len(leave)]))
            leave[-1].start()
    hidden_in.wait()
    leave.append(pltpu.make_async_copy(hid_buf, hid_out, out_sem.at[len(leave)]))
    leave[-1].start()
    for copy in leave:
        copy.wait()


def solution(mesh):
    n_x, n_y = mesh.shape['x'], mesh.shape['y']
    cache_spec = P(None, ('dp', 'x'), None, 'y', None)
    col_spec = P(None, 'x', 'y')
    row_spec = P(None, 'y', 'x')
    in_specs = (P('dp', 'x'), P('dp'), cache_spec, cache_spec, P(None, 'x'), P(None, 'x'), P(), P(), col_spec, col_spec, col_spec, row_spec, col_spec, col_spec, row_spec)
    out_specs = (P('dp', 'x'), cache_spec, cache_spec)

    def device_step(hidden, positions, k_cache, v_cache, g_attn, g_mlp, q_gain, k_gain, w_q, w_k, w_v, w_o, w_gate, w_up, w_down):
        batch, depth = hidden.shape
        layers, n_seq, slots, kv_heads, _ = k_cache.shape
        q_cols, kv_cols, ffn = w_q.shape[2], w_k.shape[2], w_gate.shape[2]
        rows = batch // n_y
        slots2 = slots * kv_heads
        dims = (layers, n_y, n_x, rows, depth, q_cols, kv_cols, ffn)
        cols_qkv = q_cols + 2 * kv_cols
        vmem = pl.BlockSpec(memory_space=pltpu.VMEM)
        hbm = pl.BlockSpec(memory_space=pl.ANY)
        cache_shape = (layers, n_seq, slots2, HEAD_DIM)
        peers = n_y * n_x
        d_tiles, f_tiles = depth // TILE, ffn // TILE
        receives = 4 + 2 * (d_tiles + 1) + 4 * len(split_tiles(f_tiles))
        positions = positions.reshape(1, batch)
        new_hidden, new_rows = pl.pallas_call(
            functools.partial(step_kernel, dims),
            out_shape=(jax.ShapeDtypeStruct((n_y, rows, depth), BF16), jax.ShapeDtypeStruct((layers, 2, kv_heads, n_seq, HEAD_DIM), F32)),
            in_specs=[hbm] * 16,
            out_specs=(vmem, vmem),
            scratch_shapes=[
                pltpu.VMEM((depth, cols_qkv), BF16),
                pltpu.VMEM((q_cols, depth), BF16),
                pltpu.VMEM((depth, ffn), BF16),
                pltpu.VMEM((depth, ffn), BF16),
                pltpu.VMEM((ffn, depth), BF16),
                pltpu.VMEM(cache_shape, BF16),
                pltpu.VMEM(cache_shape, BF16),
                pltpu.VMEM((batch, depth), BF16),
                pltpu.VMEM((2, n_x, 1, HEAD_DIM), F32),
                pltpu.VMEM((n_x, n_seq, cols_qkv), BF16),
                pltpu.VMEM((n_x, n_seq, cols_qkv), BF16),
                pltpu.VMEM((16 * n_seq, HEAD_DIM), F32),
                pltpu.VMEM((16 * n_seq, HEAD_DIM), F32),
                pltpu.VMEM((n_x, n_seq, q_cols), BF16),
                pltpu.VMEM((2, n_y, rows, depth), BF16),
                pltpu.VMEM((2, n_y, rows, depth), BF16),
                pltpu.VMEM((n_y, rows, depth), BF16),
                pltpu.VMEM((n_y, rows, depth), BF16),
                pltpu.VMEM((2, 2, 2, rows, ffn), BF16),
                pltpu.VMEM((2, 2, rows, ffn), BF16),
                pltpu.VMEM((2, rows, ffn), BF16),
                pltpu.VMEM((2, rows, ffn), BF16),
                pltpu.VMEM((n_x, rows, ffn), BF16),
                pltpu.VMEM((batch, depth), F32),
                pltpu.VMEM((1, batch), jnp.int32),
                pltpu.VMEM((1, HEAD_DIM), F32),
                pltpu.VMEM(g_attn.shape, BF16),
                pltpu.VMEM(g_mlp.shape, BF16),
                pltpu.VMEM(q_gain.shape, BF16),
                pltpu.VMEM(k_gain.shape, BF16),
                pltpu.VMEM((layers, 1, depth), F32),
                pltpu.VMEM((layers, 1, depth), F32),
                pltpu.VMEM((layers, 1, HEAD_DIM), F32),
                pltpu.VMEM((layers, 1, HEAD_DIM), F32),
                pltpu.VMEM((n_seq, 1, slots2), jnp.int32),
                pltpu.VMEM((n_x, n_seq, TILE), F32),
                pltpu.VMEM((2, kv_heads, n_seq, 1, HEAD_DIM), F32),
                pltpu.VMEM((16 * n_seq, slots2), F32),
                pltpu.VMEM((16 * n_seq, slots2), BF16),
                pltpu.SemaphoreType.DMA((12,)),
                pltpu.SemaphoreType.DMA((receives,)),
                pltpu.SemaphoreType.DMA((14 + 2 * layers,)),
            ],
            compiler_params=pltpu.CompilerParams(collective_id=0, has_side_effects=True, vmem_limit_bytes=64 * 1024 * 1024 - 65536),
        )(hidden.reshape(n_y, rows, depth), positions, inverse_frequencies(), g_attn, g_mlp, q_gain, k_gain,
          k_cache.reshape(cache_shape), v_cache.reshape(cache_shape), w_q, w_k, w_v, w_o, w_gate, w_up, w_down)
        return pl.pallas_call(
            functools.partial(cache_kernel, (layers, n_seq, kv_heads)),
            out_shape=tuple(jax.ShapeDtypeStruct(a.shape, a.dtype) for a in (hidden, k_cache, v_cache)),
            in_specs=[hbm, vmem, pl.BlockSpec(memory_space=pltpu.SMEM), hbm, hbm],
            out_specs=(hbm, hbm, hbm),
            scratch_shapes=[
                pltpu.VMEM(hidden.shape, BF16),
                pltpu.VMEM(k_cache.shape, BF16),
                pltpu.VMEM(k_cache.shape, BF16),
                pltpu.SemaphoreType.DMA((2 * layers + 1,)),
                pltpu.SemaphoreType.DMA((2 * layers + 1,)),
            ],
            compiler_params=pltpu.CompilerParams(vmem_limit_bytes=64 * 1024 * 1024 - 65536),
        )(new_hidden.reshape(batch, depth), new_rows, positions, k_cache, v_cache)

    return jax.shard_map(device_step, mesh=mesh, in_specs=in_specs, out_specs=out_specs, check_vma=False)
```

```python
import functools

import jax
import jax.numpy as jnp
import numpy as np
from jax import lax
from jax.experimental import pallas as pl
from jax.experimental.pallas import tpu as pltpu
from jax.sharding import PartitionSpec as P

HEAD_DIM = 128
NORM_EPS = 1e-6
ROPE_BASE = 1000000.0
TILE = 256
GROUP_TILES = (3, 3, 3, 3, 3, 2)
SEQS = 4
MESH = pl.DeviceIdType.MESH
F32 = jnp.float32
BF16 = jnp.bfloat16


def inverse_frequencies():
    half_dim = HEAD_DIM // 2
    freqs = np.power(np.float32(ROPE_BASE), (-2.0 * np.arange(half_dim) / HEAD_DIM).astype(np.float32))
    return np.concatenate([freqs, freqs])[None].astype(np.float32)


def split_tiles(n_tiles):
    share = n_tiles / sum(GROUP_TILES)
    edges = [round(share * sum(GROUP_TILES[:i])) for i in range(len(GROUP_TILES) + 1)]
    return [(a, b) for a, b in zip(edges, edges[1:]) if b > a]


def step_kernel(dims, *refs):
    (layers, n_y, n_x, rows, depth, q_cols, kv_cols, ffn) = dims
    (hid_any, pos_any, freq_any, ga_any, gm_any, qg_any, kg_any, kc_ref, vc_ref,
     wq_ref, wk_ref, wv_ref, wo_ref, wg_ref, wu_ref, wd_ref,
     hid_out, new_out,
     wqkv, wo, wg, wu, wd, kbuf, vbuf, n_buf, stat, qkv_part, qkv_recv, q_rows, o_rows, attn_all,
     ar_part, ar_recv, h_mid, h_end, gu_part, gu_pair, gu_send, gu_recv, act_all, acc,
     pos_ref, freq_ref, ga_raw, gm_raw, qg_raw, kg_raw, ga_ref, gm_ref, qg_ref, kg_ref, slot_ref, part_scale, pair_scale, kv_rows, gu_direct, s_rows, p_rows,
     send_sem, recv_sem, local_sem) = refs
    batch = n_y * rows
    cols_qkv = q_cols + 2 * kv_cols
    q_heads = q_cols // HEAD_DIM
    kv_heads = kv_cols // HEAD_DIM
    group = q_heads // kv_heads
    model_dim = depth * n_x
    slots2 = kbuf.shape[2]
    n_seq = batch // n_x
    peers = n_y * n_x
    d_tiles, f_tiles, qkv_tiles = depth // TILE, ffn // TILE, cols_qkv // TILE

    y = lax.axis_index("y")
    x = lax.axis_index("x")
    chip = x // 2
    core = x % 2
    partner = 2 * chip + (1 - core)
    across = 2 * (1 - chip) + core
    diagonal = 2 * (1 - chip) + (1 - core)
    from_partner = 3 - 2 * core

    groups = split_tiles(f_tiles)
    at_qkv, at_first, at_attn, at_mid = 0, 1, 3, 4
    at_end = at_mid + d_tiles + 1
    at_mlp = at_end + d_tiles + 1

    def remote(src, dst, to_send, to_recv, to_y, to_x):
        return pltpu.make_async_remote_copy(
            src_ref=src, dst_ref=dst, send_sem=send_sem.at[to_send], recv_sem=recv_sem.at[to_recv],
            device_id={"y": to_y, "x": to_x}, device_id_type=MESH)

    def received(i, like):
        pltpu.make_async_copy(like, like, recv_sem.at[i]).wait()

    def delivered(i, like):
        pltpu.make_async_copy(like, like, send_sem.at[i]).wait()

    def each(first, last, body):
        def step(i, carry):
            body(i)
            return carry

        lax.fori_loop(first, last, step, 0)

    def tile_cols(t):
        return pl.ds(pl.multiple_of(t * TILE, TILE), TILE)

    def qkv_loads(layer):
        return [pltpu.make_async_copy(wq_ref.at[layer], wqkv.at[:, 0:q_cols], local_sem.at[0]),
                pltpu.make_async_copy(wk_ref.at[layer], wqkv.at[:, q_cols:q_cols + kv_cols], local_sem.at[1]),
                pltpu.make_async_copy(wv_ref.at[layer], wqkv.at[:, q_cols + kv_cols:cols_qkv], local_sem.at[2])]

    def o_loads(layer):
        return [pltpu.make_async_copy(wo_ref.at[layer], wo, local_sem.at[3])]

    def gate_up_loads(layer, piece):
        first, last = groups[2 * piece][0], groups[min(2 * piece + 1, len(groups) - 1)][1]
        cols = pl.ds(first * TILE, (last - first) * TILE)
        return [pltpu.make_async_copy(src.at[layer, :, cols], dst.at[:, cols], local_sem.at[5 + 2 * piece + i])
                for i, (src, dst) in enumerate(((wg_ref, wg), (wu_ref, wu)))]

    pieces = range((len(groups) + 1) // 2)

    def down_loads(layer):
        return [pltpu.make_async_copy(wd_ref.at[layer], wd, local_sem.at[4])]

    def cache_loads(layer):
        return [pltpu.make_async_copy(src.at[layer], dst.at[layer], local_sem.at[5 + 2 * len(pieces) + i * layers + layer])
                for i, (src, dst) in enumerate(((kc_ref, kbuf), (vc_ref, vbuf)))]

    def start(copies):
        for copy in copies:
            copy.start()

    def finish(copies):
        for copy in copies:
            copy.wait()

    row_i = lax.broadcasted_iota(jnp.int32, (rows, HEAD_DIM), 0)
    lane_i = lax.broadcasted_iota(jnp.int32, (rows, HEAD_DIM), 1)

    def along_lanes(column, first_row):
        return jnp.sum(jnp.where(lane_i == row_i + first_row, column, 0.0), axis=0, keepdims=True)

    def along_rows(lanes, first_row):
        return jnp.sum(jnp.where(lane_i == row_i + first_row, lanes, 0.0), axis=1, keepdims=True)

    def local_norm(hidden_ref, gain, i):
        def block(b, lanes):
            vals = hidden_ref[b].astype(F32)
            sums = jnp.sum(vals * vals, axis=1, keepdims=True)
            n_buf[pl.ds(pl.multiple_of(b * rows, rows), rows), :] = (vals * lax.rsqrt(sums / depth + NORM_EPS) * gain).astype(BF16)
            return lanes + along_lanes(sums, b * rows)

        stat[i, 0] = lax.fori_loop(0, n_y, block, jnp.zeros((1, HEAD_DIM), F32))

    def corrections(i):
        total = stat[i, 0]
        for d in range(1, n_x):
            total = total + stat[i, d]
        scale = lax.rsqrt(total / model_dim + NORM_EPS)
        return lambda d: jnp.where(scale > 0.0, scale / lax.rsqrt(stat[i, d] / depth + NORM_EPS), 0.0)

    def all_reduce(i, base, tile_product, residual_ref, result_ref):
        send = 4 + 2 * i

        def scatter(t, d):
            cols = tile_cols(t)
            return remote(ar_part.at[i, (y + d) % n_y, :, cols], ar_recv.at[i, d, :, cols], send, base + t, (y + d) % n_y, x)

        def gather(t, d):
            mine = result_ref.at[y, :, tile_cols(t)]
            return remote(mine, mine, send + 1, base + d_tiles, (y + d) % n_y, x)

        def send_tile(t):
            ar_part[i, :, :, tile_cols(t)] = tile_product(tile_cols(t)).astype(BF16).reshape(n_y, rows, TILE)
            for d in (2, 3, 1):
                scatter(t, d).start()

        each(0, d_tiles, send_tile)

        def sum_tile(t):
            cols = tile_cols(t)
            received(base + t, ar_recv.at[i, 1:n_y, :, cols])
            total = ar_part[i, y, :, cols].astype(F32)
            for d in range(1, n_y):
                total = total + ar_recv[i, d, :, cols].astype(F32)
            new = (residual_ref[y, :, cols].astype(F32) + total.astype(BF16).astype(F32)).astype(BF16)
            result_ref[y, :, cols] = new
            for d in (2, 3, 1):
                gather(t, d).start()

        each(0, d_tiles, sum_tile)
        received(base + d_tiles, ar_recv.at[i, 1:n_y])

        def drain():
            delivered(send, ar_recv.at[i, 1:n_y])
            delivered(send + 1, ar_recv.at[i, 1:n_y])

        return drain

    def qkv_copies(first, last):
        cols = pl.ds(first * TILE, (last - first) * TILE)
        return [remote(qkv_part.at[(x + d) % n_x, :, cols], qkv_recv.at[d, :, cols], 0, at_qkv, y, (x + d) % n_x) for d in (2, 3, 1)]

    def sum_copies(i):
        return [remote(stat.at[i, 0], stat.at[i, d], 1 + 2 * i, at_first + i, y, (x + d) % n_x) for d in (2, 3, 1)]

    def attn_copy(d):
        return remote(attn_all.at[x], attn_all.at[x], 2, at_attn, y, (x + d) % n_x)

    def group_cols(g):
        return pl.ds(groups[g][0] * TILE, (groups[g][1] - groups[g][0]) * TILE)

    def pair_copy(g):
        cols = group_cols(g)
        return remote(gu_part.at[:, :, 1 - core, :, cols], gu_pair.at[:, :, :, cols], 9, at_mlp + g, y, partner)

    def across_copy(g):
        cols = group_cols(g)
        return remote(gu_send.at[:, :, cols], gu_recv.at[:, :, cols], 10, at_mlp + len(groups) + g, y, across)

    tail = len(groups) - 1
    before = groups[tail][0] * TILE

    def tail_copies():
        def copy(d):
            to_x = (x + d) % n_x
            return remote(gu_part.at[:, to_x // 2, to_x % 2, :, group_cols(tail)], gu_direct.at[d], 8, at_mlp + tail, y, to_x)

        return [copy(d) for d in (2, 3, 1)]

    def act_copies(g):
        mine = act_all.at[x, :, group_cols(g)]
        return [remote(mine, mine, 11, at_mlp + 2 * len(groups) + g, y, to_x) for to_x in (diagonal, across, partner)]

    def project_qkv(first, last):
        def tile(t):
            cols = tile_cols(t)
            part = jnp.dot(n_buf[...], wqkv[:, cols], preferred_element_type=F32).astype(BF16)
            qkv_part[:, :, cols] = part.reshape(n_x, n_seq, TILE)

        each(first, last, tile)

    halves = ((0, (qkv_tiles + 1) // 2), ((qkv_tiles + 1) // 2, qkv_tiles))

    small = [pltpu.make_async_copy(src, dst, local_sem.at[5 + 2 * len(pieces) + 2 * layers + i]) for i, (src, dst) in enumerate((
        (hid_any, h_end), (ga_any, ga_raw), (gm_any, gm_raw), (qg_any, qg_raw), (kg_any, kg_raw), (pos_any, pos_ref), (freq_any, freq_ref)))]
    start(small)
    start(qkv_loads(0))
    barrier = pltpu.get_barrier_semaphore()
    each(1, peers, lambda e: pl.semaphore_signal(
        barrier, inc=1, device_id={"y": (y + e // n_x) % n_y, "x": (x + e % n_x) % n_x}, device_id_type=MESH))
    finish(small)
    start(cache_loads(0) + o_loads(0))
    for piece in pieces:
        start(gate_up_loads(0, piece))
    for raw, wide in ((ga_raw, ga_ref), (gm_raw, gm_ref), (qg_raw, qg_ref), (kg_raw, kg_ref)):
        for layer in range(layers):
            wide[layer] = raw[...].astype(F32)[layer:layer + 1]
    local_norm(h_end, ga_ref[0], 0)
    q_rows[...] = jnp.zeros_like(q_rows)
    finish(qkv_loads(0))
    project_qkv(0, qkv_tiles)
    start(down_loads(0))
    for layer in range(1, layers):
        start(cache_loads(layer))
    pl.semaphore_wait(barrier, peers - 1)
    start(sum_copies(0))
    for half in halves:
        start(qkv_copies(*half))

    my_pos = jnp.sum(
        jnp.where(lax.broadcasted_iota(jnp.int32, (n_seq, batch), 1) == lax.broadcasted_iota(jnp.int32, (n_seq, batch), 0) + x * n_seq,
                  pos_ref[...].astype(F32), 0.0), axis=1, keepdims=True)
    angles = my_pos * freq_ref[...]
    cos_tab = jnp.cos(angles)
    sin_tab = jnp.where(lax.broadcasted_iota(jnp.int32, (n_seq, HEAD_DIM), 1) < HEAD_DIM // 2, -1.0, 1.0) * jnp.sin(angles)
    slot_ref[...] = jnp.broadcast_to(my_pos.astype(jnp.int32), (n_seq, slots2)).reshape(slot_ref.shape)

    slot_row = lax.broadcasted_iota(jnp.int32, (slots2, HEAD_DIM), 0)
    slot_id = slot_row // kv_heads
    head_id = slot_row % kv_heads
    score_col = lax.broadcasted_iota(jnp.int32, (16, slots2), 1)
    score_head = lax.broadcasted_iota(jnp.int32, (16, slots2), 0) // group
    score_slot = score_col // kv_heads
    score_own = (score_col % kv_heads == score_head) | (score_head >= kv_heads)

    def run_layer(layer):
        more = layer + 1 < layers

        def reload(loads):
            @pl.when(more)
            def _():
                start(loads(layer + 1))

        reload(qkv_loads)
        received(at_first, stat.at[0, 1:n_x])
        correction = corrections(0)
        for d in range(n_x):
            part_scale[d] = jnp.broadcast_to(along_rows(correction(d), x * n_seq), (n_seq, TILE))
        received(at_qkv, qkv_recv.at[1:n_x])

        def projected(cols, scale_cols):
            total = qkv_part[x, :, cols].astype(F32) * part_scale[0, :, scale_cols]
            for d in range(1, n_x):
                total = total + qkv_recv[d, :, cols].astype(F32) * part_scale[d, :, scale_cols]
            return total.astype(BF16).astype(F32)

        for h in range(q_heads + kv_heads):
            vals = projected(pl.ds(h * HEAD_DIM, HEAD_DIM), pl.ds(0, HEAD_DIM))
            mean_sq = jnp.mean(vals * vals, axis=-1, keepdims=True)
            normed = vals * lax.rsqrt(mean_sq + NORM_EPS) * (qg_ref if h < q_heads else kg_ref)[layer]
            turned = (normed * cos_tab + pltpu.roll(normed, HEAD_DIM // 2, 1) * sin_tab).astype(BF16).astype(F32)
            if h < q_heads:
                q_rows[pl.ds(h, n_seq, stride=16), :] = turned
            else:
                new_out[layer, 0, h - q_heads] = turned
                kv_rows[0, h - q_heads] = turned.reshape(n_seq, 1, HEAD_DIM)
        for h in range(kv_heads):
            vals = projected(pl.ds(q_cols + kv_cols + h * HEAD_DIM, HEAD_DIM), pl.ds(0, HEAD_DIM))
            new_out[layer, 1, h] = vals
            kv_rows[1, h] = vals.reshape(n_seq, 1, HEAD_DIM)

        finish(cache_loads(layer))

        def update(i):
            for u in range(SEQS):
                b = i * SEQS + u
                hit = slot_id == slot_ref[b][:, :HEAD_DIM]
                for j, buf in enumerate((kbuf, vbuf)):
                    fresh = kv_rows[j, 0, b]
                    for h in range(1, kv_heads):
                        fresh = jnp.where(head_id == h, kv_rows[j, h, b], fresh)
                    buf[layer, b] = jnp.where(hit, fresh, buf[layer, b].astype(F32)).astype(BF16)

        each(0, n_seq // SEQS, update)
        for b in range(n_seq):
            q_b = q_rows[b * 16:(b + 1) * 16, :].astype(BF16)
            scores = lax.dot_general(q_b, kbuf[layer, b], (((1,), (1,)), ((), ())), preferred_element_type=F32) * (HEAD_DIM ** -0.5)
            s_rows[b * 16:(b + 1) * 16, :] = jnp.where(score_own & (score_slot <= slot_ref[b]), scores, -1e30)

        def softmax(i):
            block = pl.ds(pl.multiple_of(i * 16 * SEQS, 16 * SEQS), 16 * SEQS)
            scores = s_rows[block, :]
            e = jnp.exp(scores - jnp.max(scores, axis=1, keepdims=True))
            p_rows[block, :] = (e / jnp.sum(e, axis=1, keepdims=True)).astype(BF16)

        each(0, n_seq // SEQS, softmax)
        for b in range(n_seq):
            o_rows[b * 16:(b + 1) * 16, :] = jnp.dot(p_rows[b * 16:(b + 1) * 16, :], vbuf[layer, b], preferred_element_type=F32)
        for h in range(q_heads):
            attn_all[x, :, h * HEAD_DIM:(h + 1) * HEAD_DIM] = o_rows[pl.ds(h, n_seq, stride=16), :].astype(BF16)
        for d in (2, 3, 1):
            attn_copy(d).start()
        finish(o_loads(layer))
        delivered(0, qkv_recv.at[1:n_x])
        delivered(1, stat.at[0, 1:n_x])
        received(at_attn, attn_all.at[1:n_x])

        drain_mid = all_reduce(
            0, at_mid, lambda cols: jnp.dot(attn_all[...].reshape(batch, q_cols), wo[:, cols], preferred_element_type=F32), h_end, h_mid)
        reload(o_loads)

        local_norm(h_mid, gm_ref[layer], 1)
        start(sum_copies(1))

        def project(t):
            cols = tile_cols(t)
            gate = jnp.dot(n_buf[...], wg[:, cols], preferred_element_type=F32).astype(BF16)
            up = jnp.dot(n_buf[...], wu[:, cols], preferred_element_type=F32).astype(BF16)
            gu_part[0, :, :, :, cols] = gate.reshape(2, 2, rows, TILE)
            gu_part[1, :, :, :, cols] = up.reshape(2, 2, rows, TILE)

        def cross(g):
            cols = group_cols(g)
            received(at_mlp + g, gu_pair.at[:, :, :, cols])

            def tile(t):
                cols = tile_cols(t)
                pair = gu_part[:, 1 - chip, core, :, cols].astype(F32) * pair_scale[0] + gu_pair[:, 1 - chip, :, cols].astype(F32) * pair_scale[1]
                gu_send[:, :, cols] = pair.astype(BF16)

            each(*groups[g], tile)
            across_copy(g).start()

        def activate(g):
            received(at_mlp + len(groups) + g, gu_recv.at[:, :, group_cols(g)])

            def tile(t):
                cols = tile_cols(t)
                gate_up = (gu_part[:, chip, core, :, cols].astype(F32) * part_scale[0] + gu_pair[:, chip, :, cols].astype(F32) * part_scale[from_partner]
                           + gu_recv[:, :, cols].astype(F32)).astype(BF16).astype(F32)
                act_all[x, :, cols] = (jax.nn.silu(gate_up[0]) * gate_up[1]).astype(BF16)

            each(*groups[g], tile)
            start(act_copies(g))

        def activate_tail():
            received(at_mlp + tail, gu_direct.at[1:n_x])

            def tile(t):
                cols = tile_cols(t)
                total = gu_part[:, chip, core, :, cols].astype(F32) * part_scale[0]
                for d in range(1, n_x):
                    total = total + gu_direct[d, :, :, tile_cols(t - groups[tail][0])].astype(F32) * part_scale[d]
                gate_up = total.astype(BF16).astype(F32)
                act_all[x, :, cols] = (jax.nn.silu(gate_up[0]) * gate_up[1]).astype(BF16)

            each(*groups[tail], tile)
            start(act_copies(tail))

        for g in range(len(groups)):
            if g % 2 == 0:
                finish(gate_up_loads(layer, g // 2))
            each(*groups[g], project)
            if g < tail:
                pair_copy(g).start()
            else:
                start(tail_copies())
            if g == 2:
                received(at_first + 1, stat.at[1, 1:n_x])
                correction = corrections(1)
                for d in range(n_x):
                    part_scale[d] = jnp.broadcast_to(along_rows(correction(d), x * rows), (rows, TILE))
                for i, d in enumerate((0, from_partner)):
                    pair_scale[i] = jnp.broadcast_to(along_rows(correction(d), across * rows), (rows, TILE))
            if g >= 2:
                cross(g - 2)
        for piece in pieces:
            reload(lambda layer: gate_up_loads(layer, piece))
        cross(tail - 1)
        for g in range(tail):
            activate(g)
        activate_tail()
        drain_mid()
        delivered(2, attn_all.at[1:n_x])
        finish(down_loads(layer))
        for g, (first, last) in enumerate(groups):
            cols = group_cols(g)
            received(at_mlp + 2 * len(groups) + g, act_all.at[1:n_x, :, cols])

            def down(t):
                part = jnp.dot(act_all[:, :, cols].reshape(batch, (last - first) * TILE), wd[cols, tile_cols(t)], preferred_element_type=F32)
                acc[:, tile_cols(t)] = acc[:, tile_cols(t)] + part if g else part

            each(0, d_tiles, down)
        reload(down_loads)
        drain_end = all_reduce(1, at_end, lambda cols: acc[:, cols], h_mid, h_end)

        @pl.when(more)
        def _():
            local_norm(h_end, ga_ref[layer + 1], 0)
            start(sum_copies(0))
            finish(qkv_loads(layer + 1))
            for half in halves:
                project_qkv(*half)
                start(qkv_copies(*half))

        drain_end()

        delivered(3, stat.at[1, 1:n_x])
        delivered(8, gu_direct.at[1:n_x])
        delivered(9, gu_pair.at[:, :, :, 0:before])
        delivered(10, gu_recv.at[:, :, 0:before])
        delivered(11, act_all.at[1:n_x])

    each(0, layers, run_layer)
    hid_out[...] = h_end[...]


def cache_kernel(dims, hid_ref, new_ref, pos_ref, kc_ref, vc_ref, hid_out, kc_out, vc_out, hid_buf, kbuf, vbuf, in_sem, out_sem):
    layers, n_seq, kv_heads = dims
    first = lax.axis_index("x") * n_seq
    arrive, leave = [], []
    for layer in range(layers):
        for src, dst in ((kc_ref, kbuf), (vc_ref, vbuf)):
            arrive.append(pltpu.make_async_copy(src.at[layer], dst.at[layer], in_sem.at[len(arrive)]))
            arrive[-1].start()
    hidden_in = pltpu.make_async_copy(hid_ref, hid_buf, in_sem.at[len(arrive)])
    hidden_in.start()
    for layer in range(layers):
        for i, (buf, dst) in enumerate(((kbuf, kc_out), (vbuf, vc_out))):
            arrive[2 * layer + i].wait()
            for b in range(n_seq):
                rows = jnp.concatenate([new_ref[layer, i, h, b:b + 1, :] for h in range(kv_heads)], axis=0)
                buf[layer, b, pos_ref[0, first + b]] = rows.astype(BF16)
            leave.append(pltpu.make_async_copy(buf.at[layer], dst.at[layer], out_sem.at[len(leave)]))
            leave[-1].start()
    hidden_in.wait()
    leave.append(pltpu.make_async_copy(hid_buf, hid_out, out_sem.at[len(leave)]))
    leave[-1].start()
    for copy in leave:
        copy.wait()


def solution(mesh):
    n_x, n_y = mesh.shape['x'], mesh.shape['y']
    cache_spec = P(None, ('dp', 'x'), None, 'y', None)
    col_spec = P(None, 'x', 'y')
    row_spec = P(None, 'y', 'x')
    in_specs = (P('dp', 'x'), P('dp'), cache_spec, cache_spec, P(None, 'x'), P(None, 'x'), P(), P(), col_spec, col_spec, col_spec, row_spec, col_spec, col_spec, row_spec)
    out_specs = (P('dp', 'x'), cache_spec, cache_spec)

    def device_step(hidden, positions, k_cache, v_cache, g_attn, g_mlp, q_gain, k_gain, w_q, w_k, w_v, w_o, w_gate, w_up, w_down):
        batch, depth = hidden.shape
        layers, n_seq, slots, kv_heads, _ = k_cache.shape
        q_cols, kv_cols, ffn = w_q.shape[2], w_k.shape[2], w_gate.shape[2]
        rows = batch // n_y
        slots2 = slots * kv_heads
        dims = (layers, n_y, n_x, rows, depth, q_cols, kv_cols, ffn)
        cols_qkv = q_cols + 2 * kv_cols
        vmem = pl.BlockSpec(memory_space=pltpu.VMEM)
        hbm = pl.BlockSpec(memory_space=pl.ANY)
        cache_shape = (layers, n_seq, slots2, HEAD_DIM)
        peers = n_y * n_x
        d_tiles, f_tiles = depth // TILE, ffn // TILE
        receives = 4 + 2 * (d_tiles + 1) + 3 * len(split_tiles(f_tiles))
        positions = positions.reshape(1, batch)
        new_hidden, new_rows = pl.pallas_call(
            functools.partial(step_kernel, dims),
            out_shape=(jax.ShapeDtypeStruct((n_y, rows, depth), BF16), jax.ShapeDtypeStruct((layers, 2, kv_heads, n_seq, HEAD_DIM), F32)),
            in_specs=[hbm] * 16,
            out_specs=(vmem, vmem),
            scratch_shapes=[
                pltpu.VMEM((depth, cols_qkv), BF16),
                pltpu.VMEM((q_cols, depth), BF16),
                pltpu.VMEM((depth, ffn), BF16),
                pltpu.VMEM((depth, ffn), BF16),
                pltpu.VMEM((ffn, depth), BF16),
                pltpu.VMEM(cache_shape, BF16),
                pltpu.VMEM(cache_shape, BF16),
                pltpu.VMEM((batch, depth), BF16),
                pltpu.VMEM((2, n_x, 1, HEAD_DIM), F32),
                pltpu.VMEM((n_x, n_seq, cols_qkv), BF16),
                pltpu.VMEM((n_x, n_seq, cols_qkv), BF16),
                pltpu.VMEM((16 * n_seq, HEAD_DIM), F32),
                pltpu.VMEM((16 * n_seq, HEAD_DIM), F32),
                pltpu.VMEM((n_x, n_seq, q_cols), BF16),
                pltpu.VMEM((2, n_y, rows, depth), BF16),
                pltpu.VMEM((2, n_y, rows, depth), BF16),
                pltpu.VMEM((n_y, rows, depth), BF16),
                pltpu.VMEM((n_y, rows, depth), BF16),
                pltpu.VMEM((2, 2, 2, rows, ffn), BF16),
                pltpu.VMEM((2, 2, rows, ffn), BF16),
                pltpu.VMEM((2, rows, ffn), BF16),
                pltpu.VMEM((2, rows, ffn), BF16),
                pltpu.VMEM((n_x, rows, ffn), BF16),
                pltpu.VMEM((batch, depth), F32),
                pltpu.VMEM((1, batch), jnp.int32),
                pltpu.VMEM((1, HEAD_DIM), F32),
                pltpu.VMEM(g_attn.shape, BF16),
                pltpu.VMEM(g_mlp.shape, BF16),
                pltpu.VMEM(q_gain.shape, BF16),
                pltpu.VMEM(k_gain.shape, BF16),
                pltpu.VMEM((layers, 1, depth), F32),
                pltpu.VMEM((layers, 1, depth), F32),
                pltpu.VMEM((layers, 1, HEAD_DIM), F32),
                pltpu.VMEM((layers, 1, HEAD_DIM), F32),
                pltpu.VMEM((n_seq, 1, slots2), jnp.int32),
                pltpu.VMEM((n_x, n_seq, TILE), F32),
                pltpu.VMEM((2, rows, TILE), F32),
                pltpu.VMEM((2, kv_heads, n_seq, 1, HEAD_DIM), F32),
                pltpu.VMEM((n_x, 2, rows, (split_tiles(f_tiles)[-1][1] - split_tiles(f_tiles)[-1][0]) * TILE), BF16),
                pltpu.VMEM((16 * n_seq, slots2), F32),
                pltpu.VMEM((16 * n_seq, slots2), BF16),
                pltpu.SemaphoreType.DMA((12,)),
                pltpu.SemaphoreType.DMA((receives,)),
                pltpu.SemaphoreType.DMA((12 + 2 * ((len(split_tiles(f_tiles)) + 1) // 2) + 2 * layers,)),
            ],
            compiler_params=pltpu.CompilerParams(collective_id=0, has_side_effects=True, vmem_limit_bytes=64 * 1024 * 1024 - 65536),
        )(hidden.reshape(n_y, rows, depth), positions, inverse_frequencies(), g_attn, g_mlp, q_gain, k_gain,
          k_cache.reshape(cache_shape), v_cache.reshape(cache_shape), w_q, w_k, w_v, w_o, w_gate, w_up, w_down)
        return pl.pallas_call(
            functools.partial(cache_kernel, (layers, n_seq, kv_heads)),
            out_shape=tuple(jax.ShapeDtypeStruct(a.shape, a.dtype) for a in (hidden, k_cache, v_cache)),
            in_specs=[hbm, vmem, pl.BlockSpec(memory_space=pltpu.SMEM), hbm, hbm],
            out_specs=(hbm, hbm, hbm),
            scratch_shapes=[
                pltpu.VMEM(hidden.shape, BF16),
                pltpu.VMEM(k_cache.shape, BF16),
                pltpu.VMEM(k_cache.shape, BF16),
                pltpu.SemaphoreType.DMA((2 * layers + 1,)),
                pltpu.SemaphoreType.DMA((2 * layers + 1,)),
            ],
            compiler_params=pltpu.CompilerParams(vmem_limit_bytes=64 * 1024 * 1024 - 65536),
        )(new_hidden.reshape(batch, depth), new_rows, positions, k_cache, v_cache)

    return jax.shard_map(device_step, mesh=mesh, in_specs=in_specs, out_specs=out_specs, check_vma=False)
```

```python
import functools

import jax
import jax.numpy as jnp
import numpy as np
from jax import lax
from jax.experimental import pallas as pl
from jax.experimental.pallas import tpu as pltpu
from jax.sharding import PartitionSpec as P

HEAD_DIM = 128
NORM_EPS = 1e-6
ROPE_BASE = 1000000.0
TILE = 256
GROUP_TILES = (3, 3, 3, 3, 3, 2)
SEQS = 4
MESH = pl.DeviceIdType.MESH
F32 = jnp.float32
BF16 = jnp.bfloat16


def inverse_frequencies():
    half_dim = HEAD_DIM // 2
    freqs = np.power(np.float32(ROPE_BASE), (-2.0 * np.arange(half_dim) / HEAD_DIM).astype(np.float32))
    return np.concatenate([freqs, freqs])[None].astype(np.float32)


def split_tiles(n_tiles):
    share = n_tiles / sum(GROUP_TILES)
    edges = [round(share * sum(GROUP_TILES[:i])) for i in range(len(GROUP_TILES) + 1)]
    return [(a, b) for a, b in zip(edges, edges[1:]) if b > a]


def step_kernel(dims, *refs):
    (layers, n_y, n_x, rows, depth, q_cols, kv_cols, ffn) = dims
    (hid_any, pos_any, freq_any, ga_any, gm_any, qg_any, kg_any, kc_ref, vc_ref,
     wq_ref, wk_ref, wv_ref, wo_ref, wg_ref, wu_ref, wd_ref,
     hid_out, new_out,
     wqkv, wo, wg, wu, wd, kbuf, vbuf, n_buf, stat, qkv_part, qkv_recv, q_rows, o_rows, attn_all,
     ar_part, ar_recv, h_mid, h_end, gu_part, gu_pair, gu_send, gu_recv, act_all, acc,
     pos_ref, freq_ref, ga_raw, gm_raw, qg_raw, kg_raw, ga_ref, gm_ref, qg_ref, kg_ref, slot_ref, part_scale, pair_scale, kv_rows, gu_direct, s_rows, p_rows,
     send_sem, recv_sem, local_sem) = refs
    batch = n_y * rows
    cols_qkv = q_cols + 2 * kv_cols
    q_heads = q_cols // HEAD_DIM
    kv_heads = kv_cols // HEAD_DIM
    group = q_heads // kv_heads
    model_dim = depth * n_x
    slots2 = kbuf.shape[2]
    n_seq = batch // n_x
    peers = n_y * n_x
    d_tiles, f_tiles, qkv_tiles = depth // TILE, ffn // TILE, cols_qkv // TILE

    y = lax.axis_index("y")
    x = lax.axis_index("x")
    chip = x // 2
    core = x % 2
    partner = 2 * chip + (1 - core)
    across = 2 * (1 - chip) + core
    diagonal = 2 * (1 - chip) + (1 - core)
    from_partner = 3 - 2 * core

    groups = split_tiles(f_tiles)
    at_qkv, at_first, at_attn, at_mid = 0, 1, 3, 4
    at_end = at_mid + d_tiles + 1
    at_mlp = at_end + d_tiles + 1

    def remote(src, dst, to_send, to_recv, to_y, to_x):
        return pltpu.make_async_remote_copy(
            src_ref=src, dst_ref=dst, send_sem=send_sem.at[to_send], recv_sem=recv_sem.at[to_recv],
            device_id={"y": to_y, "x": to_x}, device_id_type=MESH)

    def received(i, like):
        pltpu.make_async_copy(like, like, recv_sem.at[i]).wait()

    def delivered(i, like):
        pltpu.make_async_copy(like, like, send_sem.at[i]).wait()

    def each(first, last, body):
        def step(i, carry):
            body(i)
            return carry

        lax.fori_loop(first, last, step, 0)

    def tile_cols(t):
        return pl.ds(pl.multiple_of(t * TILE, TILE), TILE)

    def qkv_loads(layer):
        return [pltpu.make_async_copy(wq_ref.at[layer], wqkv.at[:, 0:q_cols], local_sem.at[0]),
                pltpu.make_async_copy(wk_ref.at[layer], wqkv.at[:, q_cols:q_cols + kv_cols], local_sem.at[1]),
                pltpu.make_async_copy(wv_ref.at[layer], wqkv.at[:, q_cols + kv_cols:cols_qkv], local_sem.at[2])]

    def o_loads(layer):
        return [pltpu.make_async_copy(wo_ref.at[layer], wo, local_sem.at[3])]

    def gate_up_loads(layer, piece):
        first, last = groups[2 * piece][0], groups[min(2 * piece + 1, len(groups) - 1)][1]
        cols = pl.ds(first * TILE, (last - first) * TILE)
        return [pltpu.make_async_copy(src.at[layer, :, cols], dst.at[:, cols], local_sem.at[5 + 2 * piece + i])
                for i, (src, dst) in enumerate(((wg_ref, wg), (wu_ref, wu)))]

    pieces = range((len(groups) + 1) // 2)

    def down_loads(layer):
        return [pltpu.make_async_copy(wd_ref.at[layer], wd, local_sem.at[4])]

    def cache_loads(layer):
        return [pltpu.make_async_copy(src.at[layer], dst.at[layer], local_sem.at[5 + 2 * len(pieces) + i * layers + layer])
                for i, (src, dst) in enumerate(((kc_ref, kbuf), (vc_ref, vbuf)))]

    def start(copies):
        for copy in copies:
            copy.start()

    def finish(copies):
        for copy in copies:
            copy.wait()

    row_i = lax.broadcasted_iota(jnp.int32, (rows, HEAD_DIM), 0)
    lane_i = lax.broadcasted_iota(jnp.int32, (rows, HEAD_DIM), 1)

    def along_lanes(column, first_row):
        return jnp.sum(jnp.where(lane_i == row_i + first_row, column, 0.0), axis=0, keepdims=True)

    def along_rows(lanes, first_row):
        return jnp.sum(jnp.where(lane_i == row_i + first_row, lanes, 0.0), axis=1, keepdims=True)

    def local_norm(hidden_ref, gain, i):
        def block(b, lanes):
            vals = hidden_ref[b].astype(F32)
            sums = jnp.sum(vals * vals, axis=1, keepdims=True)
            n_buf[pl.ds(pl.multiple_of(b * rows, rows), rows), :] = (vals * lax.rsqrt(sums / depth + NORM_EPS) * gain).astype(BF16)
            return lanes + along_lanes(sums, b * rows)

        stat[i, 0] = lax.fori_loop(0, n_y, block, jnp.zeros((1, HEAD_DIM), F32))

    def corrections(i):
        total = stat[i, 0]
        for d in range(1, n_x):
            total = total + stat[i, d]
        scale = lax.rsqrt(total / model_dim + NORM_EPS)
        return lambda d: jnp.where(scale > 0.0, scale / lax.rsqrt(stat[i, d] / depth + NORM_EPS), 0.0)

    def all_reduce(i, base, tile_product, residual_ref, result_ref):
        send = 4 + 2 * i

        def scatter(t, d):
            cols = tile_cols(t)
            return remote(ar_part.at[i, (y + d) % n_y, :, cols], ar_recv.at[i, d, :, cols], send, base + t, (y + d) % n_y, x)

        def gather(t, d):
            mine = result_ref.at[y, :, tile_cols(t)]
            return remote(mine, mine, send + 1, base + d_tiles, (y + d) % n_y, x)

        def send_tile(t):
            ar_part[i, :, :, tile_cols(t)] = tile_product(tile_cols(t)).astype(BF16).reshape(n_y, rows, TILE)
            for d in (2, 3, 1):
                scatter(t, d).start()

        each(0, d_tiles, send_tile)

        def sum_tile(t):
            cols = tile_cols(t)
            received(base + t, ar_recv.at[i, 1:n_y, :, cols])
            total = ar_part[i, y, :, cols].astype(F32)
            for d in range(1, n_y):
                total = total + ar_recv[i, d, :, cols].astype(F32)
            new = (residual_ref[y, :, cols].astype(F32) + total.astype(BF16).astype(F32)).astype(BF16)
            result_ref[y, :, cols] = new
            for d in (2, 3, 1):
                gather(t, d).start()

        each(0, d_tiles, sum_tile)
        received(base + d_tiles, ar_recv.at[i, 1:n_y])

        def drain():
            delivered(send, ar_recv.at[i, 1:n_y])
            delivered(send + 1, ar_recv.at[i, 1:n_y])

        return drain

    def qkv_copies(first, last):
        cols = pl.ds(first * TILE, (last - first) * TILE)
        return [remote(qkv_part.at[(x + d) % n_x, :, cols], qkv_recv.at[d, :, cols], 0, at_qkv, y, (x + d) % n_x) for d in (2, 3, 1)]

    def sum_copies(i):
        return [remote(stat.at[i, 0], stat.at[i, d], 1 + 2 * i, at_first + i, y, (x + d) % n_x) for d in (2, 3, 1)]

    def attn_copy(d):
        return remote(attn_all.at[x], attn_all.at[x], 2, at_attn, y, (x + d) % n_x)

    def group_cols(g):
        return pl.ds(groups[g][0] * TILE, (groups[g][1] - groups[g][0]) * TILE)

    def pair_copy(g):
        cols = group_cols(g)
        return remote(gu_part.at[:, :, 1 - core, :, cols], gu_pair.at[:, :, :, cols], 9, at_mlp + g, y, partner)

    def across_copy(g):
        cols = group_cols(g)
        return remote(gu_send.at[:, :, cols], gu_recv.at[:, :, cols], 10, at_mlp + len(groups) + g, y, across)

    tail = len(groups) - 1
    before = groups[tail][0] * TILE

    def tail_copies():
        def copy(d):
            to_x = (x + d) % n_x
            return remote(gu_part.at[:, to_x // 2, to_x % 2, :, group_cols(tail)], gu_direct.at[d], 8, at_mlp + tail, y, to_x)

        return [copy(d) for d in (2, 3, 1)]

    def act_copies(g):
        mine = act_all.at[x, :, group_cols(g)]
        return [remote(mine, mine, 11, at_mlp + 2 * len(groups) + g, y, to_x) for to_x in (diagonal, across, partner)]

    def project_qkv(first, last):
        def tile(t):
            cols = tile_cols(t)
            part = jnp.dot(n_buf[...], wqkv[:, cols], preferred_element_type=F32).astype(BF16)
            qkv_part[:, :, cols] = part.reshape(n_x, n_seq, TILE)

        each(first, last, tile)

    halves = ((0, (qkv_tiles + 1) // 2), ((qkv_tiles + 1) // 2, qkv_tiles))

    barrier = pltpu.get_barrier_semaphore()
    each(1, peers, lambda e: pl.semaphore_signal(
        barrier, inc=1, device_id={"y": (y + e // n_x) % n_y, "x": (x + e % n_x) % n_x}, device_id_type=MESH))
    small = [pltpu.make_async_copy(src, dst, local_sem.at[5 + 2 * len(pieces) + 2 * layers + i]) for i, (src, dst) in enumerate((
        (hid_any, h_end), (ga_any, ga_raw), (gm_any, gm_raw), (qg_any, qg_raw), (kg_any, kg_raw), (pos_any, pos_ref), (freq_any, freq_ref)))]
    start(small)
    start(qkv_loads(0))
    finish(small)
    start(cache_loads(0) + o_loads(0))
    for piece in pieces:
        start(gate_up_loads(0, piece))
    for raw, wide in ((ga_raw, ga_ref), (gm_raw, gm_ref), (qg_raw, qg_ref), (kg_raw, kg_ref)):
        for layer in range(layers):
            wide[layer] = raw[...].astype(F32)[layer:layer + 1]
    local_norm(h_end, ga_ref[0], 0)
    q_rows[...] = jnp.zeros_like(q_rows)
    finish(qkv_loads(0))
    project_qkv(0, qkv_tiles)
    start(down_loads(0))
    for layer in range(1, layers):
        start(cache_loads(layer))
    pl.semaphore_wait(barrier, peers - 1)
    start(sum_copies(0))
    for half in halves:
        start(qkv_copies(*half))

    my_pos = jnp.sum(
        jnp.where(lax.broadcasted_iota(jnp.int32, (n_seq, batch), 1) == lax.broadcasted_iota(jnp.int32, (n_seq, batch), 0) + x * n_seq,
                  pos_ref[...].astype(F32), 0.0), axis=1, keepdims=True)
    angles = my_pos * freq_ref[...]
    cos_tab = jnp.cos(angles)
    sin_tab = jnp.where(lax.broadcasted_iota(jnp.int32, (n_seq, HEAD_DIM), 1) < HEAD_DIM // 2, -1.0, 1.0) * jnp.sin(angles)
    slot_ref[...] = jnp.broadcast_to(my_pos.astype(jnp.int32), (n_seq, slots2)).reshape(slot_ref.shape)

    slot_row = lax.broadcasted_iota(jnp.int32, (slots2, HEAD_DIM), 0)
    slot_id = slot_row // kv_heads
    head_id = slot_row % kv_heads
    score_col = lax.broadcasted_iota(jnp.int32, (16, slots2), 1)
    score_head = lax.broadcasted_iota(jnp.int32, (16, slots2), 0) // group
    score_slot = score_col // kv_heads
    score_own = (score_col % kv_heads == score_head) | (score_head >= kv_heads)

    def run_layer(layer):
        more = layer + 1 < layers

        def reload(loads):
            @pl.when(more)
            def _():
                start(loads(layer + 1))

        reload(qkv_loads)
        received(at_first, stat.at[0, 1:n_x])
        correction = corrections(0)
        for d in range(n_x):
            part_scale[d] = jnp.broadcast_to(along_rows(correction(d), x * n_seq), (n_seq, TILE))
        received(at_qkv, qkv_recv.at[1:n_x])

        def projected(cols, scale_cols):
            total = qkv_part[x, :, cols].astype(F32) * part_scale[0, :, scale_cols]
            for d in range(1, n_x):
                total = total + qkv_recv[d, :, cols].astype(F32) * part_scale[d, :, scale_cols]
            return total.astype(BF16).astype(F32)

        for h in range(q_heads + kv_heads):
            vals = projected(pl.ds(h * HEAD_DIM, HEAD_DIM), pl.ds(0, HEAD_DIM))
            mean_sq = jnp.mean(vals * vals, axis=-1, keepdims=True)
            normed = vals * lax.rsqrt(mean_sq + NORM_EPS) * (qg_ref if h < q_heads else kg_ref)[layer]
            turned = (normed * cos_tab + pltpu.roll(normed, HEAD_DIM // 2, 1) * sin_tab).astype(BF16).astype(F32)
            if h < q_heads:
                q_rows[pl.ds(h, n_seq, stride=16), :] = turned
            else:
                new_out[layer, 0, h - q_heads] = turned
                kv_rows[0, h - q_heads] = turned.reshape(n_seq, 1, HEAD_DIM)
        for h in range(kv_heads):
            vals = projected(pl.ds(q_cols + kv_cols + h * HEAD_DIM, HEAD_DIM), pl.ds(0, HEAD_DIM))
            new_out[layer, 1, h] = vals
            kv_rows[1, h] = vals.reshape(n_seq, 1, HEAD_DIM)

        finish(cache_loads(layer))

        def update(i):
            for u in range(SEQS):
                b = i * SEQS + u
                hit = slot_id == slot_ref[b][:, :HEAD_DIM]
                for j, buf in enumerate((kbuf, vbuf)):
                    fresh = kv_rows[j, 0, b]
                    for h in range(1, kv_heads):
                        fresh = jnp.where(head_id == h, kv_rows[j, h, b], fresh)
                    buf[layer, b] = jnp.where(hit, fresh, buf[layer, b].astype(F32)).astype(BF16)

        each(0, n_seq // SEQS, update)
        for b in range(n_seq):
            q_b = q_rows[b * 16:(b + 1) * 16, :].astype(BF16)
            scores = lax.dot_general(q_b, kbuf[layer, b], (((1,), (1,)), ((), ())), preferred_element_type=F32) * (HEAD_DIM ** -0.5)
            s_rows[b * 16:(b + 1) * 16, :] = jnp.where(score_own & (score_slot <= slot_ref[b]), scores, -1e30)

        def softmax(i):
            block = pl.ds(pl.multiple_of(i * 16 * SEQS, 16 * SEQS), 16 * SEQS)
            scores = s_rows[block, :]
            e = jnp.exp(scores - jnp.max(scores, axis=1, keepdims=True))
            p_rows[block, :] = (e / jnp.sum(e, axis=1, keepdims=True)).astype(BF16)

        each(0, n_seq // SEQS, softmax)
        for b in range(n_seq):
            o_rows[b * 16:(b + 1) * 16, :] = jnp.dot(p_rows[b * 16:(b + 1) * 16, :], vbuf[layer, b], preferred_element_type=F32)
        for h in range(q_heads):
            attn_all[x, :, h * HEAD_DIM:(h + 1) * HEAD_DIM] = o_rows[pl.ds(h, n_seq, stride=16), :].astype(BF16)
        for d in (2, 3, 1):
            attn_copy(d).start()
        finish(o_loads(layer))
        delivered(0, qkv_recv.at[1:n_x])
        delivered(1, stat.at[0, 1:n_x])
        received(at_attn, attn_all.at[1:n_x])

        drain_mid = all_reduce(
            0, at_mid, lambda cols: jnp.dot(attn_all[...].reshape(batch, q_cols), wo[:, cols], preferred_element_type=F32), h_end, h_mid)
        reload(o_loads)

        local_norm(h_mid, gm_ref[layer], 1)
        start(sum_copies(1))

        def project(t):
            cols = tile_cols(t)
            gate = jnp.dot(n_buf[...], wg[:, cols], preferred_element_type=F32).astype(BF16)
            up = jnp.dot(n_buf[...], wu[:, cols], preferred_element_type=F32).astype(BF16)
            gu_part[0, :, :, :, cols] = gate.reshape(2, 2, rows, TILE)
            gu_part[1, :, :, :, cols] = up.reshape(2, 2, rows, TILE)

        def cross(g):
            cols = group_cols(g)
            received(at_mlp + g, gu_pair.at[:, :, :, cols])

            def tile(t):
                cols = tile_cols(t)
                pair = gu_part[:, 1 - chip, core, :, cols].astype(F32) * pair_scale[0] + gu_pair[:, 1 - chip, :, cols].astype(F32) * pair_scale[1]
                gu_send[:, :, cols] = pair.astype(BF16)

            each(*groups[g], tile)
            across_copy(g).start()

        def activate(g):
            received(at_mlp + len(groups) + g, gu_recv.at[:, :, group_cols(g)])

            def tile(t):
                cols = tile_cols(t)
                gate_up = (gu_part[:, chip, core, :, cols].astype(F32) * part_scale[0] + gu_pair[:, chip, :, cols].astype(F32) * part_scale[from_partner]
                           + gu_recv[:, :, cols].astype(F32)).astype(BF16).astype(F32)
                act_all[x, :, cols] = (jax.nn.silu(gate_up[0]) * gate_up[1]).astype(BF16)

            each(*groups[g], tile)
            start(act_copies(g))

        def activate_tail():
            received(at_mlp + tail, gu_direct.at[1:n_x])

            def tile(t):
                cols = tile_cols(t)
                total = gu_part[:, chip, core, :, cols].astype(F32) * part_scale[0]
                for d in range(1, n_x):
                    total = total + gu_direct[d, :, :, tile_cols(t - groups[tail][0])].astype(F32) * part_scale[d]
                gate_up = total.astype(BF16).astype(F32)
                act_all[x, :, cols] = (jax.nn.silu(gate_up[0]) * gate_up[1]).astype(BF16)

            each(*groups[tail], tile)
            start(act_copies(tail))

        for g in range(len(groups)):
            if g % 2 == 0:
                finish(gate_up_loads(layer, g // 2))
            each(*groups[g], project)
            if g < tail:
                pair_copy(g).start()
            else:
                start(tail_copies())
            if g == 2:
                received(at_first + 1, stat.at[1, 1:n_x])
                correction = corrections(1)
                for d in range(n_x):
                    part_scale[d] = jnp.broadcast_to(along_rows(correction(d), x * rows), (rows, TILE))
                for i, d in enumerate((0, from_partner)):
                    pair_scale[i] = jnp.broadcast_to(along_rows(correction(d), across * rows), (rows, TILE))
            if g >= 2:
                cross(g - 2)
        cross(tail - 1)
        for g in range(tail):
            activate(g)
        activate_tail()
        for piece in pieces:
            reload(lambda layer: gate_up_loads(layer, piece))
        drain_mid()
        delivered(2, attn_all.at[1:n_x])
        finish(down_loads(layer))
        for g, (first, last) in enumerate(groups):
            cols = group_cols(g)
            received(at_mlp + 2 * len(groups) + g, act_all.at[1:n_x, :, cols])

            def down(t):
                part = jnp.dot(act_all[:, :, cols].reshape(batch, (last - first) * TILE), wd[cols, tile_cols(t)], preferred_element_type=F32)
                acc[:, tile_cols(t)] = acc[:, tile_cols(t)] + part if g else part

            each(0, d_tiles, down)
        reload(down_loads)
        drain_end = all_reduce(1, at_end, lambda cols: acc[:, cols], h_mid, h_end)

        @pl.when(more)
        def _():
            local_norm(h_end, ga_ref[layer + 1], 0)
            start(sum_copies(0))
            finish(qkv_loads(layer + 1))
            for half in halves:
                project_qkv(*half)
                start(qkv_copies(*half))

        drain_end()

        delivered(3, stat.at[1, 1:n_x])
        delivered(8, gu_direct.at[1:n_x])
        delivered(9, gu_pair.at[:, :, :, 0:before])
        delivered(10, gu_recv.at[:, :, 0:before])
        delivered(11, act_all.at[1:n_x])

    each(0, layers, run_layer)
    hid_out[...] = h_end[...]


def cache_kernel(dims, hid_ref, new_ref, pos_ref, kc_ref, vc_ref, hid_out, kc_out, vc_out, hid_buf, kbuf, vbuf, in_sem, out_sem):
    layers, n_seq, kv_heads = dims
    first = lax.axis_index("x") * n_seq
    arrive, leave = [], []
    for layer in range(layers):
        for src, dst in ((kc_ref, kbuf), (vc_ref, vbuf)):
            arrive.append(pltpu.make_async_copy(src.at[layer], dst.at[layer], in_sem.at[len(arrive)]))
            arrive[-1].start()
    hidden_in = pltpu.make_async_copy(hid_ref, hid_buf, in_sem.at[len(arrive)])
    hidden_in.start()
    for layer in range(layers):
        for i, (buf, dst) in enumerate(((kbuf, kc_out), (vbuf, vc_out))):
            arrive[2 * layer + i].wait()
            for b in range(n_seq):
                rows = jnp.concatenate([new_ref[layer, i, h, b:b + 1, :] for h in range(kv_heads)], axis=0)
                buf[layer, b, pos_ref[0, first + b]] = rows.astype(BF16)
            leave.append(pltpu.make_async_copy(buf.at[layer], dst.at[layer], out_sem.at[len(leave)]))
            leave[-1].start()
    hidden_in.wait()
    leave.append(pltpu.make_async_copy(hid_buf, hid_out, out_sem.at[len(leave)]))
    leave[-1].start()
    for copy in leave:
        copy.wait()


def solution(mesh):
    n_x, n_y = mesh.shape['x'], mesh.shape['y']
    cache_spec = P(None, ('dp', 'x'), None, 'y', None)
    col_spec = P(None, 'x', 'y')
    row_spec = P(None, 'y', 'x')
    in_specs = (P('dp', 'x'), P('dp'), cache_spec, cache_spec, P(None, 'x'), P(None, 'x'), P(), P(), col_spec, col_spec, col_spec, row_spec, col_spec, col_spec, row_spec)
    out_specs = (P('dp', 'x'), cache_spec, cache_spec)

    def device_step(hidden, positions, k_cache, v_cache, g_attn, g_mlp, q_gain, k_gain, w_q, w_k, w_v, w_o, w_gate, w_up, w_down):
        batch, depth = hidden.shape
        layers, n_seq, slots, kv_heads, _ = k_cache.shape
        q_cols, kv_cols, ffn = w_q.shape[2], w_k.shape[2], w_gate.shape[2]
        rows = batch // n_y
        slots2 = slots * kv_heads
        dims = (layers, n_y, n_x, rows, depth, q_cols, kv_cols, ffn)
        cols_qkv = q_cols + 2 * kv_cols
        vmem = pl.BlockSpec(memory_space=pltpu.VMEM)
        hbm = pl.BlockSpec(memory_space=pl.ANY)
        cache_shape = (layers, n_seq, slots2, HEAD_DIM)
        peers = n_y * n_x
        d_tiles, f_tiles = depth // TILE, ffn // TILE
        receives = 4 + 2 * (d_tiles + 1) + 3 * len(split_tiles(f_tiles))
        positions = positions.reshape(1, batch)
        new_hidden, new_rows = pl.pallas_call(
            functools.partial(step_kernel, dims),
            out_shape=(jax.ShapeDtypeStruct((n_y, rows, depth), BF16), jax.ShapeDtypeStruct((layers, 2, kv_heads, n_seq, HEAD_DIM), F32)),
            in_specs=[hbm] * 16,
            out_specs=(vmem, vmem),
            scratch_shapes=[
                pltpu.VMEM((depth, cols_qkv), BF16),
                pltpu.VMEM((q_cols, depth), BF16),
                pltpu.VMEM((depth, ffn), BF16),
                pltpu.VMEM((depth, ffn), BF16),
                pltpu.VMEM((ffn, depth), BF16),
                pltpu.VMEM(cache_shape, BF16),
                pltpu.VMEM(cache_shape, BF16),
                pltpu.VMEM((batch, depth), BF16),
                pltpu.VMEM((2, n_x, 1, HEAD_DIM), F32),
                pltpu.VMEM((n_x, n_seq, cols_qkv), BF16),
                pltpu.VMEM((n_x, n_seq, cols_qkv), BF16),
                pltpu.VMEM((16 * n_seq, HEAD_DIM), F32),
                pltpu.VMEM((16 * n_seq, HEAD_DIM), F32),
                pltpu.VMEM((n_x, n_seq, q_cols), BF16),
                pltpu.VMEM((2, n_y, rows, depth), BF16),
                pltpu.VMEM((2, n_y, rows, depth), BF16),
                pltpu.VMEM((n_y, rows, depth), BF16),
                pltpu.VMEM((n_y, rows, depth), BF16),
                pltpu.VMEM((2, 2, 2, rows, ffn), BF16),
                pltpu.VMEM((2, 2, rows, ffn), BF16),
                pltpu.VMEM((2, rows, ffn), BF16),
                pltpu.VMEM((2, rows, ffn), BF16),
                pltpu.VMEM((n_x, rows, ffn), BF16),
                pltpu.VMEM((batch, depth), F32),
                pltpu.VMEM((1, batch), jnp.int32),
                pltpu.VMEM((1, HEAD_DIM), F32),
                pltpu.VMEM(g_attn.shape, BF16),
                pltpu.VMEM(g_mlp.shape, BF16),
                pltpu.VMEM(q_gain.shape, BF16),
                pltpu.VMEM(k_gain.shape, BF16),
                pltpu.VMEM((layers, 1, depth), F32),
                pltpu.VMEM((layers, 1, depth), F32),
                pltpu.VMEM((layers, 1, HEAD_DIM), F32),
                pltpu.VMEM((layers, 1, HEAD_DIM), F32),
                pltpu.VMEM((n_seq, 1, slots2), jnp.int32),
                pltpu.VMEM((n_x, n_seq, TILE), F32),
                pltpu.VMEM((2, rows, TILE), F32),
                pltpu.VMEM((2, kv_heads, n_seq, 1, HEAD_DIM), F32),
                pltpu.VMEM((n_x, 2, rows, (split_tiles(f_tiles)[-1][1] - split_tiles(f_tiles)[-1][0]) * TILE), BF16),
                pltpu.VMEM((16 * n_seq, slots2), F32),
                pltpu.VMEM((16 * n_seq, slots2), BF16),
                pltpu.SemaphoreType.DMA((12,)),
                pltpu.SemaphoreType.DMA((receives,)),
                pltpu.SemaphoreType.DMA((12 + 2 * ((len(split_tiles(f_tiles)) + 1) // 2) + 2 * layers,)),
            ],
            compiler_params=pltpu.CompilerParams(collective_id=0, has_side_effects=True, vmem_limit_bytes=64 * 1024 * 1024 - 65536),
        )(hidden.reshape(n_y, rows, depth), positions, inverse_frequencies(), g_attn, g_mlp, q_gain, k_gain,
          k_cache.reshape(cache_shape), v_cache.reshape(cache_shape), w_q, w_k, w_v, w_o, w_gate, w_up, w_down)
        return pl.pallas_call(
            functools.partial(cache_kernel, (layers, n_seq, kv_heads)),
            out_shape=tuple(jax.ShapeDtypeStruct(a.shape, a.dtype) for a in (hidden, k_cache, v_cache)),
            in_specs=[hbm, vmem, pl.BlockSpec(memory_space=pltpu.SMEM), hbm, hbm],
            out_specs=(hbm, hbm, hbm),
            scratch_shapes=[
                pltpu.VMEM(hidden.shape, BF16),
                pltpu.VMEM(k_cache.shape, BF16),
                pltpu.VMEM(k_cache.shape, BF16),
                pltpu.SemaphoreType.DMA((2 * layers + 1,)),
                pltpu.SemaphoreType.DMA((2 * layers + 1,)),
            ],
            compiler_params=pltpu.CompilerParams(vmem_limit_bytes=64 * 1024 * 1024 - 65536),
        )(new_hidden.reshape(batch, depth), new_rows, positions, k_cache, v_cache)

    return jax.shard_map(device_step, mesh=mesh, in_specs=in_specs, out_specs=out_specs, check_vma=False)
```

```python
import functools

import jax
import jax.numpy as jnp
import numpy as np
from jax import lax
from jax.experimental import pallas as pl
from jax.experimental.pallas import tpu as pltpu
from jax.sharding import PartitionSpec as P

HEAD_DIM = 128
NORM_EPS = 1e-6
ROPE_BASE = 1000000.0
TILE = 256
GROUP_TILES = (2, 3, 3, 4, 3, 2)
SEQS = 4
MESH = pl.DeviceIdType.MESH
F32 = jnp.float32
BF16 = jnp.bfloat16


def inverse_frequencies():
    half_dim = HEAD_DIM // 2
    freqs = np.power(np.float32(ROPE_BASE), (-2.0 * np.arange(half_dim) / HEAD_DIM).astype(np.float32))
    return np.concatenate([freqs, freqs])[None].astype(np.float32)


def split_tiles(n_tiles):
    share = n_tiles / sum(GROUP_TILES)
    edges = [round(share * sum(GROUP_TILES[:i])) for i in range(len(GROUP_TILES) + 1)]
    return [(a, b) for a, b in zip(edges, edges[1:]) if b > a]


def step_kernel(dims, *refs):
    (layers, n_y, n_x, rows, depth, q_cols, kv_cols, ffn) = dims
    (hid_any, pos_any, freq_any, ga_any, gm_any, qg_any, kg_any, kc_ref, vc_ref,
     wq_ref, wk_ref, wv_ref, wo_ref, wg_ref, wu_ref, wd_ref,
     hid_out, new_out,
     wqkv, wo, wg, wu, wd, kbuf, vbuf, n_buf, stat, qkv_part, qkv_recv, q_rows, o_rows, attn_all,
     ar_part, ar_recv, h_mid, h_end, gu_part, gu_pair, gu_send, gu_recv, act_all, acc,
     pos_ref, freq_ref, ga_raw, gm_raw, qg_raw, kg_raw, ga_ref, gm_ref, qg_ref, kg_ref, slot_ref, part_scale, pair_scale, kv_rows, s_rows, p_rows,
     send_sem, recv_sem, local_sem) = refs
    batch = n_y * rows
    cols_qkv = q_cols + 2 * kv_cols
    q_heads = q_cols // HEAD_DIM
    kv_heads = kv_cols // HEAD_DIM
    group = q_heads // kv_heads
    model_dim = depth * n_x
    slots2 = kbuf.shape[2]
    n_seq = batch // n_x
    peers = n_y * n_x
    d_tiles, f_tiles, qkv_tiles = depth // TILE, ffn // TILE, cols_qkv // TILE

    y = lax.axis_index("y")
    x = lax.axis_index("x")
    chip = x // 2
    core = x % 2
    partner = 2 * chip + (1 - core)
    across = 2 * (1 - chip) + core
    diagonal = 2 * (1 - chip) + (1 - core)

    groups = split_tiles(f_tiles)
    at_qkv, at_first, at_attn, at_mid = 0, 1, 3, 4
    at_end = at_mid + d_tiles + 1
    at_mlp = at_end + d_tiles + 1

    def remote(src, dst, to_send, to_recv, to_y, to_x):
        return pltpu.make_async_remote_copy(
            src_ref=src, dst_ref=dst, send_sem=send_sem.at[to_send], recv_sem=recv_sem.at[to_recv],
            device_id={"y": to_y, "x": to_x}, device_id_type=MESH)

    def received(i, like):
        pltpu.make_async_copy(like, like, recv_sem.at[i]).wait()

    def delivered(i, like):
        pltpu.make_async_copy(like, like, send_sem.at[i]).wait()

    def each(first, last, body):
        def step(i, carry):
            body(i)
            return carry

        lax.fori_loop(first, last, step, 0)

    def tile_cols(t):
        return pl.ds(pl.multiple_of(t * TILE, TILE), TILE)

    def qkv_loads(layer):
        return [pltpu.make_async_copy(wq_ref.at[layer], wqkv.at[:, 0:q_cols], local_sem.at[0]),
                pltpu.make_async_copy(wk_ref.at[layer], wqkv.at[:, q_cols:q_cols + kv_cols], local_sem.at[1]),
                pltpu.make_async_copy(wv_ref.at[layer], wqkv.at[:, q_cols + kv_cols:cols_qkv], local_sem.at[2])]

    def o_loads(layer):
        return [pltpu.make_async_copy(wo_ref.at[layer], wo, local_sem.at[3])]

    def gate_up_loads(layer):
        return [pltpu.make_async_copy(src.at[layer], dst, local_sem.at[4 + i]) for i, (src, dst) in enumerate(((wg_ref, wg), (wu_ref, wu)))]

    def down_loads(layer):
        return [pltpu.make_async_copy(wd_ref.at[layer], wd, local_sem.at[6])]

    def cache_loads(layer):
        return [pltpu.make_async_copy(src.at[layer], dst.at[layer], local_sem.at[7 + i * layers + layer])
                for i, (src, dst) in enumerate(((kc_ref, kbuf), (vc_ref, vbuf)))]

    def start(copies):
        for copy in copies:
            copy.start()

    def finish(copies):
        for copy in copies:
            copy.wait()

    row_i = lax.broadcasted_iota(jnp.int32, (rows, HEAD_DIM), 0)
    lane_i = lax.broadcasted_iota(jnp.int32, (rows, HEAD_DIM), 1)

    def along_lanes(column, first_row):
        return jnp.sum(jnp.where(lane_i == row_i + first_row, column, 0.0), axis=0, keepdims=True)

    def along_rows(lanes, first_row):
        return jnp.sum(jnp.where(lane_i == row_i + first_row, lanes, 0.0), axis=1, keepdims=True)

    def local_norm(hidden_ref, gain, i):
        def block(b, lanes):
            vals = hidden_ref[b].astype(F32)
            sums = jnp.sum(vals * vals, axis=1, keepdims=True)
            n_buf[pl.ds(pl.multiple_of(b * rows, rows), rows), :] = (vals * lax.rsqrt(sums / depth + NORM_EPS) * gain).astype(BF16)
            return lanes + along_lanes(sums, b * rows)

        stat[i, 0] = lax.fori_loop(0, n_y, block, jnp.zeros((1, HEAD_DIM), F32))

    def corrections(i):
        total = stat[i, 0]
        for d in range(1, n_x):
            total = total + stat[i, d]
        scale = lax.rsqrt(total / model_dim + NORM_EPS)
        return lambda *d: ratio(scale, local_scale(i, *d))

    def local_scale(i, *d):
        return lax.rsqrt(sum(stat[i, k] for k in d) / (len(d) * depth) + NORM_EPS)

    def ratio(scale, local):
        return jnp.where(scale > 0.0, scale / local, 0.0)

    def all_reduce(i, base, tile_product, residual_ref, result_ref):
        send = 4 + 2 * i

        def scatter(t, d):
            cols = tile_cols(t)
            return remote(ar_part.at[i, (y + d) % n_y, :, cols], ar_recv.at[i, d, :, cols], send, base + t, (y + d) % n_y, x)

        def gather(t, d):
            mine = result_ref.at[y, :, tile_cols(t)]
            return remote(mine, mine, send + 1, base + d_tiles, (y + d) % n_y, x)

        def send_tile(t):
            ar_part[i, :, :, tile_cols(t)] = tile_product(tile_cols(t)).astype(BF16).reshape(n_y, rows, TILE)
            for d in (2, 3, 1):
                scatter(t, d).start()

        each(0, d_tiles, send_tile)

        def sum_tile(t):
            cols = tile_cols(t)
            received(base + t, ar_recv.at[i, 1:n_y, :, cols])
            total = ar_part[i, y, :, cols].astype(F32)
            for d in range(1, n_y):
                total = total + ar_recv[i, d, :, cols].astype(F32)
            new = (residual_ref[y, :, cols].astype(F32) + total.astype(BF16).astype(F32)).astype(BF16)
            result_ref[y, :, cols] = new
            for d in (2, 3, 1):
                gather(t, d).start()

        each(0, d_tiles, sum_tile)
        received(base + d_tiles, ar_recv.at[i, 1:n_y])

        def drain():
            delivered(send, ar_recv.at[i, 1:n_y])
            delivered(send + 1, ar_recv.at[i, 1:n_y])

        return drain

    def qkv_copies(first, last):
        cols = pl.ds(first * TILE, (last - first) * TILE)
        return [remote(qkv_part.at[(x + d) % n_x, :, cols], qkv_recv.at[d, :, cols], 0, at_qkv, y, (x + d) % n_x) for d in (2, 3, 1)]

    def sum_copies(i):
        if i == 0:
            return [remote(stat.at[0, 0], stat.at[0, d], 1, at_first, y, (x + d) % n_x) for d in (2, 3, 1)]
        return [remote(stat.at[1, 0], stat.at[1, k], 3, at_first + 1 if k > 1 else at_mlp + 3 * len(groups), y, to_x)
                for k, to_x in ((1, partner), (2, across), (3, diagonal))]

    def attn_copy(d):
        return remote(attn_all.at[x], attn_all.at[x], 2, at_attn, y, (x + d) % n_x)

    def group_cols(g):
        return pl.ds(groups[g][0] * TILE, (groups[g][1] - groups[g][0]) * TILE)

    def pair_copy(g):
        cols = group_cols(g)
        return remote(gu_part.at[:, :, 1 - core, :, cols], gu_pair.at[:, :, :, cols], 9, at_mlp + g, y, partner)

    def across_copy(g):
        cols = group_cols(g)
        return remote(gu_send.at[:, :, cols], gu_recv.at[:, :, cols], 10, at_mlp + len(groups) + g, y, across)

    def act_copies(g):
        mine = act_all.at[x, :, group_cols(g)]
        return [remote(mine, mine, 11, at_mlp + 2 * len(groups) + g, y, to_x) for to_x in (diagonal, across, partner)]

    def project_qkv(first, last):
        def tile(t):
            cols = tile_cols(t)
            part = jnp.dot(n_buf[...], wqkv[:, cols], preferred_element_type=F32).astype(BF16)
            qkv_part[:, :, cols] = part.reshape(n_x, n_seq, TILE)

        each(first, last, tile)

    halves = ((0, (qkv_tiles + 1) // 2), ((qkv_tiles + 1) // 2, qkv_tiles))

    barrier = pltpu.get_barrier_semaphore()
    each(1, peers, lambda e: pl.semaphore_signal(
        barrier, inc=1, device_id={"y": (y + e // n_x) % n_y, "x": (x + e % n_x) % n_x}, device_id_type=MESH))
    small = [pltpu.make_async_copy(src, dst, local_sem.at[7 + 2 * layers + i]) for i, (src, dst) in enumerate((
        (hid_any, h_end), (ga_any, ga_raw), (gm_any, gm_raw), (qg_any, qg_raw), (kg_any, kg_raw), (pos_any, pos_ref), (freq_any, freq_ref)))]
    start(small)
    start(qkv_loads(0))
    finish(small)
    start(o_loads(0) + cache_loads(0) + gate_up_loads(0) + down_loads(0))
    for layer in range(1, layers):
        start(cache_loads(layer))
    for raw, wide in ((ga_raw, ga_ref), (gm_raw, gm_ref), (qg_raw, qg_ref), (kg_raw, kg_ref)):
        for layer in range(layers):
            wide[layer] = raw[...].astype(F32)[layer:layer + 1]
    local_norm(h_end, ga_ref[0], 0)
    q_rows[...] = jnp.zeros_like(q_rows)
    finish(qkv_loads(0))
    project_qkv(0, qkv_tiles)
    pl.semaphore_wait(barrier, peers - 1)
    start(sum_copies(0))
    for half in halves:
        start(qkv_copies(*half))

    my_pos = jnp.sum(
        jnp.where(lax.broadcasted_iota(jnp.int32, (n_seq, batch), 1) == lax.broadcasted_iota(jnp.int32, (n_seq, batch), 0) + x * n_seq,
                  pos_ref[...].astype(F32), 0.0), axis=1, keepdims=True)
    angles = my_pos * freq_ref[...]
    cos_tab = jnp.cos(angles)
    sin_tab = jnp.where(lax.broadcasted_iota(jnp.int32, (n_seq, HEAD_DIM), 1) < HEAD_DIM // 2, -1.0, 1.0) * jnp.sin(angles)
    slot_ref[...] = jnp.broadcast_to(my_pos.astype(jnp.int32), (n_seq, slots2)).reshape(slot_ref.shape)

    slot_row = lax.broadcasted_iota(jnp.int32, (slots2, HEAD_DIM), 0)
    slot_id = slot_row // kv_heads
    head_id = slot_row % kv_heads
    score_col = lax.broadcasted_iota(jnp.int32, (16, slots2), 1)
    score_head = lax.broadcasted_iota(jnp.int32, (16, slots2), 0) // group
    score_slot = score_col // kv_heads
    score_own = (score_col % kv_heads == score_head) | (score_head >= kv_heads)

    def run_layer(layer):
        more = layer + 1 < layers

        def reload(loads):
            @pl.when(more)
            def _():
                start(loads(layer + 1))

        reload(qkv_loads)
        received(at_first, stat.at[0, 1:n_x])
        correction = corrections(0)
        for d in range(n_x):
            part_scale[d] = jnp.broadcast_to(along_rows(correction(d), x * n_seq), (n_seq, TILE))
        received(at_qkv, qkv_recv.at[1:n_x])

        def projected(cols, scale_cols):
            total = qkv_part[x, :, cols].astype(F32) * part_scale[0, :, scale_cols]
            for d in range(1, n_x):
                total = total + qkv_recv[d, :, cols].astype(F32) * part_scale[d, :, scale_cols]
            return total.astype(BF16).astype(F32)

        for h in range(q_heads + kv_heads):
            vals = projected(pl.ds(h * HEAD_DIM, HEAD_DIM), pl.ds(0, HEAD_DIM))
            mean_sq = jnp.mean(vals * vals, axis=-1, keepdims=True)
            normed = vals * lax.rsqrt(mean_sq + NORM_EPS) * (qg_ref if h < q_heads else kg_ref)[layer]
            turned = (normed * cos_tab + pltpu.roll(normed, HEAD_DIM // 2, 1) * sin_tab).astype(BF16).astype(F32)
            if h < q_heads:
                q_rows[pl.ds(h, n_seq, stride=16), :] = turned
            else:
                new_out[layer, 0, h - q_heads] = turned
                kv_rows[0, h - q_heads] = turned.reshape(n_seq, 1, HEAD_DIM)
        for h in range(kv_heads):
            vals = projected(pl.ds(q_cols + kv_cols + h * HEAD_DIM, HEAD_DIM), pl.ds(0, HEAD_DIM))
            new_out[layer, 1, h] = vals
            kv_rows[1, h] = vals.reshape(n_seq, 1, HEAD_DIM)

        finish(cache_loads(layer))

        def update(i):
            for u in range(SEQS):
                b = i * SEQS + u
                hit = slot_id == slot_ref[b][:, :HEAD_DIM]
                for j, buf in enumerate((kbuf, vbuf)):
                    fresh = kv_rows[j, 0, b]
                    for h in range(1, kv_heads):
                        fresh = jnp.where(head_id == h, kv_rows[j, h, b], fresh)
                    buf[layer, b] = jnp.where(hit, fresh, buf[layer, b].astype(F32)).astype(BF16)

        each(0, n_seq // SEQS, update)
        for b in range(n_seq):
            q_b = q_rows[b * 16:(b + 1) * 16, :].astype(BF16)
            scores = lax.dot_general(q_b, kbuf[layer, b], (((1,), (1,)), ((), ())), preferred_element_type=F32) * (HEAD_DIM ** -0.5)
            s_rows[b * 16:(b + 1) * 16, :] = jnp.where(score_own & (score_slot <= slot_ref[b]), scores, -1e30)

        def softmax(i):
            block = pl.ds(pl.multiple_of(i * 16 * SEQS, 16 * SEQS), 16 * SEQS)
            scores = s_rows[block, :]
            e = jnp.exp(scores - jnp.max(scores, axis=1, keepdims=True))
            p_rows[block, :] = (e / jnp.sum(e, axis=1, keepdims=True)).astype(BF16)

        each(0, n_seq // SEQS, softmax)
        for b in range(n_seq):
            o_rows[b * 16:(b + 1) * 16, :] = jnp.dot(p_rows[b * 16:(b + 1) * 16, :], vbuf[layer, b], preferred_element_type=F32)
        for h in range(q_heads):
            attn_all[x, :, h * HEAD_DIM:(h + 1) * HEAD_DIM] = o_rows[pl.ds(h, n_seq, stride=16), :].astype(BF16)
        for d in (2, 3, 1):
            attn_copy(d).start()
        finish(o_loads(layer))
        delivered(0, qkv_recv.at[1:n_x])
        delivered(1, stat.at[0, 1:n_x])
        received(at_attn, attn_all.at[1:n_x])

        drain_mid = all_reduce(
            0, at_mid, lambda cols: jnp.dot(attn_all[...].reshape(batch, q_cols), wo[:, cols], preferred_element_type=F32), h_end, h_mid)
        reload(o_loads)

        local_norm(h_mid, gm_ref[layer], 1)
        start(sum_copies(1))
        finish(gate_up_loads(layer))

        def project(t):
            cols = tile_cols(t)
            gate = jnp.dot(n_buf[...], wg[:, cols], preferred_element_type=F32).astype(BF16)
            up = jnp.dot(n_buf[...], wu[:, cols], preferred_element_type=F32).astype(BF16)
            gu_part[0, :, :, :, cols] = gate.reshape(2, 2, rows, TILE)
            gu_part[1, :, :, :, cols] = up.reshape(2, 2, rows, TILE)

        def cross(g):
            cols = group_cols(g)
            received(at_mlp + g, gu_pair.at[:, :, :, cols])

            def tile(t):
                cols = tile_cols(t)
                pair = gu_part[:, 1 - chip, core, :, cols].astype(F32) * pair_scale[0] + gu_pair[:, 1 - chip, :, cols].astype(F32) * pair_scale[1]
                gu_send[:, :, cols] = pair.astype(BF16)

            each(*groups[g], tile)
            across_copy(g).start()

        def activate(g):
            received(at_mlp + len(groups) + g, gu_recv.at[:, :, group_cols(g)])

            def tile(t):
                cols = tile_cols(t)
                gate_up = (gu_part[:, chip, core, :, cols].astype(F32) * part_scale[0] + gu_pair[:, chip, :, cols].astype(F32) * part_scale[1]
                           + gu_recv[:, :, cols].astype(F32) * part_scale[2]).astype(BF16).astype(F32)
                act_all[x, :, cols] = (jax.nn.silu(gate_up[0]) * gate_up[1]).astype(BF16)

            each(*groups[g], tile)
            start(act_copies(g))

        for g in range(len(groups)):
            each(*groups[g], project)
            pair_copy(g).start()
            if g == 2:
                received(at_mlp + 3 * len(groups), stat.at[1, 1:2])
                for k in range(2):
                    column = along_rows(ratio(local_scale(1, 0, 1), local_scale(1, k)), across * rows)
                    pair_scale[k] = jnp.broadcast_to(column, (rows, TILE))
            if g >= 2:
                cross(g - 2)
        reload(gate_up_loads)
        for g in range(max(len(groups) - 2, 0), len(groups)):
            cross(g)
        received(at_first + 1, stat.at[1, 2:4])
        correction = corrections(1)
        for k, sources in enumerate(((0,), (1,), (2, 3))):
            part_scale[k] = jnp.broadcast_to(along_rows(correction(*sources), x * rows), (rows, TILE))
        for g in range(len(groups)):
            activate(g)
        drain_mid()
        delivered(2, attn_all.at[1:n_x])
        finish(down_loads(layer))
        for g, (first, last) in enumerate(groups):
            cols = group_cols(g)
            received(at_mlp + 2 * len(groups) + g, act_all.at[1:n_x, :, cols])

            def down(t):
                part = jnp.dot(act_all[:, :, cols].reshape(batch, (last - first) * TILE), wd[cols, tile_cols(t)], preferred_element_type=F32)
                acc[:, tile_cols(t)] = acc[:, tile_cols(t)] + part if g else part

            each(0, d_tiles, down)
        reload(down_loads)
        drain_end = all_reduce(1, at_end, lambda cols: acc[:, cols], h_mid, h_end)

        @pl.when(more)
        def _():
            local_norm(h_end, ga_ref[layer + 1], 0)
            start(sum_copies(0))
            finish(qkv_loads(layer + 1))
            for half in halves:
                project_qkv(*half)
                start(qkv_copies(*half))

        drain_end()

        delivered(3, stat.at[1, 1:n_x])
        delivered(9, gu_pair)
        delivered(10, gu_recv)
        delivered(11, act_all.at[1:n_x])

    each(0, layers, run_layer)
    hid_out[...] = h_end[...]


def cache_kernel(dims, hid_ref, new_ref, pos_ref, kc_ref, vc_ref, hid_out, kc_out, vc_out, hid_buf, kbuf, vbuf, in_sem, out_sem):
    layers, n_seq, kv_heads = dims
    first = lax.axis_index("x") * n_seq
    arrive, leave = [], []
    for layer in range(layers):
        for src, dst in ((kc_ref, kbuf), (vc_ref, vbuf)):
            arrive.append(pltpu.make_async_copy(src.at[layer], dst.at[layer], in_sem.at[len(arrive)]))
            arrive[-1].start()
    hidden_in = pltpu.make_async_copy(hid_ref, hid_buf, in_sem.at[len(arrive)])
    hidden_in.start()
    for layer in range(layers):
        for i, (buf, dst) in enumerate(((kbuf, kc_out), (vbuf, vc_out))):
            arrive[2 * layer + i].wait()
            for b in range(n_seq):
                rows = jnp.concatenate([new_ref[layer, i, h, b:b + 1, :] for h in range(kv_heads)], axis=0)
                buf[layer, b, pos_ref[0, first + b]] = rows.astype(BF16)
            leave.append(pltpu.make_async_copy(buf.at[layer], dst.at[layer], out_sem.at[len(leave)]))
            leave[-1].start()
    hidden_in.wait()
    leave.append(pltpu.make_async_copy(hid_buf, hid_out, out_sem.at[len(leave)]))
    leave[-1].start()
    for copy in leave:
        copy.wait()


def solution(mesh):
    n_x, n_y = mesh.shape['x'], mesh.shape['y']
    cache_spec = P(None, ('dp', 'x'), None, 'y', None)
    col_spec = P(None, 'x', 'y')
    row_spec = P(None, 'y', 'x')
    in_specs = (P('dp', 'x'), P('dp'), cache_spec, cache_spec, P(None, 'x'), P(None, 'x'), P(), P(), col_spec, col_spec, col_spec, row_spec, col_spec, col_spec, row_spec)
    out_specs = (P('dp', 'x'), cache_spec, cache_spec)

    def device_step(hidden, positions, k_cache, v_cache, g_attn, g_mlp, q_gain, k_gain, w_q, w_k, w_v, w_o, w_gate, w_up, w_down):
        batch, depth = hidden.shape
        layers, n_seq, slots, kv_heads, _ = k_cache.shape
        q_cols, kv_cols, ffn = w_q.shape[2], w_k.shape[2], w_gate.shape[2]
        rows = batch // n_y
        slots2 = slots * kv_heads
        dims = (layers, n_y, n_x, rows, depth, q_cols, kv_cols, ffn)
        cols_qkv = q_cols + 2 * kv_cols
        vmem = pl.BlockSpec(memory_space=pltpu.VMEM)
        hbm = pl.BlockSpec(memory_space=pl.ANY)
        cache_shape = (layers, n_seq, slots2, HEAD_DIM)
        peers = n_y * n_x
        d_tiles, f_tiles = depth // TILE, ffn // TILE
        receives = 4 + 2 * (d_tiles + 1) + 3 * len(split_tiles(f_tiles)) + 1
        positions = positions.reshape(1, batch)
        new_hidden, new_rows = pl.pallas_call(
            functools.partial(step_kernel, dims),
            out_shape=(jax.ShapeDtypeStruct((n_y, rows, depth), BF16), jax.ShapeDtypeStruct((layers, 2, kv_heads, n_seq, HEAD_DIM), F32)),
            in_specs=[hbm] * 16,
            out_specs=(vmem, vmem),
            scratch_shapes=[
                pltpu.VMEM((depth, cols_qkv), BF16),
                pltpu.VMEM((q_cols, depth), BF16),
                pltpu.VMEM((depth, ffn), BF16),
                pltpu.VMEM((depth, ffn), BF16),
                pltpu.VMEM((ffn, depth), BF16),
                pltpu.VMEM(cache_shape, BF16),
                pltpu.VMEM(cache_shape, BF16),
                pltpu.VMEM((batch, depth), BF16),
                pltpu.VMEM((2, n_x, 1, HEAD_DIM), F32),
                pltpu.VMEM((n_x, n_seq, cols_qkv), BF16),
                pltpu.VMEM((n_x, n_seq, cols_qkv), BF16),
                pltpu.VMEM((16 * n_seq, HEAD_DIM), F32),
                pltpu.VMEM((16 * n_seq, HEAD_DIM), F32),
                pltpu.VMEM((n_x, n_seq, q_cols), BF16),
                pltpu.VMEM((2, n_y, rows, depth), BF16),
                pltpu.VMEM((2, n_y, rows, depth), BF16),
                pltpu.VMEM((n_y, rows, depth), BF16),
                pltpu.VMEM((n_y, rows, depth), BF16),
                pltpu.VMEM((2, 2, 2, rows, ffn), BF16),
                pltpu.VMEM((2, 2, rows, ffn), BF16),
                pltpu.VMEM((2, rows, ffn), BF16),
                pltpu.VMEM((2, rows, ffn), BF16),
                pltpu.VMEM((n_x, rows, ffn), BF16),
                pltpu.VMEM((batch, depth), F32),
                pltpu.VMEM((1, batch), jnp.int32),
                pltpu.VMEM((1, HEAD_DIM), F32),
                pltpu.VMEM(g_attn.shape, BF16),
                pltpu.VMEM(g_mlp.shape, BF16),
                pltpu.VMEM(q_gain.shape, BF16),
                pltpu.VMEM(k_gain.shape, BF16),
                pltpu.VMEM((layers, 1, depth), F32),
                pltpu.VMEM((layers, 1, depth), F32),
                pltpu.VMEM((layers, 1, HEAD_DIM), F32),
                pltpu.VMEM((layers, 1, HEAD_DIM), F32),
                pltpu.VMEM((n_seq, 1, slots2), jnp.int32),
                pltpu.VMEM((n_x, n_seq, TILE), F32),
                pltpu.VMEM((2, rows, TILE), F32),
                pltpu.VMEM((2, kv_heads, n_seq, 1, HEAD_DIM), F32),
                pltpu.VMEM((16 * n_seq, slots2), F32),
                pltpu.VMEM((16 * n_seq, slots2), BF16),
                pltpu.SemaphoreType.DMA((12,)),
                pltpu.SemaphoreType.DMA((receives,)),
                pltpu.SemaphoreType.DMA((14 + 2 * layers,)),
            ],
            compiler_params=pltpu.CompilerParams(collective_id=0, has_side_effects=True, vmem_limit_bytes=64 * 1024 * 1024 - 65536),
        )(hidden.reshape(n_y, rows, depth), positions, inverse_frequencies(), g_attn, g_mlp, q_gain, k_gain,
          k_cache.reshape(cache_shape), v_cache.reshape(cache_shape), w_q, w_k, w_v, w_o, w_gate, w_up, w_down)
        return pl.pallas_call(
            functools.partial(cache_kernel, (layers, n_seq, kv_heads)),
            out_shape=tuple(jax.ShapeDtypeStruct(a.shape, a.dtype) for a in (hidden, k_cache, v_cache)),
            in_specs=[hbm, vmem, pl.BlockSpec(memory_space=pltpu.SMEM), hbm, hbm],
            out_specs=(hbm, hbm, hbm),
            scratch_shapes=[
                pltpu.VMEM(hidden.shape, BF16),
                pltpu.VMEM(k_cache.shape, BF16),
                pltpu.VMEM(k_cache.shape, BF16),
                pltpu.SemaphoreType.DMA((2 * layers + 1,)),
                pltpu.SemaphoreType.DMA((2 * layers + 1,)),
            ],
            compiler_params=pltpu.CompilerParams(vmem_limit_bytes=64 * 1024 * 1024 - 65536),
        )(new_hidden.reshape(batch, depth), new_rows, positions, k_cache, v_cache)

    return jax.shard_map(device_step, mesh=mesh, in_specs=in_specs, out_specs=out_specs, check_vma=False)
```
